32 devices in a mesh: batch: 8 (over z, y), block: 2 (over x), tensor: 2 (over core).
Axes of the slice: x: 2, y: 2, z: 4, core: 2. Of those that a mesh axis runs over, the one named last changes fastest.
Arguments:
- tokens: bfloat16 [8, 1024, 768], P('batch', 'block'), may hold values from -6 to 6
- segment_ids: int32 [8, 1024], P('batch'), may hold values from 0 to 3, never falling along the last dimension, each value on 1 to 512 neighbouring positions
- head_perm: int32 [12], P('tensor'), may hold values from 0 to 1, as said below
- w_qkv: bfloat16 [768, 3, 768], P(None, None, 'tensor'), may hold values from -0.21875 to 0.21875
- b_qv: float32 [2, 768], P(None, 'tensor'), may hold values from -0.625 to 0.625
- w_out: bfloat16 [768, 768], P('tensor'), may hold values from -2.5 to 2.5
- b_out: float32 [768], replicated, may hold values from -3 to 3
- norm1_gain: float32 [768], replicated, may hold values from 0.5 to 1.5
- norm1_shift: float32 [768], replicated, may hold values from -3 to 3
- w_up: bfloat16 [768, 3072], P(None, 'tensor'), may hold values from -0.21875 to 0.21875
- b_up: float32 [3072], P('tensor'), may hold values from -3 to 3
- w_down: bfloat16 [3072, 768], P('tensor'), may hold values from -0.109375 to 0.109375
- b_down: float32 [768], replicated, may hold values from -3 to 3
- norm2_gain: float32 [768], replicated, may hold values from 0.5 to 1.5
- norm2_shift: float32 [768], replicated, may hold values from -3 to 3
- grad_out: bfloat16 [8, 1024, 768], P('batch', 'block'), may hold values from -6 to 6
Outputs:
- output: bfloat16 [8, 1024, 768], P('batch', 'block')
- grad_tokens: bfloat16 [8, 1024, 768], P('batch', 'block')
- grad_w_qkv: float32 [768, 3, 768], P('batch', None, 'tensor')
- grad_b_qv: float32 [2, 768], P(None, ('tensor', 'batch'))
- grad_w_out: float32 [768, 768], P('tensor', 'batch')
- grad_b_out: float32 [768], P('batch')
- grad_norm1_gain: float32 [768], P('batch')
- grad_norm1_shift: float32 [768], P('batch')
- grad_w_up: float32 [768, 3072], P('batch', 'tensor')
- grad_b_up: float32 [3072], P(('tensor', 'batch'))
- grad_w_down: float32 [3072, 768], P('tensor', 'batch')
- grad_b_down: float32 [768], P('batch')
- grad_norm2_gain: float32 [768], P('batch')
- grad_norm2_shift: float32 [768], P('batch')
The draws below stay inside these ranges and needn't reach their ends.
Inputs may be any that keep to these rules, and one draw needn't show every extreme that they name: `head_perm`: heads are taken in aligned groups of 6 (heads 0 to 5, 6 to 11, and so on); in each such group exactly half have 1 and half have 0.
All inputs are finite; a program needn't handle non-finite values.
Results may differ from the reference program's by a relative error of at most 0.02.
The reference program's roundings to bfloat16 on the way count: a program that leaves them out, or rounds other values in their place, can miss the bound.
Values may be sent and summed in bfloat16 or wider, within the bound.
A program may use at most 128 MiB of HBM per device.

```python
import math
import jax
import jax.numpy as jnp
import numpy as np
from jax import lax

D = 768
H = 12
DH = 64
FF = 3072
BLK = 512
DOCS = 4
SEQS = 8
LEN = 1024
HT = 6
N_BLOCK = 2


def draw_head_perm(key, part):
    pattern = (jnp.arange(HT) >= HT // 2).astype(jnp.int32)
    group_keys = jax.random.split(key, H // HT)

    def shuffle(group_key):
        return jax.random.permutation(group_key, pattern)
    return jax.vmap(shuffle)(group_keys).reshape(H)


def spiked(array, key, source, target, shards_of, factor):
    owner, partner = [(jnp.arange(array.shape[dim]) // (array.shape[dim] // shards_of)).reshape([-1 if axis == dim else 1 for axis in range(array.ndim)]) for dim in (source, target)]
    chosen = jax.random.permutation(key, shards_of)[partner]
    strong = (owner == chosen) | (owner == (partner + shards_of // 2) % shards_of)
    return jnp.where(strong, factor * array, array)


def steps_of(stream_key, extent, cuts, smallest, largest):
    loudness = 1.0
    for dim, blocks in cuts:
        draws = jax.random.uniform(jax.random.fold_in(jax.random.fold_in(stream_key, 6), dim), (blocks,), jnp.float32, smallest / len(cuts), largest / len(cuts))
        loudness = loudness * jnp.repeat(jnp.exp(draws), extent[dim] // blocks).reshape((-1,) + (1,) * (len(extent) - 1 - dim))
    return loudness


def profile(count, total, bound, skew):
    portions = [(1 << 20) // math.isqrt(grade ** skew) + 1 for grade in range(2, count + 1)]
    spare, counts = total - bound - (count - 1), [1] * (count - 1)
    while spare > 0:
        movable = [i for i in range(count - 1) if counts[i] < bound]
        mass, budget = sum([portions[i] for i in movable]), spare
        for i in movable:
            extra = min(bound - counts[i], max(1, budget * portions[i] // mass), spare)
            counts[i] = counts[i] + extra
            spare = spare - extra
    return np.array([bound] + counts)


def uneven(rng, count, total, limit, slope):
    if count == 2:
        one = jax.random.randint(rng, (), max(1, total - limit), min(limit, total - 1) + 1)
        return jnp.stack([one, total - one])
    sizes = jnp.asarray(profile(count, total, limit, slope), jnp.int32)
    couples = (count - 1) // 2
    source_of, receiver = sizes[1:1 + 2 * couples:2], sizes[2:2 + 2 * couples:2]
    slack = jnp.minimum(source_of - 1, limit - receiver)
    shifted = jax.random.randint(jax.random.fold_in(rng, 1), (couples,), 0, 1 << 20) % (slack + 1)
    sizes = sizes.at[1:1 + 2 * couples:2].set(source_of - shifted).at[2:2 + 2 * couples:2].set(receiver + shifted)
    return sizes[jax.random.permutation(jax.random.fold_in(rng, 2), count)]


def scatter_about(key, shape, scale, limit, shards=(), dtype=jnp.bfloat16):
    array = scale * jax.random.normal(key, shape, jnp.float32)
    if shards:
        array = array * steps_of(key, shape, shards, -0.22, 0.18)
    return jnp.clip(array, -limit, limit).astype(dtype)


def heavy_noise(own_key, extent, scale, bound, pieces, heavy, kind=jnp.bfloat16):
    values = scale * jax.random.normal(own_key, extent, jnp.float32)
    if pieces:
        values = values * steps_of(own_key, extent, pieces, -0.22, 0.18)
    return jnp.clip(spiked(values, jax.random.fold_in(own_key, 3), *heavy), -bound, bound).astype(kind)


def setup_inputs(seed: int = 0) -> dict:
    seeds = jax.random.split(jax.random.key(seed), 17)
    return {
        "tokens": heavy_noise(seeds[0], (SEQS, LEN, D), 1.0, 6.0, ((0, 8), (1, 2)), (0, 2, 8, 2.0)),
        "segment_ids": jax.vmap(lambda own: jnp.searchsorted(jnp.cumsum(uneven(own, DOCS, LEN, BLK, 0)), jnp.arange(LEN), side="right"))(jax.random.split(seeds[1], SEQS)).reshape((SEQS, LEN)).astype(jnp.int32),
        "head_perm": draw_head_perm(jax.random.fold_in(seeds[16], 71), 0),
        "w_qkv": scatter_about(seeds[3], (D, 3, D), D ** -0.5, 0.21875, ((2, 2),)),
        "b_qv": scatter_about(seeds[4], (2, D), 0.1, 0.625, ((1, 2),), jnp.float32),
        "w_out": scatter_about(seeds[5], (D, D), (D // 128) ** -0.5, 2.5, ((0, 2),)),
        "b_out": scatter_about(seeds[6], (D,), 0.5, 3.0, (), jnp.float32),
        "norm1_gain": jnp.clip(1.0 + 0.1 * jax.random.normal(seeds[7], (D,), jnp.float32), 0.5, 1.5),
        "norm1_shift": scatter_about(seeds[8], (D,), 0.5, 3.0, (), jnp.float32),
        "w_up": scatter_about(seeds[9], (D, FF), D ** -0.5, 0.21875, ((1, 2),)),
        "b_up": scatter_about(seeds[10], (FF,), 0.5, 3.0, ((0, 2),), jnp.float32),
        "w_down": scatter_about(seeds[11], (FF, D), FF ** -0.5, 0.109375, ((0, 2),)),
        "b_down": scatter_about(seeds[12], (D,), 0.5, 3.0, (), jnp.float32),
        "norm2_gain": jnp.clip(1.0 + 0.1 * jax.random.normal(seeds[13], (D,), jnp.float32), 0.5, 1.5),
        "norm2_shift": scatter_about(seeds[14], (D,), 0.5, 3.0, (), jnp.float32),
        "grad_out": heavy_noise(seeds[15], (SEQS, LEN, D), 1.0, 6.0, ((0, 8), (1, 2)), (0, 2, 8, 2.0)),
    }


EPSILON = 1e-12
MASKED = -1000000000.0
PRECISE = lax.Precision.HIGHEST

@jax.custom_vjp
def low(v):
    return lax.optimization_barrier(v.astype(jnp.bfloat16)).astype(jnp.float32)

@jax.custom_vjp
def low_back(v):
    return v

def low_keep(v):
    return (low(v), None)

def low_pass(kept, grad):
    return (grad,)

def back_keep(v):
    return (v, None)

def back_low(kept, grad):
    return (low(grad),)
low.defvjp(low_keep, low_pass)
low_back.defvjp(back_keep, back_low)

def layer_norm(hidden, gain, shift):
    center = lax.optimization_barrier(jnp.mean(hidden, axis=-1, keepdims=True))
    offset = hidden - center
    spread = lax.optimization_barrier(jnp.mean(offset * offset, axis=-1, keepdims=True))
    return offset * lax.rsqrt(spread + EPSILON) * gain + shift

def attend_sequence(queries, key_rows, value_rows, seg_row, head_perm):
    split_shape = (N_BLOCK, BLK, H, DH)
    query_blocks = queries.reshape(split_shape)
    key_blocks = key_rows.reshape(split_shape)
    value_blocks = value_rows.reshape(split_shape)
    seg_blocks = seg_row.reshape(N_BLOCK, BLK)
    swapped = (head_perm == 1)[None, None, :, None]
    key_source = jnp.where(swapped, key_blocks[::-1], key_blocks)
    value_source = jnp.where(swapped, value_blocks[::-1], value_blocks)
    key_segs = jnp.where((head_perm == 1)[None, :, None], seg_blocks[::-1][:, None, :], seg_blocks[:, None, :])
    allowed = seg_blocks[:, None, :, None] == key_segs[:, :, None, :]
    scores = low_back(jnp.einsum('bqhd,bkhd->bhqk', query_blocks, key_source, precision=PRECISE) * DH ** (-0.5))
    row_peak = lax.optimization_barrier(jnp.max(jnp.where(allowed, scores, MASKED), axis=-1, keepdims=True))
    weights_exp = jnp.exp(jnp.where(allowed, scores - row_peak, MASKED))
    row_total = lax.optimization_barrier(jnp.sum(weights_exp, axis=-1, keepdims=True))
    probabilities = low(weights_exp / jnp.where(row_total > 0, row_total, 1.0))
    context = jnp.einsum('bhqk,bkhd->bqhd', probabilities, value_source, precision=PRECISE)
    return context.reshape(LEN, H * DH)

def encoder_layer(inputs, segments, head_perm, w_qkv, b_qv, w_out, b_out, gain_first, shift_first, w_up, b_up, w_down, b_down, gain_second, shift_second):
    flat_rows = inputs.reshape(-1, D)
    projected = jnp.einsum('td,dcj->tcj', flat_rows, w_qkv, precision=PRECISE)
    queries = low_back(low(projected[:, 0] + b_qv[0]))
    key_rows = low_back(low(projected[:, 1]))
    value_rows = low_back(low(projected[:, 2] + b_qv[1]))
    seq_shape = (inputs.shape[0], LEN, H, DH)

    def attend_record(record):
        return attend_sequence(record[0], record[1], record[2], record[3], head_perm)
    context = lax.map(jax.checkpoint(attend_record), (queries.reshape(seq_shape), key_rows.reshape(seq_shape), value_rows.reshape(seq_shape), segments))
    context_rows = low_back(low(context.reshape(-1, D)))
    attention = low_back(jnp.dot(context_rows, w_out, precision=PRECISE))
    first_norm = layer_norm(flat_rows + b_out + attention, gain_first, shift_first)
    up_rows = low_back(jnp.dot(low(first_norm), w_up, precision=PRECISE) + b_up)
    activated = low(jax.nn.gelu(up_rows, approximate=False))
    branch = low_back(jnp.dot(activated, w_down, precision=PRECISE))
    result = layer_norm(first_norm + b_down + branch, gain_second, shift_second)
    return result.reshape(inputs.shape)

def reference(tokens, segment_ids, head_perm, w_qkv, b_qv, w_out, b_out, norm1_gain, norm1_shift, w_up, b_up, w_down, b_down, norm2_gain, norm2_shift, grad_out):
    weights = tuple((piece.astype(jnp.float32) for piece in (w_qkv, b_qv, w_out, b_out, norm1_gain, norm1_shift, w_up, b_up, w_down, b_down, norm2_gain, norm2_shift)))
    groups = SEQS // 4
    inputs = tokens.astype(jnp.float32).reshape(groups, 4, LEN, D)
    segments = segment_ids.reshape(groups, 4, LEN)
    cotangents = grad_out.astype(jnp.float32).reshape(groups, 4, LEN, D)

    def step(totals, record):
        group_tokens, group_segs, group_cot = record

        def forward(layer_in, *params):
            return encoder_layer(layer_in, group_segs, head_perm, *params)
        result, pullback = jax.vjp(forward, group_tokens, *weights)
        grads = pullback(group_cot)
        totals = tuple((total + grad for total, grad in zip(totals, grads[1:])))
        return (totals, (result, grads[0]))
    zeros = tuple((jnp.zeros(piece.shape, jnp.float32) for piece in weights))
    totals, (results, grad_inputs) = lax.scan(step, zeros, (inputs, segments, cotangents))
    output = results.reshape(SEQS, LEN, D).astype(jnp.bfloat16)
    grad_tokens = grad_inputs.reshape(SEQS, LEN, D).astype(jnp.bfloat16)
    return (output, grad_tokens, totals[0], totals[1], totals[2], totals[3], totals[4], totals[5], totals[6], totals[7], totals[8], totals[9], totals[10], totals[11])
```

```python
import jax
import jax.numpy as jnp
from jax import lax
from jax.sharding import PartitionSpec as P

EPSILON = 1e-12
MASKED = -1000000000.0


def swapped(value, axis, stride):
    mask = 2**stride
    pairs = [(source, source ^ mask) for source in range(lax.axis_size(axis))]
    return lax.ppermute(value, axis, pairs)


def pair_sum(value, axis):
    total = value.astype(jnp.float32)
    return total + swapped(value, axis, 0).astype(jnp.float32)


def halve(value, axis, bit, dim):
    mine = (lax.axis_index(axis) // 2**bit) % 2
    keep = lax.dynamic_index_in_dim(value, mine, dim, keepdims=False)
    give = lax.dynamic_index_in_dim(value, 1 - mine, dim, keepdims=False)
    got = swapped(give.astype(jnp.bfloat16), axis, bit)
    return keep.astype(jnp.float32) + got.astype(jnp.float32)


def scatter_sum(value, order):
    n_batch, rows, width = value.shape
    bits = n_batch.bit_length() - 1
    live = list(reversed(range(bits)))
    value = value.reshape((2,) * bits + (rows, width))
    gather = False
    for stage in order:
        if stage == "x":
            if live:
                value = value.reshape(value.shape[:-1] + (2, value.shape[-1] // 2))
                value = halve(value, "block", 0, value.ndim - 2)
                gather = True
            else:
                value = pair_sum(value.astype(jnp.bfloat16), "block")
        else:
            value = halve(value, "batch", stage, live.index(stage))
            live.remove(stage)
        if stage != order[-1] or gather:
            value = value.astype(jnp.bfloat16)
    if gather:
        other = swapped(value, "block", 0)
        first = lax.axis_index("block") == 0
        value = jnp.concatenate(
            [jnp.where(first, value, other), jnp.where(first, other, value)], axis=-1
        )
    return value.astype(jnp.float32)


def layer_norm(hidden, gain, shift):
    center = jnp.mean(hidden, axis=-1, keepdims=True)
    offset = hidden - center
    spread = jnp.mean(offset * offset, axis=-1, keepdims=True)
    return offset * lax.rsqrt(spread + EPSILON) * gain + shift


def gelu_exact(hidden):
    return jax.nn.gelu(hidden, approximate=False)


def block_scores(queries, key_rows, score_scale):
    return (
        jnp.einsum("qhd,khd->hqk", queries, key_rows, preferred_element_type=jnp.float32)
        * score_scale
    )


def forward_block(queries, key_rows, value_rows, query_segs, key_segs, score_scale):
    allowed = query_segs[None, :, None] == key_segs[:, None, :]
    scores = block_scores(queries, key_rows, score_scale)
    row_peak = jnp.max(jnp.where(allowed, scores, MASKED), axis=-1, keepdims=True)
    weights_exp = jnp.exp(jnp.where(allowed, scores - row_peak, MASKED))
    row_total = jnp.sum(weights_exp, axis=-1, keepdims=True)
    safe_total = jnp.where(row_total > 0, row_total, 1.0)
    probabilities = weights_exp / safe_total
    context = jnp.einsum(
        "hqk,khd->qhd",
        probabilities.astype(jnp.bfloat16),
        value_rows,
        preferred_element_type=jnp.float32,
    )
    logsum = jnp.where(row_total > 0, row_peak + jnp.log(safe_total), 0.0)
    return (context.astype(jnp.bfloat16), logsum)


def backward_block(
    queries, key_rows, value_rows, query_segs, key_segs, logsum, grad_context, score_scale
):
    allowed = query_segs[None, :, None] == key_segs[:, None, :]
    scores = block_scores(queries, key_rows, score_scale)
    probabilities = jnp.exp(jnp.where(allowed, scores - logsum, MASKED))
    grad_prob = jnp.einsum(
        "qhd,khd->hqk", grad_context, value_rows, preferred_element_type=jnp.float32
    )
    row_delta = jnp.sum(probabilities * grad_prob, axis=-1, keepdims=True)
    grad_scores = (probabilities * (grad_prob - row_delta)).astype(jnp.bfloat16)
    grad_queries = (
        jnp.einsum("hqk,khd->qhd", grad_scores, key_rows, preferred_element_type=jnp.float32)
        * score_scale
    )
    grad_keys = (
        jnp.einsum("hqk,qhd->khd", grad_scores, queries, preferred_element_type=jnp.float32)
        * score_scale
    )
    grad_values = jnp.einsum(
        "hqk,qhd->khd",
        probabilities.astype(jnp.bfloat16),
        grad_context,
        preferred_element_type=jnp.float32,
    )
    return (grad_queries, grad_keys, grad_values)


def local(
    tokens,
    segment_ids,
    head_perm,
    w_qkv,
    b_qv,
    w_out,
    b_out,
    norm1_gain,
    norm1_shift,
    w_up,
    b_up,
    w_down,
    b_down,
    norm2_gain,
    norm2_shift,
    grad_out,
):
    seq_count, block_rows, model_width = tokens.shape
    head_count = head_perm.shape[0]
    local_width = w_qkv.shape[2]
    head_dim = local_width // head_count
    near_heads = head_count // 2
    split_at = near_heads * head_dim
    far_width = local_width - split_at
    score_scale = head_dim ** (-0.5)
    token_count = seq_count * block_rows
    split_shape = (seq_count, block_rows, head_count, head_dim)
    flat_rows = tokens.reshape(token_count, model_width)
    head_order = jnp.argsort(head_perm, stable=True)
    head_undo = jnp.argsort(head_order, stable=True)
    sorted_qkv = jnp.take(
        w_qkv.reshape(model_width, 3, head_count, head_dim), head_order, axis=2
    ).reshape(model_width, 3 * local_width)
    sorted_bias = jnp.take(b_qv.reshape(2, head_count, head_dim), head_order, axis=1).reshape(
        2, local_width
    )
    sorted_out = jnp.take(
        w_out.reshape(head_count, head_dim, model_width), head_order, axis=0
    ).reshape(local_width, model_width)
    projected = jnp.dot(flat_rows, sorted_qkv, preferred_element_type=jnp.float32).reshape(
        token_count, 3, local_width
    )
    queries = (projected[:, 0] + sorted_bias[0]).astype(jnp.bfloat16)
    key_rows = projected[:, 1].astype(jnp.bfloat16)
    value_rows = (projected[:, 2] + sorted_bias[1]).astype(jnp.bfloat16)
    outgoing = jnp.concatenate([key_rows[:, split_at:], value_rows[:, split_at:]], axis=1).reshape(
        seq_count, block_rows, 2 * far_width
    )
    own_block = lax.axis_index("block")
    own_segs = lax.dynamic_slice_in_dim(segment_ids, own_block * block_rows, block_rows, 1)
    other_segs = lax.dynamic_slice_in_dim(segment_ids, (1 - own_block) * block_rows, block_rows, 1)
    key_segs = jnp.concatenate(
        [
            jnp.broadcast_to(own_segs[:, None, :], (seq_count, near_heads, block_rows)),
            jnp.broadcast_to(
                other_segs[:, None, :], (seq_count, head_count - near_heads, block_rows)
            ),
        ],
        axis=1,
    )
    partner = swapped(outgoing, "block", 0).reshape(token_count, 2 * far_width)
    all_keys = jnp.concatenate([key_rows[:, :split_at], partner[:, :far_width]], axis=1)
    all_values = jnp.concatenate([value_rows[:, :split_at], partner[:, far_width:]], axis=1)
    keys_full = all_keys.reshape(split_shape)
    values_full = all_values.reshape(split_shape)
    query_blocks = queries.reshape(split_shape)

    def forward_record(record):
        return forward_block(record[0], record[1], record[2], record[3], record[4], score_scale)

    context, logsum = lax.map(
        forward_record, (query_blocks, keys_full, values_full, own_segs, key_segs)
    )
    context_rows = context.reshape(token_count, local_width)
    attention = pair_sum(
        jnp.dot(context_rows, sorted_out, preferred_element_type=jnp.float32).astype(jnp.bfloat16),
        "tensor",
    )
    first_sum = flat_rows.astype(jnp.float32) + b_out + attention
    first_norm, first_back = jax.vjp(layer_norm, first_sum, norm1_gain, norm1_shift)
    first_low = first_norm.astype(jnp.bfloat16)
    up_rows = jnp.dot(first_low, w_up, preferred_element_type=jnp.float32) + b_up
    activated, gelu_back = jax.vjp(gelu_exact, up_rows)
    activated_low = activated.astype(jnp.bfloat16)
    branch = pair_sum(
        jnp.dot(activated_low, w_down, preferred_element_type=jnp.float32).astype(jnp.bfloat16),
        "tensor",
    )
    second_sum = first_norm + b_down + branch
    result, second_back = jax.vjp(layer_norm, second_sum, norm2_gain, norm2_shift)
    grad_second, grad_gain2, grad_shift2 = second_back(
        grad_out.reshape(token_count, model_width).astype(jnp.float32)
    )
    grad_second_low = grad_second.astype(jnp.bfloat16)
    grad_b_down = jnp.sum(grad_second, axis=0)
    grad_w_down = jnp.dot(grad_second_low.T, activated_low, preferred_element_type=jnp.float32)
    n_batch = lax.axis_size("batch")
    bits = tuple(range(n_batch.bit_length() - 1))
    y_last = ("x",) + bits[1:] + bits[:1]
    x_last = bits + ("x",)
    part_rows = model_width // n_batch
    final_w_down = scatter_sum(grad_w_down.reshape(n_batch, part_rows, -1), y_last).T
    (grad_up,) = gelu_back(jnp.dot(grad_second_low, w_down.T, preferred_element_type=jnp.float32))
    grad_up_low = grad_up.astype(jnp.bfloat16)
    grad_b_up = jnp.sum(grad_up_low.astype(jnp.float32), axis=0)
    grad_w_up = jnp.dot(first_low.T, grad_up_low, preferred_element_type=jnp.float32)
    final_w_up = scatter_sum(grad_w_up.reshape(n_batch, part_rows, -1), x_last)
    grad_first = grad_second + pair_sum(
        jnp.dot(grad_up_low, w_up.T, preferred_element_type=jnp.float32).astype(jnp.bfloat16),
        "tensor",
    )
    grad_middle, grad_gain1, grad_shift1 = first_back(grad_first)
    grad_middle_low = grad_middle.astype(jnp.bfloat16)
    grad_b_out = jnp.sum(grad_middle, axis=0)
    grad_out_sorted = jnp.dot(grad_middle_low.T, context_rows, preferred_element_type=jnp.float32)
    grad_context = (
        jnp.dot(grad_middle_low, sorted_out.T, preferred_element_type=jnp.float32)
        .astype(jnp.bfloat16)
        .reshape(split_shape)
    )
    back_keys, back_values = (keys_full, values_full)

    def backward_record(record):
        return backward_block(
            record[0], record[1], record[2], record[3], record[4], record[5], record[6], score_scale
        )

    grad_query, grad_key, grad_value = lax.map(
        backward_record,
        (query_blocks, back_keys, back_values, own_segs, key_segs, logsum, grad_context),
    )
    grad_query_low = grad_query.astype(jnp.bfloat16).reshape(token_count, local_width)
    grad_key_low = grad_key.astype(jnp.bfloat16).reshape(token_count, local_width)
    grad_value_low = grad_value.astype(jnp.bfloat16).reshape(token_count, local_width)
    returning = jnp.concatenate(
        [grad_key_low[:, split_at:], grad_value_low[:, split_at:]], axis=1
    ).reshape(seq_count, block_rows, 2 * far_width)
    returned = swapped(returning, "block", 0).reshape(token_count, 2 * far_width)
    grad_key_all = jnp.concatenate([grad_key_low[:, :split_at], returned[:, :far_width]], axis=1)
    grad_value_all = jnp.concatenate(
        [grad_value_low[:, :split_at], returned[:, far_width:]], axis=1
    )
    grad_qkv = jnp.stack([grad_query_low, grad_key_all, grad_value_all], axis=1).reshape(
        token_count, 3 * local_width
    )
    grad_qkv_sorted = jnp.dot(flat_rows.T, grad_qkv, preferred_element_type=jnp.float32)
    grad_bias_sorted = jnp.stack(
        [
            jnp.sum(grad_query_low.astype(jnp.float32), axis=0),
            jnp.sum(grad_value_all.astype(jnp.float32), axis=0),
        ]
    )
    grad_input = grad_middle + pair_sum(
        jnp.dot(grad_qkv, sorted_qkv.T, preferred_element_type=jnp.float32).astype(jnp.bfloat16),
        "tensor",
    )
    grad_w_qkv = jnp.take(
        grad_qkv_sorted.reshape(model_width, 3, head_count, head_dim), head_undo, axis=2
    ).reshape(model_width, 3, local_width)
    grad_b_qv = jnp.take(
        grad_bias_sorted.reshape(2, head_count, head_dim), head_undo, axis=1
    ).reshape(2, local_width)
    grad_w_out = jnp.take(
        grad_out_sorted.reshape(model_width, head_count, head_dim), head_undo, axis=1
    ).reshape(model_width, local_width)
    by_place = grad_w_qkv.reshape(n_batch, part_rows, 3, local_width)
    first_part = scatter_sum(by_place[:, :, :2].reshape(n_batch, part_rows, -1), y_last)
    second_part = scatter_sum(
        jnp.concatenate(
            [by_place[:, :, 2], grad_w_out.reshape(n_batch, part_rows, local_width)], axis=2
        ),
        x_last,
    )
    final_w_qkv = jnp.concatenate([first_part, second_part[:, :local_width]], axis=1).reshape(
        part_rows, 3, local_width
    )
    final_w_out = second_part[:, local_width:].T
    small = [
        grad_b_qv[0],
        grad_b_qv[1],
        grad_b_out,
        grad_gain1,
        grad_shift1,
        grad_b_up,
        grad_b_down,
        grad_gain2,
        grad_shift2,
    ]
    joined = jnp.concatenate([piece.reshape(n_batch, -1) for piece in small], axis=1)
    total = scatter_sum(joined[:, None, :], x_last)[0]
    ends, at = [], 0
    for piece in small:
        ends.append(total[at : at + piece.size // n_batch])
        at += piece.size // n_batch
    (bq, bv, final_b_out, final_gain1, final_shift1, final_b_up, final_b_down) = ends[:7]
    final_gain2, final_shift2 = ends[7:]
    final_b_qv = jnp.stack([bq, bv])
    output = result.astype(jnp.bfloat16).reshape(seq_count, block_rows, model_width)
    grad_tokens = grad_input.astype(jnp.bfloat16).reshape(seq_count, block_rows, model_width)
    return (
        output,
        grad_tokens,
        final_w_qkv,
        final_b_qv,
        final_w_out,
        final_b_out,
        final_gain1,
        final_shift1,
        final_w_up,
        final_b_up,
        final_w_down,
        final_b_down,
        final_gain2,
        final_shift2,
    )


def solution(mesh):
    placed = (
        P("batch", "block", None),
        P("batch", None),
        P("tensor"),
        P(None, None, "tensor"),
        P(None, "tensor"),
        P("tensor", None),
        P(),
        P(),
        P(),
        P(None, "tensor"),
        P("tensor"),
        P("tensor", None),
        P(),
        P(),
        P(),
        P("batch", "block", None),
    )
    return jax.shard_map(
        local,
        mesh=mesh,
        in_specs=placed,
        out_specs=(
            P("batch", "block", None),
            P("batch", "block", None),
            P("batch", None, "tensor"),
            P(None, ("tensor", "batch")),
            P("tensor", "batch"),
            P("batch"),
            P("batch"),
            P("batch"),
            P("batch", "tensor"),
            P(("tensor", "batch")),
            P("tensor", "batch"),
            P("batch"),
            P("batch"),
            P("batch"),
        ),
        check_vma=False,
    )
```

```python
import jax
import jax.numpy as jnp
from jax import lax
from jax.experimental import pallas as pl
from jax.experimental.pallas import tpu as pltpu
from jax.sharding import PartitionSpec as P

EPSILON = 1e-12
MASKED = -1000000000.0


def swapped(value, axis, stride):
    mask = 2**stride
    pairs = [(source, source ^ mask) for source in range(lax.axis_size(axis))]
    return lax.ppermute(value, axis, pairs)


def pair_sum(value, axis):
    total = value.astype(jnp.float32)
    return total + swapped(value, axis, 0).astype(jnp.float32)


def halve(value, axis, bit, dim):
    mine = (lax.axis_index(axis) // 2**bit) % 2
    keep = lax.dynamic_index_in_dim(value, mine, dim, keepdims=False)
    give = lax.dynamic_index_in_dim(value, 1 - mine, dim, keepdims=False)
    got = swapped(give.astype(jnp.bfloat16), axis, bit)
    return keep.astype(jnp.float32) + got.astype(jnp.float32)


def scatter_sum(value, order):
    n_batch, rows, width = value.shape
    bits = n_batch.bit_length() - 1
    live = list(reversed(range(bits)))
    value = value.reshape((2,) * bits + (rows, width))
    gather = False
    for stage in order:
        if stage == "x":
            if live:
                value = value.reshape(value.shape[:-1] + (2, value.shape[-1] // 2))
                value = halve(value, "block", 0, value.ndim - 2)
                gather = True
            else:
                value = pair_sum(value.astype(jnp.bfloat16), "block")
        else:
            value = halve(value, "batch", stage, live.index(stage))
            live.remove(stage)
        if stage != order[-1] or gather:
            value = value.astype(jnp.bfloat16)
    if gather:
        other = swapped(value, "block", 0)
        first = lax.axis_index("block") == 0
        value = jnp.concatenate(
            [jnp.where(first, value, other), jnp.where(first, other, value)], axis=-1
        )
    return value.astype(jnp.float32)


def layer_norm(hidden, gain, shift):
    center = jnp.mean(hidden, axis=-1, keepdims=True)
    offset = hidden - center
    spread = jnp.mean(offset * offset, axis=-1, keepdims=True)
    return offset * lax.rsqrt(spread + EPSILON) * gain + shift


def gelu_exact(hidden):
    return jax.nn.gelu(hidden, approximate=False)


def block_scores(queries, key_rows, score_scale):
    return (
        jnp.einsum("qhd,khd->hqk", queries, key_rows, preferred_element_type=jnp.float32)
        * score_scale
    )


def forward_block(queries, key_rows, value_rows, query_segs, key_segs, score_scale):
    allowed = query_segs[None, :, None] == key_segs[:, None, :]
    scores = block_scores(queries, key_rows, score_scale)
    row_peak = jnp.max(jnp.where(allowed, scores, MASKED), axis=-1, keepdims=True)
    weights_exp = jnp.exp(jnp.where(allowed, scores - row_peak, MASKED))
    row_total = jnp.sum(weights_exp, axis=-1, keepdims=True)
    safe_total = jnp.where(row_total > 0, row_total, 1.0)
    probabilities = weights_exp / safe_total
    context = jnp.einsum(
        "hqk,khd->qhd",
        probabilities.astype(jnp.bfloat16),
        value_rows,
        preferred_element_type=jnp.float32,
    )
    logsum = jnp.where(row_total > 0, row_peak + jnp.log(safe_total), 0.0)
    return (context.astype(jnp.bfloat16), logsum)


def backward_block(
    queries, key_rows, value_rows, query_segs, key_segs, logsum, grad_context, score_scale
):
    allowed = query_segs[None, :, None] == key_segs[:, None, :]
    scores = block_scores(queries, key_rows, score_scale)
    probabilities = jnp.exp(jnp.where(allowed, scores - logsum, MASKED))
    grad_prob = jnp.einsum(
        "qhd,khd->hqk", grad_context, value_rows, preferred_element_type=jnp.float32
    )
    row_delta = jnp.sum(probabilities * grad_prob, axis=-1, keepdims=True)
    grad_scores = (probabilities * (grad_prob - row_delta)).astype(jnp.bfloat16)
    grad_queries = (
        jnp.einsum("hqk,khd->qhd", grad_scores, key_rows, preferred_element_type=jnp.float32)
        * score_scale
    )
    grad_keys = (
        jnp.einsum("hqk,qhd->khd", grad_scores, queries, preferred_element_type=jnp.float32)
        * score_scale
    )
    grad_values = jnp.einsum(
        "hqk,qhd->khd",
        probabilities.astype(jnp.bfloat16),
        grad_context,
        preferred_element_type=jnp.float32,
    )
    return (grad_queries, grad_keys, grad_values)


def local(
    tokens,
    segment_ids,
    head_perm,
    w_qkv,
    b_qv,
    w_out,
    b_out,
    norm1_gain,
    norm1_shift,
    w_up,
    b_up,
    w_down,
    b_down,
    norm2_gain,
    norm2_shift,
    grad_out,
):
    seq_count, block_rows, model_width = tokens.shape
    head_count = head_perm.shape[0]
    local_width = w_qkv.shape[2]
    head_dim = local_width // head_count
    near_heads = head_count // 2
    split_at = near_heads * head_dim
    far_width = local_width - split_at
    score_scale = head_dim ** (-0.5)
    token_count = seq_count * block_rows
    split_shape = (seq_count, block_rows, head_count, head_dim)
    flat_rows = tokens.reshape(token_count, model_width)
    head_order = jnp.argsort(head_perm, stable=True)
    head_undo = jnp.argsort(head_order, stable=True)
    sorted_qkv = jnp.take(
        w_qkv.reshape(model_width, 3, head_count, head_dim), head_order, axis=2
    ).reshape(model_width, 3 * local_width)
    sorted_bias = jnp.take(b_qv.reshape(2, head_count, head_dim), head_order, axis=1).reshape(
        2, local_width
    )
    sorted_out = jnp.take(
        w_out.reshape(head_count, head_dim, model_width), head_order, axis=0
    ).reshape(local_width, model_width)
    projected = jnp.dot(flat_rows, sorted_qkv, preferred_element_type=jnp.float32).reshape(
        token_count, 3, local_width
    )
    queries = (projected[:, 0] + sorted_bias[0]).astype(jnp.bfloat16)
    key_rows = projected[:, 1].astype(jnp.bfloat16)
    value_rows = (projected[:, 2] + sorted_bias[1]).astype(jnp.bfloat16)
    outgoing = jnp.concatenate([key_rows[:, split_at:], value_rows[:, split_at:]], axis=1).reshape(
        seq_count, block_rows, 2 * far_width
    )
    own_block = lax.axis_index("block")
    own_segs = lax.dynamic_slice_in_dim(segment_ids, own_block * block_rows, block_rows, 1)
    other_segs = lax.dynamic_slice_in_dim(segment_ids, (1 - own_block) * block_rows, block_rows, 1)
    key_segs = jnp.concatenate(
        [
            jnp.broadcast_to(own_segs[:, None, :], (seq_count, near_heads, block_rows)),
            jnp.broadcast_to(
                other_segs[:, None, :], (seq_count, head_count - near_heads, block_rows)
            ),
        ],
        axis=1,
    )
    partner = swapped(outgoing, "block", 0).reshape(token_count, 2 * far_width)
    all_keys = jnp.concatenate([key_rows[:, :split_at], partner[:, :far_width]], axis=1)
    all_values = jnp.concatenate([value_rows[:, :split_at], partner[:, far_width:]], axis=1)
    keys_full = all_keys.reshape(split_shape)
    values_full = all_values.reshape(split_shape)
    query_blocks = queries.reshape(split_shape)

    def forward_record(record):
        return forward_block(record[0], record[1], record[2], record[3], record[4], score_scale)

    context, logsum = lax.map(
        forward_record, (query_blocks, keys_full, values_full, own_segs, key_segs)
    )
    context_rows = context.reshape(token_count, local_width)
    attention = pair_sum(
        jnp.dot(context_rows, sorted_out, preferred_element_type=jnp.float32).astype(jnp.bfloat16),
        "tensor",
    )
    first_sum = flat_rows.astype(jnp.float32) + b_out + attention
    first_norm, first_back = jax.vjp(layer_norm, first_sum, norm1_gain, norm1_shift)
    first_low = first_norm.astype(jnp.bfloat16)
    up_rows = jnp.dot(first_low, w_up, preferred_element_type=jnp.float32) + b_up
    activated, gelu_back = jax.vjp(gelu_exact, up_rows)
    activated_low = activated.astype(jnp.bfloat16)
    branch = pair_sum(
        jnp.dot(activated_low, w_down, preferred_element_type=jnp.float32).astype(jnp.bfloat16),
        "tensor",
    )
    second_sum = first_norm + b_down + branch
    result, second_back = jax.vjp(layer_norm, second_sum, norm2_gain, norm2_shift)
    grad_second, grad_gain2, grad_shift2 = second_back(
        grad_out.reshape(token_count, model_width).astype(jnp.float32)
    )
    grad_second_low = grad_second.astype(jnp.bfloat16)
    grad_b_down = jnp.sum(grad_second, axis=0)
    grad_w_down = jnp.dot(grad_second_low.T, activated_low, preferred_element_type=jnp.float32)
    n_batch = lax.axis_size("batch")
    bits = tuple(range(n_batch.bit_length() - 1))
    y_last = ("x",) + bits[1:] + bits[:1]
    x_last = bits + ("x",)
    part_rows = model_width // n_batch
    final_w_down = scatter_sum(grad_w_down.reshape(n_batch, part_rows, -1), y_last).T
    (grad_up,) = gelu_back(jnp.dot(grad_second_low, w_down.T, preferred_element_type=jnp.float32))
    grad_up_low = grad_up.astype(jnp.bfloat16)
    grad_b_up = jnp.sum(grad_up_low.astype(jnp.float32), axis=0)
    grad_w_up = jnp.dot(first_low.T, grad_up_low, preferred_element_type=jnp.float32)
    final_w_up = scatter_sum(grad_w_up.reshape(n_batch, part_rows, -1), x_last)
    grad_first = grad_second + pair_sum(
        jnp.dot(grad_up_low, w_up.T, preferred_element_type=jnp.float32).astype(jnp.bfloat16),
        "tensor",
    )
    grad_middle, grad_gain1, grad_shift1 = first_back(grad_first)
    grad_middle_low = grad_middle.astype(jnp.bfloat16)
    grad_b_out = jnp.sum(grad_middle, axis=0)
    grad_out_sorted = jnp.dot(grad_middle_low.T, context_rows, preferred_element_type=jnp.float32)
    grad_context = (
        jnp.dot(grad_middle_low, sorted_out.T, preferred_element_type=jnp.float32)
        .astype(jnp.bfloat16)
        .reshape(split_shape)
    )
    back_keys, back_values = (keys_full, values_full)

    def backward_record(record):
        return backward_block(
            record[0], record[1], record[2], record[3], record[4], record[5], record[6], score_scale
        )

    grad_query, grad_key, grad_value = lax.map(
        backward_record,
        (query_blocks, back_keys, back_values, own_segs, key_segs, logsum, grad_context),
    )
    grad_query_low = grad_query.astype(jnp.bfloat16).reshape(token_count, local_width)
    grad_key_low = grad_key.astype(jnp.bfloat16).reshape(token_count, local_width)
    grad_value_low = grad_value.astype(jnp.bfloat16).reshape(token_count, local_width)
    returning = jnp.concatenate(
        [grad_key_low[:, split_at:], grad_value_low[:, split_at:]], axis=1
    ).reshape(seq_count, block_rows, 2 * far_width)
    returned = swapped(returning, "block", 0).reshape(token_count, 2 * far_width)
    grad_key_all = jnp.concatenate([grad_key_low[:, :split_at], returned[:, :far_width]], axis=1)
    grad_value_all = jnp.concatenate(
        [grad_value_low[:, :split_at], returned[:, far_width:]], axis=1
    )
    grad_qkv = jnp.stack([grad_query_low, grad_key_all, grad_value_all], axis=1).reshape(
        token_count, 3 * local_width
    )
    grad_qkv_sorted = jnp.dot(flat_rows.T, grad_qkv, preferred_element_type=jnp.float32)
    grad_bias_sorted = jnp.stack(
        [
            jnp.sum(grad_query_low.astype(jnp.float32), axis=0),
            jnp.sum(grad_value_all.astype(jnp.float32), axis=0),
        ]
    )
    grad_input = grad_middle + pair_sum(
        jnp.dot(grad_qkv, sorted_qkv.T, preferred_element_type=jnp.float32).astype(jnp.bfloat16),
        "tensor",
    )
    grad_w_qkv = jnp.take(
        grad_qkv_sorted.reshape(model_width, 3, head_count, head_dim), head_undo, axis=2
    ).reshape(model_width, 3, local_width)
    grad_b_qv = jnp.take(
        grad_bias_sorted.reshape(2, head_count, head_dim), head_undo, axis=1
    ).reshape(2, local_width)
    grad_w_out = jnp.take(
        grad_out_sorted.reshape(model_width, head_count, head_dim), head_undo, axis=1
    ).reshape(model_width, local_width)
    by_place = grad_w_qkv.reshape(n_batch, part_rows, 3, local_width)
    first_part = scatter_sum(by_place[:, :, :2].reshape(n_batch, part_rows, -1), y_last)
    second_part = scatter_sum(
        jnp.concatenate(
            [by_place[:, :, 2], grad_w_out.reshape(n_batch, part_rows, local_width)], axis=2
        ),
        x_last,
    )
    final_w_qkv = jnp.concatenate([first_part, second_part[:, :local_width]], axis=1).reshape(
        part_rows, 3, local_width
    )
    final_w_out = second_part[:, local_width:].T
    small = [
        grad_b_qv[0],
        grad_b_qv[1],
        grad_b_out,
        grad_gain1,
        grad_shift1,
        grad_b_up,
        grad_b_down,
        grad_gain2,
        grad_shift2,
    ]
    joined = jnp.concatenate([piece.reshape(n_batch, -1) for piece in small], axis=1)
    total = scatter_sum(joined[:, None, :], x_last)[0]
    ends, at = [], 0
    for piece in small:
        ends.append(total[at : at + piece.size // n_batch])
        at += piece.size // n_batch
    (bq, bv, final_b_out, final_gain1, final_shift1, final_b_up, final_b_down) = ends[:7]
    final_gain2, final_shift2 = ends[7:]
    final_b_qv = jnp.stack([bq, bv])
    output = result.astype(jnp.bfloat16).reshape(seq_count, block_rows, model_width)
    grad_tokens = grad_input.astype(jnp.bfloat16).reshape(seq_count, block_rows, model_width)
    return (
        output,
        grad_tokens,
        final_w_qkv,
        final_b_qv,
        final_w_out,
        final_b_out,
        final_gain1,
        final_shift1,
        final_w_up,
        final_b_up,
        final_w_down,
        final_b_down,
        final_gain2,
        final_shift2,
    )


F32 = jnp.float32
BF16 = jnp.bfloat16
MESH = pl.DeviceIdType.MESH
ROOT_HALF = 0.7071067811865476
DENSITY = 0.3989422804014327


def nn(left, right):
    return jnp.dot(left, right, preferred_element_type=F32)


def nt(left, right):
    return lax.dot_general(left, right, (((1,), (1,)), ((), ())), preferred_element_type=F32)


def loop(count, start=0):
    def run(body):
        def step(index, carry):
            body(index)
            return carry

        lax.fori_loop(start, start + count, step, 0)

    return run


def row(value, step, size):
    return pl.ds(pl.multiple_of(value * step, step), size)


def fold_rows(value):
    return jnp.sum(value.reshape(value.shape[0] // 8, 8, value.shape[1]), axis=0)


def layer_kernel(
    x,
    seg,
    perm,
    b_qv,
    b_out,
    gain1,
    shift1,
    b_up,
    b_down,
    gain2,
    shift2,
    h_wqkv,
    h_wout,
    h_wup,
    h_wdown,
    h_gout,
    out,
    gtok,
    o_down,
    o_up,
    o_qk,
    o_vo,
    o_small,
    wqkv,
    wout,
    wup,
    wdown,
    gout,
    heads_t,
    kv_send,
    kv_recv,
    kv_near,
    q_slots,
    ctx_t,
    ctx,
    lse,
    seg_col,
    ex_send,
    ex_recv,
    a1,
    a1_t,
    n1,
    r1,
    act,
    slope,
    dz,
    dz2,
    dz_t,
    du,
    dctx_t,
    dctx_s,
    dq_t,
    dkv_t,
    dkv_send,
    dqkv,
    x_t,
    part,
    ra1,
    ra2,
    ra3,
    ra4,
    ra5,
    fin,
    rb1,
    rb2,
    rb3,
    rb4,
    fin_b,
    acc,
    acc_up,
    acc_qv,
    sm_send,
    sm_recv,
    load_sem,
    kv_ss,
    kv_rs,
    dkv_ss,
    dkv_rs,
    ex_ss,
    ex_rs,
    a_ss,
    a_rs,
    b_ss,
    b_rs,
    s_ss,
    s_rs,
):
    tokens = x.shape[0]
    width = x.shape[1]
    local = wout.shape[0]
    hidden = wup.shape[1]
    n_heads = perm.shape[0]
    dim = local // n_heads
    near = n_heads // 2
    span = near * dim
    scale = dim ** (-0.5)
    rows = part.shape[4]
    half = rows // 2

    me_b = lax.axis_index("batch")
    bx = lax.axis_index("block")
    tc = lax.axis_index("tensor")
    yi = lax.rem(me_b, 2)
    zl = lax.rem(me_b // 2, 2)
    zh = me_b // 4
    to_core = {"tensor": 1 - tc}
    to_x = {"block": 1 - bx}
    to_y = {"batch": me_b + 1 - 2 * yi}
    to_z1 = {"batch": me_b + 2 - 4 * zl}
    to_z2 = {"batch": me_b + 4 - 8 * zh}

    def remote(src, dst, send, recv, where):
        return pltpu.make_async_remote_copy(
            src_ref=src,
            dst_ref=dst,
            send_sem=send,
            recv_sem=recv,
            device_id=where,
            device_id_type=MESH,
        )

    loads = [
        pltpu.make_async_copy(h_wqkv, wqkv, load_sem.at[0]),
        pltpu.make_async_copy(h_wout, wout, load_sem.at[1]),
        pltpu.make_async_copy(h_wup, wup, load_sem.at[2]),
        pltpu.make_async_copy(h_wdown, wdown, load_sem.at[3]),
        pltpu.make_async_copy(h_gout, gout, load_sem.at[4]),
    ]
    for copy in loads:
        copy.start()

    barrier = pltpu.get_barrier_semaphore()
    for where in (to_core, to_x, to_y, to_z1, to_z2):
        pl.semaphore_signal(barrier, inc=1, device_id=where, device_id_type=MESH)

    far = [perm[h] for h in range(n_heads)]
    far_rank, near_rank = [], []
    f_count, n_count = jnp.int32(0), jnp.int32(0)
    for h in range(n_heads):
        far_rank.append(f_count)
        near_rank.append(n_count)
        f_count = f_count + far[h]
        n_count = n_count + (1 - far[h])
    rank = [far[h] * far_rank[h] + (1 - far[h]) * near_rank[h] for h in range(n_heads)]

    held = [
        [[(far[h] == g) & (rank[h] == j) for h in range(n_heads)] for j in range(near)]
        for g in range(2)
    ]

    def pick(g, j, bands):
        value = bands(j)
        for h in range(j + 1, j + 1 + n_heads - near):
            value = jnp.where(held[g][j][h], bands(h), value)
        return value

    def unpick(h, bands):
        value = None
        for g in range(2):
            for j in range(max(0, h - (n_heads - near)), min(h, near - 1) + 1):
                band = bands(g, j)
                value = band if value is None else jnp.where(held[g][j][h], band, value)
        return value

    def turned(which):
        return lambda h: heads_t[which, h * dim : (h + 1) * dim, :]

    for g in range(2):
        block = bx if g == 0 else 1 - bx
        line = seg[:, row(block, tokens, tokens)].astype(F32)
        seg_col[g] = jnp.broadcast_to(line, (128, tokens)).T

    loads[0].wait()
    pl.semaphore_wait(barrier, 5)

    for which in (1, 2, 0):
        bias = None if which == 1 else b_qv[0 if which == 0 else 1 : (0 if which == 0 else 1) + 1, :]

        @loop(2)
        def _(blk, which=which, bias=bias):
            value = nn(x[row(blk, tokens // 2, tokens // 2), :], wqkv[which])
            if bias is not None:
                value = value + bias
            heads_t[which, :, row(blk, tokens // 2, tokens // 2)] = value.astype(BF16).T

        if which == 2:

            for j in range(near):
                kv_send[j * dim : (j + 1) * dim, :] = pick(1, j, turned(1))
                kv_send[span + j * dim : span + (j + 1) * dim, :] = pick(1, j, turned(2))

            kv_copy = remote(kv_send, kv_recv, kv_ss, kv_rs, to_x)
            kv_copy.start()

    q_tile = tokens // 2
    for j in range(near):
        kv_near[j * dim : (j + 1) * dim, :] = pick(0, j, turned(1))
        kv_near[span + j * dim : span + (j + 1) * dim, :] = pick(0, j, turned(2))
        for g in range(2):
            q_slots[g * span + j * dim : g * span + (j + 1) * dim, :] = pick(g, j, turned(0))

    def head_bands(g, j):
        source = kv_recv if g else kv_near
        return (
            q_slots[row(g * near + j, dim, dim), :],
            source[row(j, dim, dim), :],
            source[row(j + near, dim, dim), :],
        )

    def allowed_of(g, t):
        key_side = jnp.concatenate([seg_col[g]] * (q_tile // 128), axis=1)
        query_side = seg[:, row(2 * bx + t, q_tile, q_tile)].astype(F32)
        return key_side == query_side

    def attend(g):
        @loop(near)
        def _(j):
            q_band, k_band, v_band = head_bands(g, j)
            keys = k_band.T
            for t in range(2):
                cols = slice(t * q_tile, (t + 1) * q_tile)
                scores = nn(keys, q_band[:, cols]) * scale
                allowed = allowed_of(g, t)
                peak = jnp.max(jnp.where(allowed, scores, MASKED), axis=0, keepdims=True)
                weights = jnp.exp(jnp.where(allowed, scores - peak, MASKED))
                total = jnp.sum(weights, axis=0, keepdims=True)
                safe = jnp.where(total > 0, total, 1.0)
                probs = (weights * (1.0 / safe)).astype(BF16)
                band = row(g * near + j, dim, dim)
                ctx_t[band, cols] = nn(v_band, probs).astype(BF16)
                lse[pl.ds(g * near + j, 1), cols] = jnp.where(total > 0, peak + jnp.log(safe), 0.0)

    attend(0)
    kv_copy.wait()
    attend(1)

    for h in range(n_heads):
        band = unpick(h, lambda g, j: ctx_t[(g * near + j) * dim : (g * near + j + 1) * dim, :])
        ctx[:, h * dim : (h + 1) * dim] = band.T

    r_tile = tokens // 2

    def exchange(index, blk):
        area = pl.ds(blk * r_tile, r_tile)
        return remote(
            ex_send.at[index, area],
            ex_recv.at[index, area],
            ex_ss.at[index, blk],
            ex_rs.at[index, blk],
            to_core,
        )

    def both(index, area):
        return ex_send[index, area, :].astype(F32) + ex_recv[index, area, :].astype(F32)

    loads[1].wait()
    for blk in range(2):
        area = pl.ds(blk * r_tile, r_tile)
        ex_send[0, area, :] = nn(ctx[area, :], wout[...]).astype(BF16)
        exchange(0, blk).start()

    sub = 128

    def norm(value):
        center = jnp.mean(value, axis=-1, keepdims=True)
        offset = value - center
        spread = jnp.mean(offset * offset, axis=-1, keepdims=True)
        inverse = lax.rsqrt(spread + EPSILON)
        return offset * inverse, inverse

    for blk in range(2):
        exchange(0, blk).wait()

        @loop(r_tile // sub, start=blk * (r_tile // sub))
        def _(i):
            area = row(i, sub, sub)
            value = x[area, :].astype(F32) + b_out[...] + both(0, area)
            normal, inverse = norm(value)
            n1[area, :] = normal
            r1[area, :] = jnp.broadcast_to(inverse, (sub, 128))
            low = (normal * gain1[...] + shift1[...]).astype(BF16)
            a1[area, :] = low
            a1_t[:, area] = low.T

    loads[2].wait()
    f_tile = 256

    @loop(hidden // f_tile)
    def _(i):
        cols = row(i, f_tile, f_tile)
        for blk in range(2):
            area = pl.ds(blk * r_tile, r_tile)
            up = nn(a1[area, :], wup[:, cols]) + b_up[:, cols]
            below = 0.5 + 0.5 * lax.erf(up * ROOT_HALF)
            act[area, cols] = (up * below).astype(BF16)
            slope[area, cols] = below + up * (DENSITY * jnp.exp(-0.5 * up * up))

    loads[3].wait()
    for blk in range(2):
        area = pl.ds(blk * r_tile, r_tile)
        ex_send[1, area, :] = nn(act[area, :], wdown[...]).astype(BF16)
        exchange(1, blk).start()

    acc[...] = jnp.zeros_like(acc)
    loads[4].wait()
    for blk in range(2):
        exchange(1, blk).wait()

        @loop(r_tile // sub, start=blk * (r_tile // sub))
        def _(i):
            area = row(i, sub, sub)
            first = n1[area, :] * gain1[...] + shift1[...]
            value = first + b_down[...] + both(1, area)
            normal, inverse = norm(value)
            out[area, :] = (normal * gain2[...] + shift2[...]).astype(BF16)
            up = gout[area, :].astype(F32)
            acc[0] += fold_rows(up)
            acc[1] += fold_rows(up * normal)
            scaled = up * gain2[...]
            mean_r = jnp.mean(scaled, axis=-1, keepdims=True)
            mean_rn = jnp.mean(scaled * normal, axis=-1, keepdims=True)
            down = (scaled - mean_r - normal * mean_rn) * inverse
            acc[2] += fold_rows(down)
            dz[area, :] = down
            low = down.astype(BF16)
            dz2[area, :] = low
            dz_t[:, area] = low.T

    def a_copy(i, chain, k):
        mine, other = row(bx, half, half), row(1 - bx, half, half)
        src, dst, where = (
            lambda: (part.at[chain, :, :, :, other, :], ra1.at[i], to_x),
            lambda: (part.at[chain, :, 1 - zl, :, mine, :], ra2.at[i], to_z1),
            lambda: (part.at[chain, 1 - zh, zl, :, mine, :], ra3.at[i], to_z2),
            lambda: (part.at[chain, zh, zl, 1 - yi, mine, :], ra4.at[i], to_y),
            lambda: (fin.at[i], ra5.at[i], to_x),
        )[k]()
        return remote(src, dst, a_ss.at[i, k], a_rs.at[i, k], where)

    def b_copy(i, chain, k):
        src, dst, where = (
            lambda: (part.at[chain, :, :, 1 - yi], rb1.at[i], to_y),
            lambda: (part.at[chain, :, 1 - zl, yi], rb2.at[i], to_z1),
            lambda: (part.at[chain, 1 - zh, zl, yi], rb3.at[i], to_z2),
            lambda: (fin_b.at[i], rb4.at[i], to_x),
        )[k]()
        return remote(src, dst, b_ss.at[i, k], b_rs.at[i, k], where)

    def plus(left, right):
        return left.astype(F32) + right.astype(F32)

    def a_step(i, chain, k, target):
        a_copy(i, chain, k).wait()
        mine, other = row(bx, half, half), row(1 - bx, half, half)
        if k == 0:

            @loop(8)
            def _(d):
                a, b, c = d // 4, lax.rem(d // 2, 2), lax.rem(d, 2)
                part[chain, a, b, c, mine, :] = plus(
                    part[chain, a, b, c, mine, :], ra1[i, a, b, c]
                ).astype(BF16)
        elif k == 1:

            @loop(4)
            def _(d):
                a, c = d // 2, lax.rem(d, 2)
                part[chain, a, zl, c, mine, :] = plus(
                    part[chain, a, zl, c, mine, :], ra2[i, a, c]
                ).astype(BF16)
        elif k == 2:

            @loop(2)
            def _(c):
                part[chain, zh, zl, c, mine, :] = plus(
                    part[chain, zh, zl, c, mine, :], ra3[i, c]
                ).astype(BF16)
        elif k == 3:
            total = plus(part[chain, zh, zl, yi, mine, :], ra4[i]).astype(BF16)
            fin[i] = total
            target[mine, :] = total.astype(F32)
        else:
            target[other, :] = ra5[i].astype(F32)
        if k < 4:
            a_copy(i, chain, k + 1).start()

    def b_step(i, chain, k, target):
        b_copy(i, chain, k).wait()
        if k == 0:

            @loop(4)
            def _(d):
                a, b = d // 2, lax.rem(d, 2)
                part[chain, a, b, yi] = plus(part[chain, a, b, yi], rb1[i, a, b]).astype(BF16)
        elif k == 1:

            @loop(2)
            def _(a):
                part[chain, a, zl, yi] = plus(part[chain, a, zl, yi], rb2[i, a]).astype(BF16)
        elif k == 2:
            fin_b[i] = plus(part[chain, zh, zl, yi], rb3[i]).astype(BF16)
        else:
            target[...] = plus(fin_b[i], rb4[i])
        if k < 3:
            b_copy(i, chain, k + 1).start()

    def store_part(chain, cols, value):
        for d in range(8):
            part[chain, d // 4, (d // 2) % 2, d % 2, :, cols] = value[
                d * rows : (d + 1) * rows, :
            ].astype(BF16)

    def weight_grad(chain, left, right, base, tile, count, at=0):
        @loop(count)
        def _(n):
            value = nn(left[...], right[:, row(base // tile + n, tile, tile)])
            store_part(chain, row(at // tile + n, tile, tile), value)

    targets = (
        o_down.at[:, pl.ds(0, width)],
        o_down.at[:, pl.ds(width, width)],
        o_up.at[:, pl.ds(0, width)],
        o_up.at[:, pl.ds(width, width)],
        o_qk,
        o_vo,
    )

    def advance(chain, k):
        if chain % 2 == 0:
            a_step(chain // 2, chain, k, targets[chain])
        else:
            b_step(chain // 2, chain, k, targets[chain])

    weight_grad(0, dz_t, act, 0, 256, width // 256)
    a_copy(0, 0, 0).start()
    weight_grad(1, dz_t, act, width, 256, width // 256)
    b_copy(0, 1, 0).start()

    @loop(hidden // f_tile)
    def _(i):
        cols = row(i, f_tile, f_tile)
        total = jnp.zeros((8, f_tile), F32)
        for blk in range(2):
            area = pl.ds(blk * r_tile, r_tile)
            value = (nt(dz2[area, :], wdown[cols, :]) * slope[area, cols]).astype(BF16)
            du[area, cols] = value
            total = total + fold_rows(value.astype(F32))
        acc_up[:, cols] = total

    weight_grad(2, a1_t, du, 0, 256, width // 256)
    a_copy(1, 2, 0).start()
    weight_grad(3, a1_t, du, width, 256, width // 256)
    b_copy(1, 3, 0).start()

    for blk in range(2):
        area = pl.ds(blk * r_tile, r_tile)
        ex_send[2, area, :] = nt(du[area, :], wup[...]).astype(BF16)
        exchange(2, blk).start()

    @loop(tokens // sub)
    def _(i):
        area = row(i, sub, sub)
        x_t[:, area] = x[area, :].T

    for blk in range(2):
        exchange(2, blk).wait()

        @loop(r_tile // sub, start=blk * (r_tile // sub))
        def _(i):
            area = row(i, sub, sub)
            up = dz[area, :] + both(2, area)
            normal = n1[area, :]
            acc[3] += fold_rows(up)
            acc[4] += fold_rows(up * normal)
            scaled = up * gain1[...]
            mean_r = jnp.mean(scaled, axis=-1, keepdims=True)
            mean_rn = jnp.mean(scaled * normal, axis=-1, keepdims=True)
            down = (scaled - mean_r - normal * mean_rn) * r1[area, 0:1]
            acc[5] += fold_rows(down)
            dz[area, :] = down
            dz_t[:, area] = down.astype(BF16).T

    dctx_t[...] = nn(wout[...], dz_t[...]).astype(BF16)
    for g in range(2):
        for j in range(near):
            at = (g * near + j) * dim
            dctx_s[at : at + dim, :] = pick(g, j, lambda h: dctx_t[h * dim : (h + 1) * dim, :])

    advance(0, 0)
    advance(1, 0)

    def attend_back(g, target, base):
        @loop(near)
        def _(j):
            q_band, k_band, v_band = head_bands(g, j)
            c_band = dctx_s[row(g * near + j, dim, dim), :]
            keys, values = k_band.T, v_band.T
            d_key = jnp.zeros((dim, tokens), F32)
            d_value = jnp.zeros((dim, tokens), F32)
            for t in range(2):
                cols = slice(t * q_tile, (t + 1) * q_tile)
                scores = nn(keys, q_band[:, cols]) * scale
                shifted = scores - lse[pl.ds(g * near + j, 1), cols]
                probs = jnp.exp(jnp.where(allowed_of(g, t), shifted, MASKED))
                d_probs = nn(values, c_band[:, cols])
                delta = jnp.sum(probs * d_probs, axis=0, keepdims=True)
                d_scores = (probs * (d_probs - delta)).astype(BF16)
                d_value = d_value + nt(c_band[:, cols], probs.astype(BF16))
                d_key = d_key + nt(q_band[:, cols], d_scores)
                dq_t[row(g * near + j, dim, dim), cols] = (nn(k_band, d_scores) * scale).astype(
                    BF16
                )
            target[row(j, dim, dim), :] = (d_key * scale).astype(BF16)
            target[row(j + near, dim, dim), :] = d_value.astype(BF16)

    attend_back(1, dkv_send, 0)
    dkv_copy = remote(dkv_send, dkv_t.at[1], dkv_ss, dkv_rs, to_x)
    dkv_copy.start()
    advance(2, 0)
    advance(3, 0)
    attend_back(0, dkv_t.at[0], 0)
    advance(0, 1)
    advance(1, 1)
    weight_grad(5, dz_t, ctx, 0, local, 1, at=local)

    def restore(which):
        for h in range(n_heads):
            if which == 0:
                band = unpick(
                    h, lambda g, j: dq_t[(g * near + j) * dim : (g * near + j + 1) * dim, :]
                )
            else:
                base = (which - 1) * near
                band = unpick(
                    h, lambda g, j: dkv_t[g, (base + j) * dim : (base + j + 1) * dim, :]
                )
            dqkv[:, which * local + h * dim : which * local + (h + 1) * dim] = band.T

    restore(0)
    weight_grad(4, x_t, dqkv, 0, local, 1)
    dkv_copy.wait()
    restore(1)
    weight_grad(4, x_t, dqkv, local, local, 1, at=local)
    a_copy(2, 4, 0).start()
    restore(2)
    weight_grad(5, x_t, dqkv, 2 * local, local, 1)
    b_copy(2, 5, 0).start()

    for blk in range(2):
        area = pl.ds(blk * r_tile, r_tile)
        total = nt(dqkv[area, 0:local], wqkv[0])
        total = total + nt(dqkv[area, local : 2 * local], wqkv[1])
        total = total + nt(dqkv[area, 2 * local : 3 * local], wqkv[2])
        ex_send[3, area, :] = total.astype(BF16)
        exchange(3, blk).start()

    acc_qv[:, 0:local] = fold_rows(dqkv[:, 0:local].astype(F32))
    acc_qv[:, local:] = fold_rows(dqkv[:, 2 * local :].astype(F32))

    small = [jnp.sum(acc[i], axis=0, keepdims=True) for i in range(6)]
    small.append(jnp.sum(acc_up[:, 0:width], axis=0, keepdims=True))
    small.append(jnp.sum(acc_up[:, width:], axis=0, keepdims=True))
    small.append(jnp.sum(acc_qv[...], axis=0, keepdims=True))
    sm_send[...] = jnp.zeros_like(sm_send)
    for i, piece in enumerate(small):
        sm_send[0, i : i + 1, :] = piece

    def small_copy(k):
        where = (to_x, to_y, to_z1, to_z2)[k]
        return remote(sm_send.at[k], sm_recv.at[k], s_ss.at[k], s_rs.at[k], where)

    def small_step(k):
        small_copy(k).wait()
        total = sm_send[k] + sm_recv[k]
        if k < 3:
            sm_send[k + 1] = total
            small_copy(k + 1).start()
        else:
            o_small[...] = total

    small_copy(0).start()
    for blk in range(2):
        exchange(3, blk).wait()

        @loop(r_tile // sub, start=blk * (r_tile // sub))
        def _(i):
            area = row(i, sub, sub)
            gtok[area, :] = (dz[area, :] + both(3, area)).astype(BF16)

    for chain, k in TAIL:
        if chain == 6:
            small_step(k)
        else:
            advance(chain, k)


TAIL = (
    (0, 2), (1, 2), (6, 0), (2, 1), (3, 1), (0, 3), (1, 3), (6, 1), (0, 4), (2, 2), (3, 2),
    (6, 2), (2, 3), (3, 3), (2, 4), (6, 3), (4, 0), (5, 0), (4, 1), (5, 1), (4, 2), (5, 2),
    (4, 3), (5, 3), (4, 4),
)


def fast_local(
    tokens,
    segment_ids,
    head_perm,
    w_qkv,
    b_qv,
    w_out,
    b_out,
    norm1_gain,
    norm1_shift,
    w_up,
    b_up,
    w_down,
    b_down,
    norm2_gain,
    norm2_shift,
    grad_out,
):
    seq_count, block_rows, width = tokens.shape
    count = seq_count * block_rows
    local_width = w_qkv.shape[2]
    hidden = w_up.shape[1]
    n_batch = lax.axis_size("batch")
    rows = width // n_batch
    half = rows // 2
    dma, vm = pltpu.SemaphoreType.DMA, pltpu.VMEM
    in_vmem = pl.BlockSpec(memory_space=pltpu.VMEM)
    in_place = pl.BlockSpec(memory_space=pl.ANY)
    in_smem = pl.BlockSpec(memory_space=pltpu.SMEM)
    line = lambda value: value.reshape(1, -1)
    outs = pl.pallas_call(
        layer_kernel,
        out_shape=(
            jax.ShapeDtypeStruct((count, width), BF16),
            jax.ShapeDtypeStruct((count, width), BF16),
            jax.ShapeDtypeStruct((rows, hidden), F32),
            jax.ShapeDtypeStruct((rows, hidden), F32),
            jax.ShapeDtypeStruct((rows, width), F32),
            jax.ShapeDtypeStruct((rows, width), F32),
            jax.ShapeDtypeStruct((16, width), F32),
        ),
        in_specs=[in_vmem, in_vmem, in_smem] + [in_vmem] * 8 + [in_place] * 5,
        out_specs=[in_vmem] * 7,
        scratch_shapes=[
            vm((3, width, local_width), BF16),
            vm((local_width, width), BF16),
            vm((width, hidden), BF16),
            vm((hidden, width), BF16),
            vm((count, width), BF16),
            vm((3, local_width, count), BF16),
            vm((local_width, count), BF16),
            vm((local_width, count), BF16),
            vm((local_width, count), BF16),
            vm((local_width, count), BF16),
            vm((local_width, count), BF16),
            vm((count, local_width), BF16),
            vm((8, count), F32),
            vm((2, count, 128), F32),
            vm((4, count, width), BF16),
            vm((4, count, width), BF16),
            vm((count, width), BF16),
            vm((width, count), BF16),
            vm((count, width), F32),
            vm((count, 128), F32),
            vm((count, hidden), BF16),
            vm((count, hidden), F32),
            vm((count, width), F32),
            vm((count, width), BF16),
            vm((width, count), BF16),
            vm((count, hidden), BF16),
            vm((local_width, count), BF16),
            vm((local_width, count), BF16),
            vm((local_width, count), BF16),
            vm((2, local_width, count), BF16),
            vm((local_width, count), BF16),
            vm((count, 3 * local_width), BF16),
            vm((width, count), BF16),
            vm((6, 2, 2, 2, rows, width), BF16),
            vm((3, 2, 2, 2, half, width), BF16),
            vm((3, 2, 2, half, width), BF16),
            vm((3, 2, half, width), BF16),
            vm((3, half, width), BF16),
            vm((3, half, width), BF16),
            vm((3, half, width), BF16),
            vm((3, 2, 2, rows, width), BF16),
            vm((3, 2, rows, width), BF16),
            vm((3, rows, width), BF16),
            vm((3, rows, width), BF16),
            vm((3, rows, width), BF16),
            vm((6, 8, width), F32),
            vm((8, hidden), F32),
            vm((8, 2 * local_width), F32),
            vm((4, 16, width), F32),
            vm((4, 16, width), F32),
            dma((5,)),
            dma,
            dma,
            dma,
            dma,
            dma((4, 2)),
            dma((4, 2)),
            dma((3, 5)),
            dma((3, 5)),
            dma((3, 4)),
            dma((3, 4)),
            dma((4,)),
            dma((4,)),
        ],
        compiler_params=pltpu.CompilerParams(
            collective_id=0, has_side_effects=True, vmem_limit_bytes=67043328
        ),
        name="layer",
    )(
        tokens.reshape(count, width),
        segment_ids,
        head_perm,
        b_qv,
        line(b_out),
        line(norm1_gain),
        line(norm1_shift),
        line(b_up),
        line(b_down),
        line(norm2_gain),
        line(norm2_shift),
        jnp.transpose(w_qkv, (1, 0, 2)),
        w_out,
        w_up,
        w_down,
        grad_out.reshape(count, width),
    )
    output, grad_tokens, down, up, qk, vo, small = outs
    place = lax.axis_index("batch")

    def cut(value, parts):
        size = value.shape[-1] // parts
        return lax.dynamic_slice_in_dim(value, place * size, size, value.ndim - 1)

    lines = cut(small[:6], n_batch)
    return (
        output.reshape(tokens.shape),
        grad_tokens.reshape(tokens.shape),
        jnp.concatenate([qk, vo[:, :local_width]], axis=1).reshape(rows, 3, local_width),
        cut(small[8].reshape(2, local_width), n_batch),
        vo[:, local_width:].T,
        lines[5],
        lines[4],
        lines[3],
        up,
        cut(small[6:8].reshape(hidden), n_batch),
        down.T,
        lines[2],
        lines[1],
        lines[0],
    )


def solution(mesh):
    placed = (
        P("batch", "block", None),
        P("batch", None),
        P("tensor"),
        P(None, None, "tensor"),
        P(None, "tensor"),
        P("tensor", None),
        P(),
        P(),
        P(),
        P(None, "tensor"),
        P("tensor"),
        P("tensor", None),
        P(),
        P(),
        P(),
        P("batch", "block", None),
    )
    small_slice = mesh.shape["batch"] == 8 and mesh.shape["block"] == 2
    return jax.shard_map(
        fast_local if small_slice else local,
        mesh=mesh,
        in_specs=placed,
        out_specs=(
            P("batch", "block", None),
            P("batch", "block", None),
            P("batch", None, "tensor"),
            P(None, ("tensor", "batch")),
            P("tensor", "batch"),
            P("batch"),
            P("batch"),
            P("batch"),
            P("batch", "tensor"),
            P(("tensor", "batch")),
            P("tensor", "batch"),
            P("batch"),
            P("batch"),
            P("batch"),
        ),
        check_vma=False,
    )
```

```python
import functools

import jax
import jax.numpy as jnp
from jax import lax
from jax.experimental import pallas as pl
from jax.experimental.pallas import tpu as pltpu
from jax.sharding import PartitionSpec as P

EPSILON = 1e-12
MASKED = -1000000000.0


def swapped(value, axis, stride):
    mask = 2**stride
    pairs = [(source, source ^ mask) for source in range(lax.axis_size(axis))]
    return lax.ppermute(value, axis, pairs)


def pair_sum(value, axis):
    total = value.astype(jnp.float32)
    return total + swapped(value, axis, 0).astype(jnp.float32)


def halve(value, axis, bit, dim):
    mine = (lax.axis_index(axis) // 2**bit) % 2
    keep = lax.dynamic_index_in_dim(value, mine, dim, keepdims=False)
    give = lax.dynamic_index_in_dim(value, 1 - mine, dim, keepdims=False)
    got = swapped(give.astype(jnp.bfloat16), axis, bit)
    return keep.astype(jnp.float32) + got.astype(jnp.float32)


def scatter_sum(value, order):
    n_batch, rows, width = value.shape
    bits = n_batch.bit_length() - 1
    live = list(reversed(range(bits)))
    value = value.reshape((2,) * bits + (rows, width))
    gather = False
    for stage in order:
        if stage == "x":
            if live:
                value = value.reshape(value.shape[:-1] + (2, value.shape[-1] // 2))
                value = halve(value, "block", 0, value.ndim - 2)
                gather = True
            else:
                value = pair_sum(value.astype(jnp.bfloat16), "block")
        else:
            value = halve(value, "batch", stage, live.index(stage))
            live.remove(stage)
        if stage != order[-1] or gather:
            value = value.astype(jnp.bfloat16)
    if gather:
        other = swapped(value, "block", 0)
        first = lax.axis_index("block") == 0
        value = jnp.concatenate(
            [jnp.where(first, value, other), jnp.where(first, other, value)], axis=-1
        )
    return value.astype(jnp.float32)


def layer_norm(hidden, gain, shift):
    center = jnp.mean(hidden, axis=-1, keepdims=True)
    offset = hidden - center
    spread = jnp.mean(offset * offset, axis=-1, keepdims=True)
    return offset * lax.rsqrt(spread + EPSILON) * gain + shift


def gelu_exact(hidden):
    return jax.nn.gelu(hidden, approximate=False)


def block_scores(queries, key_rows, score_scale):
    return (
        jnp.einsum("qhd,khd->hqk", queries, key_rows, preferred_element_type=jnp.float32)
        * score_scale
    )


def forward_block(queries, key_rows, value_rows, query_segs, key_segs, score_scale):
    allowed = query_segs[None, :, None] == key_segs[:, None, :]
    scores = block_scores(queries, key_rows, score_scale)
    row_peak = jnp.max(jnp.where(allowed, scores, MASKED), axis=-1, keepdims=True)
    weights_exp = jnp.exp(jnp.where(allowed, scores - row_peak, MASKED))
    row_total = jnp.sum(weights_exp, axis=-1, keepdims=True)
    safe_total = jnp.where(row_total > 0, row_total, 1.0)
    probabilities = weights_exp / safe_total
    context = jnp.einsum(
        "hqk,khd->qhd",
        probabilities.astype(jnp.bfloat16),
        value_rows,
        preferred_element_type=jnp.float32,
    )
    logsum = jnp.where(row_total > 0, row_peak + jnp.log(safe_total), 0.0)
    return (context.astype(jnp.bfloat16), logsum)


def backward_block(
    queries, key_rows, value_rows, query_segs, key_segs, logsum, grad_context, score_scale
):
    allowed = query_segs[None, :, None] == key_segs[:, None, :]
    scores = block_scores(queries, key_rows, score_scale)
    probabilities = jnp.exp(jnp.where(allowed, scores - logsum, MASKED))
    grad_prob = jnp.einsum(
        "qhd,khd->hqk", grad_context, value_rows, preferred_element_type=jnp.float32
    )
    row_delta = jnp.sum(probabilities * grad_prob, axis=-1, keepdims=True)
    grad_scores = (probabilities * (grad_prob - row_delta)).astype(jnp.bfloat16)
    grad_queries = (
        jnp.einsum("hqk,khd->qhd", grad_scores, key_rows, preferred_element_type=jnp.float32)
        * score_scale
    )
    grad_keys = (
        jnp.einsum("hqk,qhd->khd", grad_scores, queries, preferred_element_type=jnp.float32)
        * score_scale
    )
    grad_values = jnp.einsum(
        "hqk,qhd->khd",
        probabilities.astype(jnp.bfloat16),
        grad_context,
        preferred_element_type=jnp.float32,
    )
    return (grad_queries, grad_keys, grad_values)


def local(
    tokens,
    segment_ids,
    head_perm,
    w_qkv,
    b_qv,
    w_out,
    b_out,
    norm1_gain,
    norm1_shift,
    w_up,
    b_up,
    w_down,
    b_down,
    norm2_gain,
    norm2_shift,
    grad_out,
):
    seq_count, block_rows, model_width = tokens.shape
    head_count = head_perm.shape[0]
    local_width = w_qkv.shape[2]
    head_dim = local_width // head_count
    near_heads = head_count // 2
    split_at = near_heads * head_dim
    far_width = local_width - split_at
    score_scale = head_dim ** (-0.5)
    token_count = seq_count * block_rows
    split_shape = (seq_count, block_rows, head_count, head_dim)
    flat_rows = tokens.reshape(token_count, model_width)
    head_order = jnp.argsort(head_perm, stable=True)
    head_undo = jnp.argsort(head_order, stable=True)
    sorted_qkv = jnp.take(
        w_qkv.reshape(model_width, 3, head_count, head_dim), head_order, axis=2
    ).reshape(model_width, 3 * local_width)
    sorted_bias = jnp.take(b_qv.reshape(2, head_count, head_dim), head_order, axis=1).reshape(
        2, local_width
    )
    sorted_out = jnp.take(
        w_out.reshape(head_count, head_dim, model_width), head_order, axis=0
    ).reshape(local_width, model_width)
    projected = jnp.dot(flat_rows, sorted_qkv, preferred_element_type=jnp.float32).reshape(
        token_count, 3, local_width
    )
    queries = (projected[:, 0] + sorted_bias[0]).astype(jnp.bfloat16)
    key_rows = projected[:, 1].astype(jnp.bfloat16)
    value_rows = (projected[:, 2] + sorted_bias[1]).astype(jnp.bfloat16)
    outgoing = jnp.concatenate([key_rows[:, split_at:], value_rows[:, split_at:]], axis=1).reshape(
        seq_count, block_rows, 2 * far_width
    )
    own_block = lax.axis_index("block")
    own_segs = lax.dynamic_slice_in_dim(segment_ids, own_block * block_rows, block_rows, 1)
    other_segs = lax.dynamic_slice_in_dim(segment_ids, (1 - own_block) * block_rows, block_rows, 1)
    key_segs = jnp.concatenate(
        [
            jnp.broadcast_to(own_segs[:, None, :], (seq_count, near_heads, block_rows)),
            jnp.broadcast_to(
                other_segs[:, None, :], (seq_count, head_count - near_heads, block_rows)
            ),
        ],
        axis=1,
    )
    partner = swapped(outgoing, "block", 0).reshape(token_count, 2 * far_width)
    all_keys = jnp.concatenate([key_rows[:, :split_at], partner[:, :far_width]], axis=1)
    all_values = jnp.concatenate([value_rows[:, :split_at], partner[:, far_width:]], axis=1)
    keys_full = all_keys.reshape(split_shape)
    values_full = all_values.reshape(split_shape)
    query_blocks = queries.reshape(split_shape)

    def forward_record(record):
        return forward_block(record[0], record[1], record[2], record[3], record[4], score_scale)

    context, logsum = lax.map(
        forward_record, (query_blocks, keys_full, values_full, own_segs, key_segs)
    )
    context_rows = context.reshape(token_count, local_width)
    attention = pair_sum(
        jnp.dot(context_rows, sorted_out, preferred_element_type=jnp.float32).astype(jnp.bfloat16),
        "tensor",
    )
    first_sum = flat_rows.astype(jnp.float32) + b_out + attention
    first_norm, first_back = jax.vjp(layer_norm, first_sum, norm1_gain, norm1_shift)
    first_low = first_norm.astype(jnp.bfloat16)
    up_rows = jnp.dot(first_low, w_up, preferred_element_type=jnp.float32) + b_up
    activated, gelu_back = jax.vjp(gelu_exact, up_rows)
    activated_low = activated.astype(jnp.bfloat16)
    branch = pair_sum(
        jnp.dot(activated_low, w_down, preferred_element_type=jnp.float32).astype(jnp.bfloat16),
        "tensor",
    )
    second_sum = first_norm + b_down + branch
    result, second_back = jax.vjp(layer_norm, second_sum, norm2_gain, norm2_shift)
    grad_second, grad_gain2, grad_shift2 = second_back(
        grad_out.reshape(token_count, model_width).astype(jnp.float32)
    )
    grad_second_low = grad_second.astype(jnp.bfloat16)
    grad_b_down = jnp.sum(grad_second, axis=0)
    grad_w_down = jnp.dot(grad_second_low.T, activated_low, preferred_element_type=jnp.float32)
    n_batch = lax.axis_size("batch")
    bits = tuple(range(n_batch.bit_length() - 1))
    y_last = ("x",) + bits[1:] + bits[:1]
    x_last = bits + ("x",)
    part_rows = model_width // n_batch
    final_w_down = scatter_sum(grad_w_down.reshape(n_batch, part_rows, -1), y_last).T
    (grad_up,) = gelu_back(jnp.dot(grad_second_low, w_down.T, preferred_element_type=jnp.float32))
    grad_up_low = grad_up.astype(jnp.bfloat16)
    grad_b_up = jnp.sum(grad_up_low.astype(jnp.float32), axis=0)
    grad_w_up = jnp.dot(first_low.T, grad_up_low, preferred_element_type=jnp.float32)
    final_w_up = scatter_sum(grad_w_up.reshape(n_batch, part_rows, -1), x_last)
    grad_first = grad_second + pair_sum(
        jnp.dot(grad_up_low, w_up.T, preferred_element_type=jnp.float32).astype(jnp.bfloat16),
        "tensor",
    )
    grad_middle, grad_gain1, grad_shift1 = first_back(grad_first)
    grad_middle_low = grad_middle.astype(jnp.bfloat16)
    grad_b_out = jnp.sum(grad_middle, axis=0)
    grad_out_sorted = jnp.dot(grad_middle_low.T, context_rows, preferred_element_type=jnp.float32)
    grad_context = (
        jnp.dot(grad_middle_low, sorted_out.T, preferred_element_type=jnp.float32)
        .astype(jnp.bfloat16)
        .reshape(split_shape)
    )
    back_keys, back_values = (keys_full, values_full)

    def backward_record(record):
        return backward_block(
            record[0], record[1], record[2], record[3], record[4], record[5], record[6], score_scale
        )

    grad_query, grad_key, grad_value = lax.map(
        backward_record,
        (query_blocks, back_keys, back_values, own_segs, key_segs, logsum, grad_context),
    )
    grad_query_low = grad_query.astype(jnp.bfloat16).reshape(token_count, local_width)
    grad_key_low = grad_key.astype(jnp.bfloat16).reshape(token_count, local_width)
    grad_value_low = grad_value.astype(jnp.bfloat16).reshape(token_count, local_width)
    returning = jnp.concatenate(
        [grad_key_low[:, split_at:], grad_value_low[:, split_at:]], axis=1
    ).reshape(seq_count, block_rows, 2 * far_width)
    returned = swapped(returning, "block", 0).reshape(token_count, 2 * far_width)
    grad_key_all = jnp.concatenate([grad_key_low[:, :split_at], returned[:, :far_width]], axis=1)
    grad_value_all = jnp.concatenate(
        [grad_value_low[:, :split_at], returned[:, far_width:]], axis=1
    )
    grad_qkv = jnp.stack([grad_query_low, grad_key_all, grad_value_all], axis=1).reshape(
        token_count, 3 * local_width
    )
    grad_qkv_sorted = jnp.dot(flat_rows.T, grad_qkv, preferred_element_type=jnp.float32)
    grad_bias_sorted = jnp.stack(
        [
            jnp.sum(grad_query_low.astype(jnp.float32), axis=0),
            jnp.sum(grad_value_all.astype(jnp.float32), axis=0),
        ]
    )
    grad_input = grad_middle + pair_sum(
        jnp.dot(grad_qkv, sorted_qkv.T, preferred_element_type=jnp.float32).astype(jnp.bfloat16),
        "tensor",
    )
    grad_w_qkv = jnp.take(
        grad_qkv_sorted.reshape(model_width, 3, head_count, head_dim), head_undo, axis=2
    ).reshape(model_width, 3, local_width)
    grad_b_qv = jnp.take(
        grad_bias_sorted.reshape(2, head_count, head_dim), head_undo, axis=1
    ).reshape(2, local_width)
    grad_w_out = jnp.take(
        grad_out_sorted.reshape(model_width, head_count, head_dim), head_undo, axis=1
    ).reshape(model_width, local_width)
    by_place = grad_w_qkv.reshape(n_batch, part_rows, 3, local_width)
    first_part = scatter_sum(by_place[:, :, :2].reshape(n_batch, part_rows, -1), y_last)
    second_part = scatter_sum(
        jnp.concatenate(
            [by_place[:, :, 2], grad_w_out.reshape(n_batch, part_rows, local_width)], axis=2
        ),
        x_last,
    )
    final_w_qkv = jnp.concatenate([first_part, second_part[:, :local_width]], axis=1).reshape(
        part_rows, 3, local_width
    )
    final_w_out = second_part[:, local_width:].T
    small = [
        grad_b_qv[0],
        grad_b_qv[1],
        grad_b_out,
        grad_gain1,
        grad_shift1,
        grad_b_up,
        grad_b_down,
        grad_gain2,
        grad_shift2,
    ]
    joined = jnp.concatenate([piece.reshape(n_batch, -1) for piece in small], axis=1)
    total = scatter_sum(joined[:, None, :], x_last)[0]
    ends, at = [], 0
    for piece in small:
        ends.append(total[at : at + piece.size // n_batch])
        at += piece.size // n_batch
    (bq, bv, final_b_out, final_gain1, final_shift1, final_b_up, final_b_down) = ends[:7]
    final_gain2, final_shift2 = ends[7:]
    final_b_qv = jnp.stack([bq, bv])
    output = result.astype(jnp.bfloat16).reshape(seq_count, block_rows, model_width)
    grad_tokens = grad_input.astype(jnp.bfloat16).reshape(seq_count, block_rows, model_width)
    return (
        output,
        grad_tokens,
        final_w_qkv,
        final_b_qv,
        final_w_out,
        final_b_out,
        final_gain1,
        final_shift1,
        final_w_up,
        final_b_up,
        final_w_down,
        final_b_down,
        final_gain2,
        final_shift2,
    )


F32 = jnp.float32
BF16 = jnp.bfloat16
MESH = pl.DeviceIdType.MESH
ROOT_HALF = 0.7071067811865476
DENSITY = 0.3989422804014327


def nn(left, right):
    return jnp.dot(left, right, preferred_element_type=F32)


def nt(left, right):
    return lax.dot_general(left, right, (((1,), (1,)), ((), ())), preferred_element_type=F32)


def loop(count, start=0):
    def run(body):
        def step(index, carry):
            body(index)
            return carry

        lax.fori_loop(start, start + count, step, 0)

    return run


def row(value, step, size):
    return pl.ds(pl.multiple_of(value * step, step), size)


def fold_rows(value):
    return jnp.sum(value.reshape(value.shape[0] // 8, 8, value.shape[1]), axis=0)


def layer_kernel(
    x,
    seg,
    perm,
    b_qv,
    i_b_out,
    i_gain1,
    i_shift1,
    i_b_up,
    i_b_down,
    i_gain2,
    i_shift2,
    h_wqkv,
    h_wout,
    h_wup,
    h_wdown,
    h_gout,
    out,
    gtok,
    o_down,
    o_up,
    o_out,
    o_qkv,
    o_small,
    b_out,
    gain1,
    shift1,
    b_up,
    b_down,
    gain2,
    shift2,
    wqkv,
    wout,
    wup,
    wdown,
    gout,
    heads_t,
    kv_send,
    kv_recv,
    kv_near,
    q_slots,
    ctx_t,
    ctx,
    lse,
    seg_col,
    ex_send,
    ex_recv,
    a1,
    a1_t,
    n1,
    r1,
    act,
    slope,
    dz,
    dz2,
    dz_t,
    du,
    dctx_t,
    dctx_s,
    dq_t,
    dkv_near,
    dkv_far,
    dkv_send,
    dqkv,
    x_t,
    part_f,
    rf0,
    rf1,
    rf2,
    rf3,
    rf4,
    fin_f,
    part_l,
    rl0,
    rl1,
    rl2,
    rl3,
    rl4,
    fin_l,
    acc,
    acc_up,
    acc_qv,
    sm_send,
    sm_recv,
    load_sem,
    kv_ss,
    kv_rs,
    dkv_ss,
    dkv_rs,
    ex_ss,
    ex_rs,
    c_ss,
    c_rs,
    s_ss,
    s_rs,
):
    tokens = x.shape[0]
    width = x.shape[1]
    local = wout.shape[0]
    hidden = wup.shape[1]
    n_heads = perm.shape[0]
    dim = local // n_heads
    near = n_heads // 2
    span = near * dim
    scale = dim ** (-0.5)
    half = part_f.shape[5]
    rows = 2 * half

    me_b = lax.axis_index("batch")
    bx = lax.axis_index("block")
    tc = lax.axis_index("tensor")
    yi = lax.rem(me_b, 2)
    zl = lax.rem(me_b // 2, 2)
    zh = me_b // 4
    to_core = {"tensor": 1 - tc}
    to_x = {"block": 1 - bx}
    to_y = {"batch": me_b + 1 - 2 * yi}
    to_z1 = {"batch": me_b + 2 - 4 * zl}
    to_z2 = {"batch": me_b + 4 - 8 * zh}

    def remote(src, dst, send, recv, where):
        return pltpu.make_async_remote_copy(
            src_ref=src,
            dst_ref=dst,
            send_sem=send,
            recv_sem=recv,
            device_id=where,
            device_id_type=MESH,
        )

    loads = [
        pltpu.make_async_copy(h_wqkv, wqkv, load_sem.at[0]),
        pltpu.make_async_copy(h_wout, wout, load_sem.at[1]),
        pltpu.make_async_copy(h_wup, wup, load_sem.at[2]),
        pltpu.make_async_copy(h_wdown, wdown, load_sem.at[3]),
        pltpu.make_async_copy(h_gout, gout, load_sem.at[4]),
    ]
    for copy in loads:
        copy.start()
    for target, source in (
        (b_out, i_b_out),
        (gain1, i_gain1),
        (shift1, i_shift1),
        (b_up, i_b_up),
        (b_down, i_b_down),
        (gain2, i_gain2),
        (shift2, i_shift2),
    ):
        target[...] = source[...].reshape(target.shape)

    barrier = pltpu.get_barrier_semaphore()
    for where in (to_core, to_x, to_y, to_z1, to_z2):
        pl.semaphore_signal(barrier, inc=1, device_id=where, device_id_type=MESH)

    far = [perm[h] for h in range(n_heads)]
    far_rank, near_rank = [], []
    f_count, n_count = jnp.int32(0), jnp.int32(0)
    for h in range(n_heads):
        far_rank.append(f_count)
        near_rank.append(n_count)
        f_count = f_count + far[h]
        n_count = n_count + (1 - far[h])
    rank = [far[h] * far_rank[h] + (1 - far[h]) * near_rank[h] for h in range(n_heads)]

    held = [
        [[(far[h] == g) & (rank[h] == j) for h in range(n_heads)] for j in range(near)]
        for g in range(2)
    ]

    def pick(g, j, bands):
        value = bands(j)
        for h in range(j + 1, j + 1 + n_heads - near):
            value = jnp.where(held[g][j][h], bands(h), value)
        return value

    def unpick(h, bands):
        value = None
        for g in range(2):
            for j in range(max(0, h - (n_heads - near)), min(h, near - 1) + 1):
                band = bands(g, j)
                value = band if value is None else jnp.where(held[g][j][h], band, value)
        return value

    def turned(which):
        return lambda h: heads_t[which, h * dim : (h + 1) * dim, :]

    for g in range(2):
        block = bx if g == 0 else 1 - bx
        line = seg[:, row(block, tokens, tokens)].astype(F32)
        seg_col[g] = jnp.broadcast_to(line, (128, tokens)).T

    loads[0].wait()
    pl.semaphore_wait(barrier, 5)

    for which in (1, 2, 0):
        bias = None if which == 1 else b_qv[0 if which == 0 else 1 : (0 if which == 0 else 1) + 1, :]

        @loop(2)
        def _(blk, which=which, bias=bias):
            value = nn(x[row(blk, tokens // 2, tokens // 2), :], wqkv[which])
            if bias is not None:
                value = value + bias
            heads_t[which, :, row(blk, tokens // 2, tokens // 2)] = value.astype(BF16).T

        if which == 2:

            kv_copies = []
            for j in range(near):
                kv_send[j, 0] = pick(1, j, turned(1))
                kv_send[j, 1] = pick(1, j, turned(2))
                kv_copies.append(
                    remote(kv_send.at[j], kv_recv.at[j], kv_ss.at[j], kv_rs.at[j], to_x)
                )
                kv_copies[j].start()

    q_tile = tokens // 2
    for j in range(near):
        kv_near[j, 0] = pick(0, j, turned(1))
        kv_near[j, 1] = pick(0, j, turned(2))
        for g in range(2):
            q_slots[g * span + j * dim : g * span + (j + 1) * dim, :] = pick(g, j, turned(0))

    def head_bands(g, j):
        source = kv_recv if g else kv_near
        return q_slots[row(g * near + j, dim, dim), :], source[j, 0], source[j, 1]

    def allowed_of(g, t):
        key_side = jnp.concatenate([seg_col[g]] * (q_tile // 128), axis=1)
        query_side = seg[:, row(2 * bx + t, q_tile, q_tile)].astype(F32)
        return key_side == query_side

    def attend(g, first, count):
        @loop(count, start=first)
        def _(j):
            q_band, k_band, v_band = head_bands(g, j)
            keys = k_band.T
            for t in range(2):
                cols = slice(t * q_tile, (t + 1) * q_tile)
                scores = nn(keys, q_band[:, cols]) * scale
                allowed = allowed_of(g, t)
                peak = jnp.max(jnp.where(allowed, scores, MASKED), axis=0, keepdims=True)
                weights = jnp.exp(jnp.where(allowed, scores - peak, MASKED))
                total = jnp.sum(weights, axis=0, keepdims=True)
                safe = jnp.where(total > 0, total, 1.0)
                probs = (weights * (1.0 / safe)).astype(BF16)
                band = row(g * near + j, dim, dim)
                ctx_t[band, cols] = nn(v_band, probs).astype(BF16)
                lse[pl.ds(g * near + j, 1), cols] = jnp.where(total > 0, peak + jnp.log(safe), 0.0)

    attend(0, 0, near)
    for j in range(near):
        kv_copies[j].wait()
        attend(1, j, 1)

    for h in range(n_heads):
        band = unpick(h, lambda g, j: ctx_t[(g * near + j) * dim : (g * near + j + 1) * dim, :])
        ctx[:, h * dim : (h + 1) * dim] = band.T

    r_tile = tokens // 2

    def exchange(index, blk):
        area = pl.ds(blk * r_tile, r_tile)
        return remote(
            ex_send.at[index, area],
            ex_recv.at[index, area],
            ex_ss.at[index, blk],
            ex_rs.at[index, blk],
            to_core,
        )

    def both(index, area):
        return ex_send[index, area, :].astype(F32) + ex_recv[index, area, :].astype(F32)

    loads[1].wait()
    for blk in range(2):
        area = pl.ds(blk * r_tile, r_tile)
        ex_send[0, area, :] = nn(ctx[area, :], wout[...]).astype(BF16)
        exchange(0, blk).start()

    sub = 128

    def norm(value):
        center = jnp.mean(value, axis=-1, keepdims=True)
        offset = value - center
        spread = jnp.mean(offset * offset, axis=-1, keepdims=True)
        inverse = lax.rsqrt(spread + EPSILON)
        return offset * inverse, inverse

    for blk in range(2):
        exchange(0, blk).wait()

        @loop(r_tile // sub, start=blk * (r_tile // sub))
        def _(i):
            area = row(i, sub, sub)
            value = x[area, :].astype(F32) + b_out[...] + both(0, area)
            normal, inverse = norm(value)
            n1[area, :] = normal
            r1[area, :] = jnp.broadcast_to(inverse, (sub, 128))
            low = (normal * gain1[...] + shift1[...]).astype(BF16)
            a1[area, :] = low
            a1_t[:, area] = low.T

    loads[2].wait()
    f_tile = 256

    @loop(hidden // f_tile)
    def _(i):
        cols = row(i, f_tile, f_tile)
        for blk in range(2):
            area = pl.ds(blk * r_tile, r_tile)
            up = nn(a1[area, :], wup[:, cols]) + b_up[:, cols]
            below = 0.5 + 0.5 * lax.erf(up * ROOT_HALF)
            act[area, cols] = (up * below).astype(BF16)
            slope[area, cols] = below + up * (DENSITY * jnp.exp(-0.5 * up * up))

    loads[3].wait()
    for blk in range(2):
        area = pl.ds(blk * r_tile, r_tile)
        ex_send[1, area, :] = nn(act[area, :], wdown[...]).astype(BF16)
        exchange(1, blk).start()

    acc[...] = jnp.zeros_like(acc)
    loads[4].wait()
    for blk in range(2):
        exchange(1, blk).wait()

        @loop(r_tile // sub, start=blk * (r_tile // sub))
        def _(i):
            area = row(i, sub, sub)
            first = n1[area, :] * gain1[...] + shift1[...]
            value = first + b_down[...] + both(1, area)
            normal, inverse = norm(value)
            out[area, :] = (normal * gain2[...] + shift2[...]).astype(BF16)
            up = gout[area, :].astype(F32)
            acc[0] += fold_rows(up)
            acc[1] += fold_rows(up * normal)
            scaled = up * gain2[...]
            mean_r = jnp.mean(scaled, axis=-1, keepdims=True)
            mean_rn = jnp.mean(scaled * normal, axis=-1, keepdims=True)
            down = (scaled - mean_r - normal * mean_rn) * inverse
            acc[2] += fold_rows(down)
            dz[area, :] = down
            low = down.astype(BF16)
            dz2[area, :] = low
            dz_t[:, area] = low.T

    mine = {"w": zh, "z": zl, "y": yi, "x": bx}
    partner = {"w": to_z2, "z": to_z1, "y": to_y, "x": to_x}

    def chain_refs(name):
        order, at, late = CHAINS[name]
        if late:
            return order, at, part_l, (rl0, rl1, rl2, rl3, rl4), fin_l, at + 6
        return order, at, part_f, (rf0, rf1, rf2, rf3, rf4), fin_f, at

    def chain_copy(name, k):
        order, at, part, got, fin, sem = chain_refs(name)
        if k == 4:
            src, where = fin.at[at], to_x
        else:
            where = partner[order[k]]
            index = [at]
            for d in "wzyx":
                if d == order[k]:
                    index.append(1 - mine[d])
                elif d in order[:k]:
                    index.append(mine[d])
                else:
                    index.append(slice(None))
            src = part.at[tuple(index)]
        return remote(src, got[k].at[at], c_ss.at[sem, k], c_rs.at[sem, k], where)

    def plus(left, right):
        return left.astype(F32) + right.astype(F32)

    def advance(name, k):
        order, at, part, got, fin, _ = chain_refs(name)
        chain_copy(name, k).wait()
        free = [d for d in "wzyx" if d not in order[: k + 1]]
        if k < 3:

            @loop(2 ** len(free))
            def _(i):
                spot = {d: lax.rem(i // 2**n, 2) for n, d in enumerate(free)}
                whole = tuple(spot[d] if d in free else mine[d] for d in "wzyx")
                some = tuple(spot[d] for d in free)
                part[(at,) + whole] = plus(part[(at,) + whole], got[k][(at,) + some]).astype(BF16)

        elif k == 3:
            total = plus(part[at, zh, zl, yi, bx], got[3][at]).astype(BF16)
            fin[at] = total
            target_of(name)[row(bx, half, half), :] = total.astype(F32)
        else:
            target_of(name)[row(1 - bx, half, half), :] = got[4][at].astype(F32)
        if k < 4:
            chain_copy(name, k + 1).start()

    def target_of(name):
        kind, n = name[0], CHAINS[name][1]
        if kind in "DU":
            size = part_f.shape[-1]
            return (o_down if kind == "D" else o_up).at[:, pl.ds((n % 3) * size, size)]
        return o_out if kind == "O" else o_qkv.at[n - 1]

    def weight_grad(name, left, right, base):
        _, at, part, _, _, _ = chain_refs(name)
        size = part.shape[-1]
        tile = 256 if size % 256 == 0 else size
        for n in range(size // tile):
            value = nn(left[...], right[:, base + n * tile : base + (n + 1) * tile])
            for d in range(16):
                part[
                    at, d // 8, (d // 4) % 2, (d // 2) % 2, d % 2, :, n * tile : (n + 1) * tile
                ] = value[d * half : (d + 1) * half, :].astype(BF16)
        chain_copy(name, 0).start()

    def grad_hidden():
        @loop(hidden // f_tile)
        def _(i):
            cols = row(i, f_tile, f_tile)
            total = jnp.zeros((8, f_tile), F32)
            for blk in range(2):
                area = pl.ds(blk * r_tile, r_tile)
                value = (nt(dz2[area, :], wdown[cols, :]) * slope[area, cols]).astype(BF16)
                du[area, cols] = value
                total = total + fold_rows(value.astype(F32))
            acc_up[:, cols] = total

    def send_first():
        for blk in range(2):
            area = pl.ds(blk * r_tile, r_tile)
            ex_send[2, area, :] = nt(du[area, :], wup[...]).astype(BF16)
            exchange(2, blk).start()

        @loop(tokens // sub)
        def _(i):
            area = row(i, sub, sub)
            x_t[:, area] = x[area, :].T

    def norm_back():
        for blk in range(2):
            exchange(2, blk).wait()

            @loop(r_tile // sub, start=blk * (r_tile // sub))
            def _(i):
                area = row(i, sub, sub)
                up = dz[area, :] + both(2, area)
                normal = n1[area, :]
                acc[3] += fold_rows(up)
                acc[4] += fold_rows(up * normal)
                scaled = up * gain1[...]
                mean_r = jnp.mean(scaled, axis=-1, keepdims=True)
                mean_rn = jnp.mean(scaled * normal, axis=-1, keepdims=True)
                down = (scaled - mean_r - normal * mean_rn) * r1[area, 0:1]
                acc[5] += fold_rows(down)
                dz[area, :] = down
                dz_t[:, area] = down.astype(BF16).T

    def grad_context():
        dctx_t[...] = nn(wout[...], dz_t[...]).astype(BF16)
        for g in range(2):
            for j in range(near):
                at = (g * near + j) * dim
                dctx_s[at : at + dim, :] = pick(g, j, lambda h: dctx_t[h * dim : (h + 1) * dim, :])

    def attend_back(g, first, count):
        target = dkv_send if g else dkv_near

        @loop(count, start=first)
        def _(j):
            q_band, k_band, v_band = head_bands(g, j)
            c_band = dctx_s[row(g * near + j, dim, dim), :]
            keys, values = k_band.T, v_band.T
            d_key = jnp.zeros((dim, tokens), F32)
            d_value = jnp.zeros((dim, tokens), F32)
            for t in range(2):
                cols = slice(t * q_tile, (t + 1) * q_tile)
                scores = nn(keys, q_band[:, cols]) * scale
                shifted = scores - lse[pl.ds(g * near + j, 1), cols]
                probs = jnp.exp(jnp.where(allowed_of(g, t), shifted, MASKED))
                d_probs = nn(values, c_band[:, cols])
                delta = jnp.sum(probs * d_probs, axis=0, keepdims=True)
                d_scores = (probs * (d_probs - delta)).astype(BF16)
                d_value = d_value + nt(c_band[:, cols], probs.astype(BF16))
                d_key = d_key + nt(q_band[:, cols], d_scores)
                dq_t[row(g * near + j, dim, dim), cols] = (nn(k_band, d_scores) * scale).astype(
                    BF16
                )
            target[j, 0] = (d_key * scale).astype(BF16)
            target[j, 1] = d_value.astype(BF16)

    def dkv_copy(j):
        return remote(dkv_send.at[j], dkv_far.at[j], dkv_ss.at[j], dkv_rs.at[j], to_x)

    def far_head(j):
        attend_back(1, j, 1)
        dkv_copy(j).start()

    def near_head(j):
        attend_back(0, j, 1)

    def keys_back():
        for j in range(near):
            dkv_copy(j).wait()

    def restore(which):
        for h in range(n_heads):
            if which == 0:
                band = unpick(
                    h, lambda g, j: dq_t[(g * near + j) * dim : (g * near + j + 1) * dim, :]
                )
            else:
                band = unpick(h, lambda g, j: (dkv_far if g else dkv_near)[j, which - 1])
            dqkv[:, which * local + h * dim : which * local + (h + 1) * dim] = band.T
        weight_grad("QKV"[which], x_t, dqkv, which * local)

    def send_input():
        for blk in range(2):
            area = pl.ds(blk * r_tile, r_tile)
            total = nt(dqkv[area, 0:local], wqkv[0])
            total = total + nt(dqkv[area, local : 2 * local], wqkv[1])
            total = total + nt(dqkv[area, 2 * local : 3 * local], wqkv[2])
            ex_send[3, area, :] = total.astype(BF16)
            exchange(3, blk).start()

    def small_copy(k):
        where = (to_x, to_y, to_z1, to_z2)[k]
        return remote(sm_send.at[k], sm_recv.at[k], s_ss.at[k], s_rs.at[k], where)

    def small_start():
        acc_qv[:, 0:local] = fold_rows(dqkv[:, 0:local].astype(F32))
        acc_qv[:, local:] = fold_rows(dqkv[:, 2 * local :].astype(F32))
        small = [jnp.sum(acc[i], axis=0, keepdims=True) for i in range(6)]
        small.append(jnp.sum(acc_up[:, 0:width], axis=0, keepdims=True))
        small.append(jnp.sum(acc_up[:, width:], axis=0, keepdims=True))
        small.append(jnp.sum(acc_qv[...], axis=0, keepdims=True))
        sm_send[...] = jnp.zeros_like(sm_send)
        for i, piece in enumerate(small):
            sm_send[0, i : i + 1, :] = piece
        small_copy(0).start()

    def small_step(k):
        small_copy(k).wait()
        total = sm_send[k] + sm_recv[k]
        if k < 3:
            sm_send[k + 1] = total
            small_copy(k + 1).start()
        else:
            o_small[...] = total

    def input_grad():
        for blk in range(2):
            exchange(3, blk).wait()

            @loop(r_tile // sub, start=blk * (r_tile // sub))
            def _(i):
                area = row(i, sub, sub)
                gtok[area, :] = (dz[area, :] + both(3, area)).astype(BF16)

    f_part = part_f.shape[-1]
    phases = {
        "gD0": lambda: weight_grad("D0", dz_t, act, 0),
        "gD1": lambda: weight_grad("D1", dz_t, act, f_part),
        "gD2": lambda: weight_grad("D2", dz_t, act, 2 * f_part),
        "dU": grad_hidden,
        "gU0": lambda: weight_grad("U0", a1_t, du, 0),
        "gU1": lambda: weight_grad("U1", a1_t, du, f_part),
        "gU2": lambda: weight_grad("U2", a1_t, du, 2 * f_part),
        "dA1": send_first,
        "ln1": norm_back,
        "dctx": grad_context,
        "gO": lambda: weight_grad("O", dz_t, ctx, 0),
        "gQ": lambda: restore(0),
        "wkv": keys_back,
        "gK": lambda: restore(1),
        "gV": lambda: restore(2),
        "dX": send_input,
        "small": small_start,
        "gt": input_grad,
    }
    for j in range(near):
        phases["f%d" % j] = functools.partial(far_head, j)
        phases["n%d" % j] = functools.partial(near_head, j)
    for item in PROGRAM:
        if isinstance(item, str):
            phases[item]()
        elif item[0] == "S":
            small_step(item[1])
        else:
            advance(*item)


CHAINS = {
    "D0": ("xyzw", 0, False),
    "D1": ("zyxw", 1, False),
    "D2": ("yzwx", 2, False),
    "U0": ("yzwx", 3, False),
    "U1": ("xyzw", 4, False),
    "U2": ("zyxw", 5, False),
    "O": ("xyzw", 0, True),
    "Q": ("zxyw", 1, True),
    "K": ("xyzw", 2, True),
    "V": ("yzxw", 3, True),
}

PROGRAM = (
    "gD0", "gD1", "gD2", "dU", "gU0", "gU1", "gU2", "dA1", "ln1", ("D0", 0), ("D1", 0), "dctx",
    ("D2", 0), "gO", "f0", "f1", "f2", ("U1", 0), ("U2", 0), ("U0", 0), "n0", ("D2", 1),
    ("D0", 1), "n1", ("O", 0), "n2", ("U0", 1), ("D1", 1), "gQ", ("D2", 2), ("D0", 2), ("U1", 1),
    "wkv", "gK", "gV", "dX", "small", ("D1", 2), ("U0", 2), ("D2", 3), ("U2", 1), "gt", ("O", 1),
    ("Q", 0), ("D0", 3), ("S", 0), ("K", 0), ("U1", 2), ("U0", 3), ("D2", 4), ("D1", 3), ("S", 1),
    ("O", 2), ("V", 0), ("U2", 2), ("U1", 3), ("K", 1), ("S", 2), ("O", 3), ("Q", 1), ("D0", 4),
    ("V", 1), ("U0", 4), ("S", 3), ("D1", 4), ("Q", 2), ("U2", 3), ("U1", 4), ("K", 2), ("O", 4),
    ("V", 2), ("Q", 3), ("U2", 4), ("K", 3), ("Q", 4), ("V", 3), ("K", 4), ("V", 4),
)


def finish_kernel(
    h_out, h_gtok, h_down, h_up, h_wout, h_qkv, small,
    out, gtok, down, up, wout, qkv, b_qv, b_out, gain1, shift1, b_up, b_down, gain2, shift2,
    t_out, t_gtok, t_down, t_up, t_wout, t_qkv, in_sem, out_sem,
):
    moves = (
        (h_out, t_out, out),
        (h_gtok, t_gtok, gtok),
        (h_down, t_down, down),
        (h_up, t_up, up),
        (h_wout, t_wout, wout),
        (h_qkv, t_qkv, qkv),
    )
    ins = [pltpu.make_async_copy(a, b, in_sem.at[i]) for i, (a, b, _) in enumerate(moves)]
    outs = [pltpu.make_async_copy(b, c, out_sem.at[i]) for i, (_, b, c) in enumerate(moves)]
    for copy in ins:
        copy.start()
    place = lax.axis_index("batch")
    width = small.shape[1]
    size = b_out.shape[0]

    def turn(value, amount):
        return pltpu.roll(value, value.shape[1] - amount, 1)

    lines = turn(small[0:8, :], place * size)
    for i, target in enumerate((shift2, gain2, b_down, shift1, gain1, b_out)):
        target[...] = lines[i, 0:size]
    long = b_up.shape[0]
    per = width // long
    upper = turn(small[6:7, :], lax.rem(place, per) * long)
    lower = turn(small[7:8, :], lax.rem(place, per) * long)
    chosen = jnp.where(place < per, upper, lower)
    b_up[...] = chosen[0, 0:long]
    short = b_qv.shape[1]
    first = turn(small[8:9, 0 : width // 2], place * short)
    second = turn(small[8:9, width // 2 :], place * short)
    b_qv[0:1, :] = first[:, 0:short]
    b_qv[1:2, :] = second[:, 0:short]
    for a, b in zip(ins, outs):
        a.wait()
        b.start()
    for b in outs:
        b.wait()


def fast_local(
    tokens,
    segment_ids,
    head_perm,
    w_qkv,
    b_qv,
    w_out,
    b_out,
    norm1_gain,
    norm1_shift,
    w_up,
    b_up,
    w_down,
    b_down,
    norm2_gain,
    norm2_shift,
    grad_out,
):
    seq_count, block_rows, width = tokens.shape
    count = seq_count * block_rows
    local_width = w_qkv.shape[2]
    hidden = w_up.shape[1]
    n_batch = lax.axis_size("batch")
    rows = width // n_batch
    half = rows // 2
    near = head_perm.shape[0] // 2
    dim = local_width // head_perm.shape[0]
    dma, vm = pltpu.SemaphoreType.DMA, pltpu.VMEM

    def chain_buffers(number, half, size):
        steps = [(2, 2, 2, 2), (2, 2, 2), (2, 2), (2,), (), (), ()]
        return [vm((number,) + step + (half, size), BF16) for step in steps]

    in_vmem = pl.BlockSpec(memory_space=pltpu.VMEM)
    in_place = pl.BlockSpec(memory_space=pl.ANY)
    in_smem = pl.BlockSpec(memory_space=pltpu.SMEM)
    outs = pl.pallas_call(
        layer_kernel,
        out_shape=(
            jax.ShapeDtypeStruct((count, width), BF16),
            jax.ShapeDtypeStruct((count, width), BF16),
            jax.ShapeDtypeStruct((rows, hidden), F32),
            jax.ShapeDtypeStruct((rows, hidden), F32),
            jax.ShapeDtypeStruct((rows, local_width), F32),
            jax.ShapeDtypeStruct((3, rows, local_width), F32),
            jax.ShapeDtypeStruct((16, width), F32),
        ),
        in_specs=[in_vmem, in_vmem, in_smem] + [in_vmem] * 8 + [in_place] * 5,
        out_specs=[in_vmem] * 7,
        scratch_shapes=[
            vm((1, width), F32),
            vm((1, width), F32),
            vm((1, width), F32),
            vm((1, hidden), F32),
            vm((1, width), F32),
            vm((1, width), F32),
            vm((1, width), F32),
            vm((3, width, local_width), BF16),
            vm((local_width, width), BF16),
            vm((width, hidden), BF16),
            vm((hidden, width), BF16),
            vm((count, width), BF16),
            vm((3, local_width, count), BF16),
            vm((near, 2, dim, count), BF16),
            vm((near, 2, dim, count), BF16),
            vm((near, 2, dim, count), BF16),
            vm((local_width, count), BF16),
            vm((local_width, count), BF16),
            vm((count, local_width), BF16),
            vm((8, count), F32),
            vm((2, count, 128), F32),
            vm((4, count, width), BF16),
            vm((4, count, width), BF16),
            vm((count, width), BF16),
            vm((width, count), BF16),
            vm((count, width), F32),
            vm((count, 128), F32),
            vm((count, hidden), BF16),
            vm((count, hidden), F32),
            vm((count, width), F32),
            vm((count, width), BF16),
            vm((width, count), BF16),
            vm((count, hidden), BF16),
            vm((local_width, count), BF16),
            vm((local_width, count), BF16),
            vm((local_width, count), BF16),
            vm((near, 2, dim, count), BF16),
            vm((near, 2, dim, count), BF16),
            vm((near, 2, dim, count), BF16),
            vm((count, 3 * local_width), BF16),
            vm((width, count), BF16),
            *chain_buffers(6, half, hidden // 3),
            *chain_buffers(4, half, local_width),
            vm((6, 8, width), F32),
            vm((8, hidden), F32),
            vm((8, 2 * local_width), F32),
            vm((4, 16, width), F32),
            vm((4, 16, width), F32),
            dma((5,)),
            dma((near,)),
            dma((near,)),
            dma((near,)),
            dma((near,)),
            dma((4, 2)),
            dma((4, 2)),
            dma((10, 5)),
            dma((10, 5)),
            dma((4,)),
            dma((4,)),
        ],
        compiler_params=pltpu.CompilerParams(
            collective_id=0, has_side_effects=True, vmem_limit_bytes=67043328
        ),
        name="layer",
    )(
        tokens.reshape(count, width),
        segment_ids,
        head_perm,
        b_qv,
        b_out,
        norm1_gain,
        norm1_shift,
        b_up,
        b_down,
        norm2_gain,
        norm2_shift,
        jnp.transpose(w_qkv, (1, 0, 2)),
        w_out,
        w_up,
        w_down,
        grad_out.reshape(count, width),
    )
    vec = jax.ShapeDtypeStruct((rows,), F32)
    results = pl.pallas_call(
        finish_kernel,
        out_shape=(
            *[jax.ShapeDtypeStruct(value.shape, value.dtype) for value in outs[:6]],
            jax.ShapeDtypeStruct((2, local_width // n_batch), F32),
            vec,
            vec,
            vec,
            jax.ShapeDtypeStruct((hidden // n_batch,), F32),
            vec,
            vec,
            vec,
        ),
        in_specs=[in_place] * 6 + [in_vmem],
        out_specs=[in_place] * 6 + [in_vmem] * 8,
        scratch_shapes=[vm(value.shape, value.dtype) for value in outs[:6]] + [dma((6,)), dma((6,))],
        name="finish",
    )(*outs)
    output, grad_tokens, down, up, g_out, g_qkv = results[:6]
    b_qv_grad, b_out_grad, gain1_grad, shift1_grad, b_up_grad, b_down_grad = results[6:12]
    return (
        output.reshape(tokens.shape),
        grad_tokens.reshape(tokens.shape),
        jnp.transpose(g_qkv, (1, 0, 2)),
        b_qv_grad,
        g_out.T,
        b_out_grad,
        gain1_grad,
        shift1_grad,
        up,
        b_up_grad,
        down.T,
        b_down_grad,
        results[12],
        results[13],
    )


def solution(mesh):
    placed = (
        P("batch", "block", None),
        P("batch", None),
        P("tensor"),
        P(None, None, "tensor"),
        P(None, "tensor"),
        P("tensor", None),
        P(),
        P(),
        P(),
        P(None, "tensor"),
        P("tensor"),
        P("tensor", None),
        P(),
        P(),
        P(),
        P("batch", "block", None),
    )
    small_slice = mesh.shape["batch"] == 8 and mesh.shape["block"] == 2
    return jax.shard_map(
        fast_local if small_slice else local,
        mesh=mesh,
        in_specs=placed,
        out_specs=(
            P("batch", "block", None),
            P("batch", "block", None),
            P("batch", None, "tensor"),
            P(None, ("tensor", "batch")),
            P("tensor", "batch"),
            P("batch"),
            P("batch"),
            P("batch"),
            P("batch", "tensor"),
            P(("tensor", "batch")),
            P("tensor", "batch"),
            P("batch"),
            P("batch"),
            P("batch"),
        ),
        check_vma=False,
    )
```

```python
import functools

import jax
import jax.numpy as jnp
from jax import lax
from jax.experimental import pallas as pl
from jax.experimental.pallas import tpu as pltpu
from jax.sharding import PartitionSpec as P

EPSILON = 1e-12
MASKED = -1000000000.0


def swapped(value, axis, stride):
    mask = 2**stride
    pairs = [(source, source ^ mask) for source in range(lax.axis_size(axis))]
    return lax.ppermute(value, axis, pairs)


def pair_sum(value, axis):
    total = value.astype(jnp.float32)
    return total + swapped(value, axis, 0).astype(jnp.float32)


def halve(value, axis, bit, dim):
    mine = (lax.axis_index(axis) // 2**bit) % 2
    keep = lax.dynamic_index_in_dim(value, mine, dim, keepdims=False)
    give = lax.dynamic_index_in_dim(value, 1 - mine, dim, keepdims=False)
    got = swapped(give.astype(jnp.bfloat16), axis, bit)
    return keep.astype(jnp.float32) + got.astype(jnp.float32)


def scatter_sum(value, order):
    n_batch, rows, width = value.shape
    bits = n_batch.bit_length() - 1
    live = list(reversed(range(bits)))
    value = value.reshape((2,) * bits + (rows, width))
    gather = False
    for stage in order:
        if stage == "x":
            if live:
                value = value.reshape(value.shape[:-1] + (2, value.shape[-1] // 2))
                value = halve(value, "block", 0, value.ndim - 2)
                gather = True
            else:
                value = pair_sum(value.astype(jnp.bfloat16), "block")
        else:
            value = halve(value, "batch", stage, live.index(stage))
            live.remove(stage)
        if stage != order[-1] or gather:
            value = value.astype(jnp.bfloat16)
    if gather:
        other = swapped(value, "block", 0)
        first = lax.axis_index("block") == 0
        value = jnp.concatenate(
            [jnp.where(first, value, other), jnp.where(first, other, value)], axis=-1
        )
    return value.astype(jnp.float32)


def layer_norm(hidden, gain, shift):
    center = jnp.mean(hidden, axis=-1, keepdims=True)
    offset = hidden - center
    spread = jnp.mean(offset * offset, axis=-1, keepdims=True)
    return offset * lax.rsqrt(spread + EPSILON) * gain + shift


def gelu_exact(hidden):
    return jax.nn.gelu(hidden, approximate=False)


def block_scores(queries, key_rows, score_scale):
    return (
        jnp.einsum("qhd,khd->hqk", queries, key_rows, preferred_element_type=jnp.float32)
        * score_scale
    )


def forward_block(queries, key_rows, value_rows, query_segs, key_segs, score_scale):
    allowed = query_segs[None, :, None] == key_segs[:, None, :]
    scores = block_scores(queries, key_rows, score_scale)
    row_peak = jnp.max(jnp.where(allowed, scores, MASKED), axis=-1, keepdims=True)
    weights_exp = jnp.exp(jnp.where(allowed, scores - row_peak, MASKED))
    row_total = jnp.sum(weights_exp, axis=-1, keepdims=True)
    safe_total = jnp.where(row_total > 0, row_total, 1.0)
    probabilities = weights_exp / safe_total
    context = jnp.einsum(
        "hqk,khd->qhd",
        probabilities.astype(jnp.bfloat16),
        value_rows,
        preferred_element_type=jnp.float32,
    )
    logsum = jnp.where(row_total > 0, row_peak + jnp.log(safe_total), 0.0)
    return (context.astype(jnp.bfloat16), logsum)


def backward_block(
    queries, key_rows, value_rows, query_segs, key_segs, logsum, grad_context, score_scale
):
    allowed = query_segs[None, :, None] == key_segs[:, None, :]
    scores = block_scores(queries, key_rows, score_scale)
    probabilities = jnp.exp(jnp.where(allowed, scores - logsum, MASKED))
    grad_prob = jnp.einsum(
        "qhd,khd->hqk", grad_context, value_rows, preferred_element_type=jnp.float32
    )
    row_delta = jnp.sum(probabilities * grad_prob, axis=-1, keepdims=True)
    grad_scores = (probabilities * (grad_prob - row_delta)).astype(jnp.bfloat16)
    grad_queries = (
        jnp.einsum("hqk,khd->qhd", grad_scores, key_rows, preferred_element_type=jnp.float32)
        * score_scale
    )
    grad_keys = (
        jnp.einsum("hqk,qhd->khd", grad_scores, queries, preferred_element_type=jnp.float32)
        * score_scale
    )
    grad_values = jnp.einsum(
        "hqk,qhd->khd",
        probabilities.astype(jnp.bfloat16),
        grad_context,
        preferred_element_type=jnp.float32,
    )
    return (grad_queries, grad_keys, grad_values)


def local(
    tokens,
    segment_ids,
    head_perm,
    w_qkv,
    b_qv,
    w_out,
    b_out,
    norm1_gain,
    norm1_shift,
    w_up,
    b_up,
    w_down,
    b_down,
    norm2_gain,
    norm2_shift,
    grad_out,
):
    seq_count, block_rows, model_width = tokens.shape
    head_count = head_perm.shape[0]
    local_width = w_qkv.shape[2]
    head_dim = local_width // head_count
    near_heads = head_count // 2
    split_at = near_heads * head_dim
    far_width = local_width - split_at
    score_scale = head_dim ** (-0.5)
    token_count = seq_count * block_rows
    split_shape = (seq_count, block_rows, head_count, head_dim)
    flat_rows = tokens.reshape(token_count, model_width)
    head_order = jnp.argsort(head_perm, stable=True)
    head_undo = jnp.argsort(head_order, stable=True)
    sorted_qkv = jnp.take(
        w_qkv.reshape(model_width, 3, head_count, head_dim), head_order, axis=2
    ).reshape(model_width, 3 * local_width)
    sorted_bias = jnp.take(b_qv.reshape(2, head_count, head_dim), head_order, axis=1).reshape(
        2, local_width
    )
    sorted_out = jnp.take(
        w_out.reshape(head_count, head_dim, model_width), head_order, axis=0
    ).reshape(local_width, model_width)
    projected = jnp.dot(flat_rows, sorted_qkv, preferred_element_type=jnp.float32).reshape(
        token_count, 3, local_width
    )
    queries = (projected[:, 0] + sorted_bias[0]).astype(jnp.bfloat16)
    key_rows = projected[:, 1].astype(jnp.bfloat16)
    value_rows = (projected[:, 2] + sorted_bias[1]).astype(jnp.bfloat16)
    outgoing = jnp.concatenate([key_rows[:, split_at:], value_rows[:, split_at:]], axis=1).reshape(
        seq_count, block_rows, 2 * far_width
    )
    own_block = lax.axis_index("block")
    own_segs = lax.dynamic_slice_in_dim(segment_ids, own_block * block_rows, block_rows, 1)
    other_segs = lax.dynamic_slice_in_dim(segment_ids, (1 - own_block) * block_rows, block_rows, 1)
    key_segs = jnp.concatenate(
        [
            jnp.broadcast_to(own_segs[:, None, :], (seq_count, near_heads, block_rows)),
            jnp.broadcast_to(
                other_segs[:, None, :], (seq_count, head_count - near_heads, block_rows)
            ),
        ],
        axis=1,
    )
    partner = swapped(outgoing, "block", 0).reshape(token_count, 2 * far_width)
    all_keys = jnp.concatenate([key_rows[:, :split_at], partner[:, :far_width]], axis=1)
    all_values = jnp.concatenate([value_rows[:, :split_at], partner[:, far_width:]], axis=1)
    keys_full = all_keys.reshape(split_shape)
    values_full = all_values.reshape(split_shape)
    query_blocks = queries.reshape(split_shape)

    def forward_record(record):
        return forward_block(record[0], record[1], record[2], record[3], record[4], score_scale)

    context, logsum = lax.map(
        forward_record, (query_blocks, keys_full, values_full, own_segs, key_segs)
    )
    context_rows = context.reshape(token_count, local_width)
    attention = pair_sum(
        jnp.dot(context_rows, sorted_out, preferred_element_type=jnp.float32).astype(jnp.bfloat16),
        "tensor",
    )
    first_sum = flat_rows.astype(jnp.float32) + b_out + attention
    first_norm, first_back = jax.vjp(layer_norm, first_sum, norm1_gain, norm1_shift)
    first_low = first_norm.astype(jnp.bfloat16)
    up_rows = jnp.dot(first_low, w_up, preferred_element_type=jnp.float32) + b_up
    activated, gelu_back = jax.vjp(gelu_exact, up_rows)
    activated_low = activated.astype(jnp.bfloat16)
    branch = pair_sum(
        jnp.dot(activated_low, w_down, preferred_element_type=jnp.float32).astype(jnp.bfloat16),
        "tensor",
    )
    second_sum = first_norm + b_down + branch
    result, second_back = jax.vjp(layer_norm, second_sum, norm2_gain, norm2_shift)
    grad_second, grad_gain2, grad_shift2 = second_back(
        grad_out.reshape(token_count, model_width).astype(jnp.float32)
    )
    grad_second_low = grad_second.astype(jnp.bfloat16)
    grad_b_down = jnp.sum(grad_second, axis=0)
    grad_w_down = jnp.dot(grad_second_low.T, activated_low, preferred_element_type=jnp.float32)
    n_batch = lax.axis_size("batch")
    bits = tuple(range(n_batch.bit_length() - 1))
    y_last = ("x",) + bits[1:] + bits[:1]
    x_last = bits + ("x",)
    part_rows = model_width // n_batch
    final_w_down = scatter_sum(grad_w_down.reshape(n_batch, part_rows, -1), y_last).T
    (grad_up,) = gelu_back(jnp.dot(grad_second_low, w_down.T, preferred_element_type=jnp.float32))
    grad_up_low = grad_up.astype(jnp.bfloat16)
    grad_b_up = jnp.sum(grad_up_low.astype(jnp.float32), axis=0)
    grad_w_up = jnp.dot(first_low.T, grad_up_low, preferred_element_type=jnp.float32)
    final_w_up = scatter_sum(grad_w_up.reshape(n_batch, part_rows, -1), x_last)
    grad_first = grad_second + pair_sum(
        jnp.dot(grad_up_low, w_up.T, preferred_element_type=jnp.float32).astype(jnp.bfloat16),
        "tensor",
    )
    grad_middle, grad_gain1, grad_shift1 = first_back(grad_first)
    grad_middle_low = grad_middle.astype(jnp.bfloat16)
    grad_b_out = jnp.sum(grad_middle, axis=0)
    grad_out_sorted = jnp.dot(grad_middle_low.T, context_rows, preferred_element_type=jnp.float32)
    grad_context = (
        jnp.dot(grad_middle_low, sorted_out.T, preferred_element_type=jnp.float32)
        .astype(jnp.bfloat16)
        .reshape(split_shape)
    )
    back_keys, back_values = (keys_full, values_full)

    def backward_record(record):
        return backward_block(
            record[0], record[1], record[2], record[3], record[4], record[5], record[6], score_scale
        )

    grad_query, grad_key, grad_value = lax.map(
        backward_record,
        (query_blocks, back_keys, back_values, own_segs, key_segs, logsum, grad_context),
    )
    grad_query_low = grad_query.astype(jnp.bfloat16).reshape(token_count, local_width)
    grad_key_low = grad_key.astype(jnp.bfloat16).reshape(token_count, local_width)
    grad_value_low = grad_value.astype(jnp.bfloat16).reshape(token_count, local_width)
    returning = jnp.concatenate(
        [grad_key_low[:, split_at:], grad_value_low[:, split_at:]], axis=1
    ).reshape(seq_count, block_rows, 2 * far_width)
    returned = swapped(returning, "block", 0).reshape(token_count, 2 * far_width)
    grad_key_all = jnp.concatenate([grad_key_low[:, :split_at], returned[:, :far_width]], axis=1)
    grad_value_all = jnp.concatenate(
        [grad_value_low[:, :split_at], returned[:, far_width:]], axis=1
    )
    grad_qkv = jnp.stack([grad_query_low, grad_key_all, grad_value_all], axis=1).reshape(
        token_count, 3 * local_width
    )
    grad_qkv_sorted = jnp.dot(flat_rows.T, grad_qkv, preferred_element_type=jnp.float32)
    grad_bias_sorted = jnp.stack(
        [
            jnp.sum(grad_query_low.astype(jnp.float32), axis=0),
            jnp.sum(grad_value_all.astype(jnp.float32), axis=0),
        ]
    )
    grad_input = grad_middle + pair_sum(
        jnp.dot(grad_qkv, sorted_qkv.T, preferred_element_type=jnp.float32).astype(jnp.bfloat16),
        "tensor",
    )
    grad_w_qkv = jnp.take(
        grad_qkv_sorted.reshape(model_width, 3, head_count, head_dim), head_undo, axis=2
    ).reshape(model_width, 3, local_width)
    grad_b_qv = jnp.take(
        grad_bias_sorted.reshape(2, head_count, head_dim), head_undo, axis=1
    ).reshape(2, local_width)
    grad_w_out = jnp.take(
        grad_out_sorted.reshape(model_width, head_count, head_dim), head_undo, axis=1
    ).reshape(model_width, local_width)
    by_place = grad_w_qkv.reshape(n_batch, part_rows, 3, local_width)
    first_part = scatter_sum(by_place[:, :, :2].reshape(n_batch, part_rows, -1), y_last)
    second_part = scatter_sum(
        jnp.concatenate(
            [by_place[:, :, 2], grad_w_out.reshape(n_batch, part_rows, local_width)], axis=2
        ),
        x_last,
    )
    final_w_qkv = jnp.concatenate([first_part, second_part[:, :local_width]], axis=1).reshape(
        part_rows, 3, local_width
    )
    final_w_out = second_part[:, local_width:].T
    small = [
        grad_b_qv[0],
        grad_b_qv[1],
        grad_b_out,
        grad_gain1,
        grad_shift1,
        grad_b_up,
        grad_b_down,
        grad_gain2,
        grad_shift2,
    ]
    joined = jnp.concatenate([piece.reshape(n_batch, -1) for piece in small], axis=1)
    total = scatter_sum(joined[:, None, :], x_last)[0]
    ends, at = [], 0
    for piece in small:
        ends.append(total[at : at + piece.size // n_batch])
        at += piece.size // n_batch
    (bq, bv, final_b_out, final_gain1, final_shift1, final_b_up, final_b_down) = ends[:7]
    final_gain2, final_shift2 = ends[7:]
    final_b_qv = jnp.stack([bq, bv])
    output = result.astype(jnp.bfloat16).reshape(seq_count, block_rows, model_width)
    grad_tokens = grad_input.astype(jnp.bfloat16).reshape(seq_count, block_rows, model_width)
    return (
        output,
        grad_tokens,
        final_w_qkv,
        final_b_qv,
        final_w_out,
        final_b_out,
        final_gain1,
        final_shift1,
        final_w_up,
        final_b_up,
        final_w_down,
        final_b_down,
        final_gain2,
        final_shift2,
    )


F32 = jnp.float32
BF16 = jnp.bfloat16
MESH = pl.DeviceIdType.MESH
ROOT_HALF = 0.7071067811865476
DENSITY = 0.3989422804014327


def nn(left, right):
    return jnp.dot(left, right, preferred_element_type=F32)


def nt(left, right):
    return lax.dot_general(left, right, (((1,), (1,)), ((), ())), preferred_element_type=F32)


def loop(count, start=0):
    def run(body):
        def step(index, carry):
            body(index)
            return carry

        lax.fori_loop(start, start + count, step, 0)

    return run


def row(value, step, size):
    return pl.ds(pl.multiple_of(value * step, step), size)


def fold_rows(value):
    return jnp.sum(value.reshape(value.shape[0] // 8, 8, value.shape[1]), axis=0)


def layer_kernel(
    seg,
    perm,
    b_qv,
    i_b_out,
    i_gain1,
    i_shift1,
    i_b_up,
    i_b_down,
    i_gain2,
    i_shift2,
    h_x,
    h_wqkv,
    h_wout,
    h_wup,
    h_wdown,
    h_gout,
    out,
    gtok,
    o_down,
    o_up,
    o_out,
    o_qkv,
    o_small,
    b_out,
    gain1,
    shift1,
    b_up,
    b_down,
    gain2,
    shift2,
    x,
    wqkv,
    wout,
    wup,
    wdown,
    gout,
    heads_t,
    kv_send,
    kv_recv,
    kv_near,
    q_slots,
    ctx_t,
    ctx,
    lse,
    seg_col,
    ex_send,
    ex_recv,
    a1,
    a1_t,
    n1,
    r1,
    act,
    slope,
    dz,
    dz2,
    dz_t,
    du,
    dctx_t,
    dctx_s,
    dq_t,
    dkv_near,
    dkv_far,
    dkv_send,
    dqkv,
    x_t,
    part_f,
    rf0,
    rf1,
    rf2,
    rf3,
    rf4,
    fin_f,
    part_l,
    rl0,
    rl1,
    rl2,
    rl3,
    rl4,
    fin_l,
    acc,
    acc_up,
    acc_qv,
    sm_send,
    sm_recv,
    load_sem,
    kv_ss,
    kv_rs,
    dkv_ss,
    dkv_rs,
    ex_ss,
    ex_rs,
    c_ss,
    c_rs,
    s_ss,
    s_rs,
):
    tokens = x.shape[0]
    width = x.shape[1]
    local = wout.shape[0]
    hidden = wup.shape[1]
    n_heads = perm.shape[0]
    dim = local // n_heads
    near = n_heads // 2
    span = near * dim
    scale = dim ** (-0.5)
    half = part_f.shape[5]
    rows = 2 * half

    me_b = lax.axis_index("batch")
    bx = lax.axis_index("block")
    tc = lax.axis_index("tensor")
    yi = lax.rem(me_b, 2)
    zl = lax.rem(me_b // 2, 2)
    zh = me_b // 4
    to_core = {"tensor": 1 - tc}
    to_x = {"block": 1 - bx}
    to_y = {"batch": me_b + 1 - 2 * yi}
    to_z1 = {"batch": me_b + 2 - 4 * zl}
    to_z2 = {"batch": me_b + 4 - 8 * zh}

    def remote(src, dst, send, recv, where):
        return pltpu.make_async_remote_copy(
            src_ref=src,
            dst_ref=dst,
            send_sem=send,
            recv_sem=recv,
            device_id=where,
            device_id_type=MESH,
        )

    def load(source, target, index):
        return pltpu.make_async_copy(source, target, load_sem.at[index])

    l_x = load(h_x, x, 0)
    l_qkv = [load(h_wqkv.at[i], wqkv.at[i], 1 + i) for i in range(3)]
    l_wout = load(h_wout, wout, 4)
    l_wup = load(h_wup, wup, 5)
    l_wdown = load(h_wdown, wdown, 6)
    l_gout = load(h_gout, gout, 7)
    l_x.start()
    for which in (1, 2, 0):
        l_qkv[which].start()

    barrier = pltpu.get_barrier_semaphore()
    for where in (to_core, to_x, to_y, to_z1, to_z2):
        pl.semaphore_signal(barrier, inc=1, device_id=where, device_id_type=MESH)

    for target, source in (
        (b_out, i_b_out),
        (gain1, i_gain1),
        (shift1, i_shift1),
        (b_up, i_b_up),
        (b_down, i_b_down),
        (gain2, i_gain2),
        (shift2, i_shift2),
    ):
        target[...] = source[...].reshape(target.shape)

    far = [perm[h] for h in range(n_heads)]
    far_rank, near_rank = [], []
    f_count, n_count = jnp.int32(0), jnp.int32(0)
    for h in range(n_heads):
        far_rank.append(f_count)
        near_rank.append(n_count)
        f_count = f_count + far[h]
        n_count = n_count + (1 - far[h])
    rank = [far[h] * far_rank[h] + (1 - far[h]) * near_rank[h] for h in range(n_heads)]

    held = [
        [[(far[h] == g) & (rank[h] == j) for h in range(n_heads)] for j in range(near)]
        for g in range(2)
    ]

    def pick(g, j, bands):
        value = bands(j)
        for h in range(j + 1, j + 1 + n_heads - near):
            value = jnp.where(held[g][j][h], bands(h), value)
        return value

    def unpick(h, bands):
        value = None
        for g in range(2):
            for j in range(max(0, h - (n_heads - near)), min(h, near - 1) + 1):
                band = bands(g, j)
                value = band if value is None else jnp.where(held[g][j][h], band, value)
        return value

    def turned(which):
        return lambda h: heads_t[which, h * dim : (h + 1) * dim, :]

    for g in range(2):
        block = bx if g == 0 else 1 - bx
        line = seg[:, row(block, tokens, tokens)].astype(F32)
        seg_col[g] = jnp.broadcast_to(line, (128, tokens)).T

    l_x.wait()

    for which in (1, 2, 0):
        l_qkv[which].wait()
        bias = None if which == 1 else b_qv[0 if which == 0 else 1 : (0 if which == 0 else 1) + 1, :]

        @loop(2)
        def _(blk, which=which, bias=bias):
            value = nn(x[row(blk, tokens // 2, tokens // 2), :], wqkv[which])
            if bias is not None:
                value = value + bias
            heads_t[which, :, row(blk, tokens // 2, tokens // 2)] = value.astype(BF16).T

        if which == 2:

            l_wout.start()
            l_wup.start()
            pl.semaphore_wait(barrier, 5)
            kv_copies = []
            for j in range(near):
                kv_send[j, 0] = pick(1, j, turned(1))
                kv_send[j, 1] = pick(1, j, turned(2))
                kv_copies.append(
                    remote(kv_send.at[j], kv_recv.at[j], kv_ss.at[j], kv_rs.at[j], to_x)
                )
                kv_copies[j].start()

    q_tile = tokens // 2
    for j in range(near):
        kv_near[j, 0] = pick(0, j, turned(1))
        kv_near[j, 1] = pick(0, j, turned(2))
        for g in range(2):
            q_slots[g * span + j * dim : g * span + (j + 1) * dim, :] = pick(g, j, turned(0))

    def head_bands(g, j):
        source = kv_recv if g else kv_near
        return q_slots[row(g * near + j, dim, dim), :], source[j, 0], source[j, 1]

    def allowed_of(g, t):
        key_side = jnp.concatenate([seg_col[g]] * (q_tile // 128), axis=1)
        query_side = seg[:, row(2 * bx + t, q_tile, q_tile)].astype(F32)
        return key_side == query_side

    def attend(g, first, count, tiles=(0, 1)):
        @loop(count, start=first)
        def _(j):
            q_band, k_band, v_band = head_bands(g, j)
            keys = k_band.T
            for t in tiles:
                cols = slice(t * q_tile, (t + 1) * q_tile)
                scores = nn(keys, q_band[:, cols]) * scale
                allowed = allowed_of(g, t)
                peak = jnp.max(jnp.where(allowed, scores, MASKED), axis=0, keepdims=True)
                weights = jnp.exp(jnp.where(allowed, scores - peak, MASKED))
                total = jnp.sum(weights, axis=0, keepdims=True)
                safe = jnp.where(total > 0, total, 1.0)
                probs = (weights * (1.0 / safe)).astype(BF16)
                band = row(g * near + j, dim, dim)
                ctx_t[band, cols] = nn(v_band, probs).astype(BF16)
                lse[pl.ds(g * near + j, 1), cols] = jnp.where(total > 0, peak + jnp.log(safe), 0.0)

    r_tile = tokens // 2

    def exchange(index, blk):
        area = pl.ds(blk * r_tile, r_tile)
        return remote(
            ex_send.at[index, area],
            ex_recv.at[index, area],
            ex_ss.at[index, blk],
            ex_rs.at[index, blk],
            to_core,
        )

    def both(index, area):
        return ex_send[index, area, :].astype(F32) + ex_recv[index, area, :].astype(F32)

    def project_out(blk):
        area = slice(blk * r_tile, (blk + 1) * r_tile)
        for h in range(n_heads):
            band = unpick(
                h, lambda g, j: ctx_t[(g * near + j) * dim : (g * near + j + 1) * dim, area]
            )
            ctx[area, h * dim : (h + 1) * dim] = band.T
        ex_send[0, area, :] = nn(ctx[area, :], wout[...]).astype(BF16)
        exchange(0, blk).start()

    attend(0, 0, near)
    l_wout.wait()
    l_wdown.start()
    for j in range(near - 1):
        kv_copies[j].wait()
        attend(1, j, 1)
    kv_copies[near - 1].wait()
    for blk in range(2):
        attend(1, near - 1, 1, (blk,))
        project_out(blk)

    sub = 128
    f_tile = 256

    def norm(value):
        center = jnp.mean(value, axis=-1, keepdims=True)
        offset = value - center
        spread = jnp.mean(offset * offset, axis=-1, keepdims=True)
        inverse = lax.rsqrt(spread + EPSILON)
        return offset * inverse, inverse

    l_wup.wait()
    l_gout.start()
    for blk in range(2):
        whole = slice(blk * r_tile, (blk + 1) * r_tile)
        exchange(0, blk).wait()

        @loop(r_tile // sub, start=blk * (r_tile // sub))
        def _(i):
            area = row(i, sub, sub)
            value = x[area, :].astype(F32) + b_out[...] + both(0, area)
            normal, inverse = norm(value)
            n1[area, :] = normal
            r1[area, :] = jnp.broadcast_to(inverse, (sub, 128))
            low = (normal * gain1[...] + shift1[...]).astype(BF16)
            a1[area, :] = low
            a1_t[:, area] = low.T

        @loop(hidden // f_tile)
        def _(i):
            cols = row(i, f_tile, f_tile)
            up = nn(a1[whole, :], wup[:, cols]) + b_up[:, cols]
            below = 0.5 + 0.5 * lax.erf(up * ROOT_HALF)
            act[whole, cols] = (up * below).astype(BF16)
            slope[whole, cols] = below + up * (DENSITY * jnp.exp(-0.5 * up * up))

        if blk == 0:
            l_wdown.wait()
        ex_send[1, whole, :] = nn(act[whole, :], wdown[...]).astype(BF16)
        exchange(1, blk).start()

    acc[...] = jnp.zeros_like(acc)
    l_gout.wait()
    for blk in range(2):
        exchange(1, blk).wait()

        @loop(r_tile // sub, start=blk * (r_tile // sub))
        def _(i):
            area = row(i, sub, sub)
            first = n1[area, :] * gain1[...] + shift1[...]
            value = first + b_down[...] + both(1, area)
            normal, inverse = norm(value)
            out[area, :] = (normal * gain2[...] + shift2[...]).astype(BF16)
            up = gout[area, :].astype(F32)
            acc[0] += fold_rows(up)
            acc[1] += fold_rows(up * normal)
            scaled = up * gain2[...]
            mean_r = jnp.mean(scaled, axis=-1, keepdims=True)
            mean_rn = jnp.mean(scaled * normal, axis=-1, keepdims=True)
            down = (scaled - mean_r - normal * mean_rn) * inverse
            acc[2] += fold_rows(down)
            dz[area, :] = down
            low = down.astype(BF16)
            dz2[area, :] = low
            dz_t[:, area] = low.T

    mine = {"w": zh, "z": zl, "y": yi, "x": bx}
    partner = {"w": to_z2, "z": to_z1, "y": to_y, "x": to_x}

    def chain_refs(name):
        order, at, late = CHAINS[name]
        if late:
            return order, at, part_l, (rl0, rl1, rl2, rl3, rl4), fin_l, at + 6
        return order, at, part_f, (rf0, rf1, rf2, rf3, rf4), fin_f, at

    def chain_copy(name, k):
        order, at, part, got, fin, sem = chain_refs(name)
        if k == 4:
            src, where = fin.at[at], to_x
        else:
            where = partner[order[k]]
            index = [at]
            for d in "wzyx":
                if d == order[k]:
                    index.append(1 - mine[d])
                elif d in order[:k]:
                    index.append(mine[d])
                else:
                    index.append(slice(None))
            src = part.at[tuple(index)]
        return remote(src, got[k].at[at], c_ss.at[sem, k], c_rs.at[sem, k], where)

    def plus(left, right):
        return left.astype(F32) + right.astype(F32)

    def advance(name, k):
        order, at, part, got, fin, _ = chain_refs(name)
        chain_copy(name, k).wait()
        free = [d for d in "wzyx" if d not in order[: k + 1]]
        if k < 3:

            @loop(2 ** len(free))
            def _(i):
                spot = {d: lax.rem(i // 2**n, 2) for n, d in enumerate(free)}
                whole = tuple(spot[d] if d in free else mine[d] for d in "wzyx")
                some = tuple(spot[d] for d in free)
                part[(at,) + whole] = plus(part[(at,) + whole], got[k][(at,) + some]).astype(BF16)

        elif k == 3:
            total = plus(part[at, zh, zl, yi, bx], got[3][at]).astype(BF16)
            fin[at] = total
            target_of(name)[row(bx, half, half), :] = total.astype(F32)
        else:
            target_of(name)[row(1 - bx, half, half), :] = got[4][at].astype(F32)
        if k < 4:
            chain_copy(name, k + 1).start()

    def target_of(name):
        kind, n = name[0], CHAINS[name][1]
        if kind in "DU":
            size = part_f.shape[-1]
            return (o_down if kind == "D" else o_up).at[:, pl.ds((n % 3) * size, size)]
        return o_out if kind == "O" else o_qkv.at[n - 1]

    def weight_grad(name, left, right, base):
        _, at, part, _, _, _ = chain_refs(name)
        size = part.shape[-1]
        tile = 256 if size % 256 == 0 else size
        for n in range(size // tile):
            value = nn(left[...], right[:, base + n * tile : base + (n + 1) * tile])
            for d in range(16):
                part[
                    at, d // 8, (d // 4) % 2, (d // 2) % 2, d % 2, :, n * tile : (n + 1) * tile
                ] = value[d * half : (d + 1) * half, :].astype(BF16)
        chain_copy(name, 0).start()

    def grad_hidden():
        @loop(hidden // f_tile)
        def _(i):
            cols = row(i, f_tile, f_tile)
            total = jnp.zeros((8, f_tile), F32)
            for blk in range(2):
                area = pl.ds(blk * r_tile, r_tile)
                value = (nt(dz2[area, :], wdown[cols, :]) * slope[area, cols]).astype(BF16)
                du[area, cols] = value
                total = total + fold_rows(value.astype(F32))
            acc_up[:, cols] = total

    def send_first():
        for blk in range(2):
            area = pl.ds(blk * r_tile, r_tile)
            ex_send[2, area, :] = nt(du[area, :], wup[...]).astype(BF16)
            exchange(2, blk).start()

        @loop(tokens // sub)
        def _(i):
            area = row(i, sub, sub)
            x_t[:, area] = x[area, :].T

    def norm_back():
        for blk in range(2):
            exchange(2, blk).wait()

            @loop(r_tile // sub, start=blk * (r_tile // sub))
            def _(i):
                area = row(i, sub, sub)
                up = dz[area, :] + both(2, area)
                normal = n1[area, :]
                acc[3] += fold_rows(up)
                acc[4] += fold_rows(up * normal)
                scaled = up * gain1[...]
                mean_r = jnp.mean(scaled, axis=-1, keepdims=True)
                mean_rn = jnp.mean(scaled * normal, axis=-1, keepdims=True)
                down = (scaled - mean_r - normal * mean_rn) * r1[area, 0:1]
                acc[5] += fold_rows(down)
                dz[area, :] = down
                dz_t[:, area] = down.astype(BF16).T

    def grad_context():
        dctx_t[...] = nn(wout[...], dz_t[...]).astype(BF16)
        for g in range(2):
            for j in range(near):
                at = (g * near + j) * dim
                dctx_s[at : at + dim, :] = pick(g, j, lambda h: dctx_t[h * dim : (h + 1) * dim, :])

    def attend_back(g, first, count):
        target = dkv_send if g else dkv_near

        @loop(count, start=first)
        def _(j):
            q_band, k_band, v_band = head_bands(g, j)
            c_band = dctx_s[row(g * near + j, dim, dim), :]
            keys, values = k_band.T, v_band.T
            d_key = jnp.zeros((dim, tokens), F32)
            d_value = jnp.zeros((dim, tokens), F32)
            for t in range(2):
                cols = slice(t * q_tile, (t + 1) * q_tile)
                scores = nn(keys, q_band[:, cols]) * scale
                shifted = scores - lse[pl.ds(g * near + j, 1), cols]
                probs = jnp.exp(jnp.where(allowed_of(g, t), shifted, MASKED))
                d_probs = nn(values, c_band[:, cols])
                delta = jnp.sum(probs * d_probs, axis=0, keepdims=True)
                d_scores = (probs * (d_probs - delta)).astype(BF16)
                d_value = d_value + nt(c_band[:, cols], probs.astype(BF16))
                d_key = d_key + nt(q_band[:, cols], d_scores)
                dq_t[row(g * near + j, dim, dim), cols] = (nn(k_band, d_scores) * scale).astype(
                    BF16
                )
            target[j, 0] = (d_key * scale).astype(BF16)
            target[j, 1] = d_value.astype(BF16)

    def dkv_copy(j):
        return remote(dkv_send.at[j], dkv_far.at[j], dkv_ss.at[j], dkv_rs.at[j], to_x)

    def far_head(j):
        attend_back(1, j, 1)
        dkv_copy(j).start()

    def near_head(j):
        attend_back(0, j, 1)

    def keys_back():
        for j in range(near):
            dkv_copy(j).wait()

    def restore(which):
        for h in range(n_heads):
            if which == 0:
                band = unpick(
                    h, lambda g, j: dq_t[(g * near + j) * dim : (g * near + j + 1) * dim, :]
                )
            else:
                band = unpick(h, lambda g, j: (dkv_far if g else dkv_near)[j, which - 1])
            dqkv[:, which * local + h * dim : which * local + (h + 1) * dim] = band.T
        weight_grad("QKV"[which], x_t, dqkv, which * local)

    def send_input():
        for blk in range(2):
            area = pl.ds(blk * r_tile, r_tile)
            total = nt(dqkv[area, 0:local], wqkv[0])
            total = total + nt(dqkv[area, local : 2 * local], wqkv[1])
            total = total + nt(dqkv[area, 2 * local : 3 * local], wqkv[2])
            ex_send[3, area, :] = total.astype(BF16)
            exchange(3, blk).start()

    def small_copy(k):
        where = (to_x, to_y, to_z1, to_z2)[k]
        return remote(sm_send.at[k], sm_recv.at[k], s_ss.at[k], s_rs.at[k], where)

    def small_start():
        acc_qv[:, 0:local] = fold_rows(dqkv[:, 0:local].astype(F32))
        acc_qv[:, local:] = fold_rows(dqkv[:, 2 * local :].astype(F32))
        small = [jnp.sum(acc[i], axis=0, keepdims=True) for i in range(6)]
        small.append(jnp.sum(acc_up[:, 0:width], axis=0, keepdims=True))
        small.append(jnp.sum(acc_up[:, width:], axis=0, keepdims=True))
        small.append(jnp.sum(acc_qv[...], axis=0, keepdims=True))
        sm_send[...] = jnp.zeros_like(sm_send)
        for i, piece in enumerate(small):
            sm_send[0, i : i + 1, :] = piece
        small_copy(0).start()

    def small_step(k):
        small_copy(k).wait()
        total = sm_send[k] + sm_recv[k]
        if k < 3:
            sm_send[k + 1] = total
            small_copy(k + 1).start()
        else:
            o_small[...] = total

    def input_grad():
        for blk in range(2):
            exchange(3, blk).wait()

            @loop(r_tile // sub, start=blk * (r_tile // sub))
            def _(i):
                area = row(i, sub, sub)
                gtok[area, :] = (dz[area, :] + both(3, area)).astype(BF16)

    f_part = part_f.shape[-1]
    phases = {
        "gD0": lambda: weight_grad("D0", dz_t, act, 0),
        "gD1": lambda: weight_grad("D1", dz_t, act, f_part),
        "gD2": lambda: weight_grad("D2", dz_t, act, 2 * f_part),
        "dU": grad_hidden,
        "gU0": lambda: weight_grad("U0", a1_t, du, 0),
        "gU1": lambda: weight_grad("U1", a1_t, du, f_part),
        "gU2": lambda: weight_grad("U2", a1_t, du, 2 * f_part),
        "dA1": send_first,
        "ln1": norm_back,
        "dctx": grad_context,
        "gO": lambda: weight_grad("O", dz_t, ctx, 0),
        "gQ": lambda: restore(0),
        "wkv": keys_back,
        "gK": lambda: restore(1),
        "gV": lambda: restore(2),
        "dX": send_input,
        "small": small_start,
        "gt": input_grad,
    }
    for j in range(near):
        phases["f%d" % j] = functools.partial(far_head, j)
        phases["n%d" % j] = functools.partial(near_head, j)
    for item in PROGRAM:
        if isinstance(item, str):
            phases[item]()
        elif item[0] == "S":
            small_step(item[1])
        else:
            advance(*item)


CHAINS = {
    "D0": ("xyzw", 0, False),
    "D1": ("zyxw", 1, False),
    "D2": ("yzwx", 2, False),
    "U0": ("yzwx", 3, False),
    "U1": ("xyzw", 4, False),
    "U2": ("zyxw", 5, False),
    "O": ("xyzw", 0, True),
    "Q": ("zxyw", 1, True),
    "K": ("xyzw", 2, True),
    "V": ("yzxw", 3, True),
}

PROGRAM = (
    "gD0", "gD1", "gD2", "dU", "gU0", "gU1", "gU2", "dA1", "ln1", ("D0", 0), ("D1", 0), "dctx",
    ("D2", 0), "gO", "f0", "f1", "f2", ("U1", 0), ("U2", 0), ("U0", 0), "n0", ("D2", 1),
    ("D0", 1), "n1", ("O", 0), "n2", ("U0", 1), ("D1", 1), "gQ", ("D2", 2), ("D0", 2), ("U1", 1),
    "wkv", "gK", "gV", "dX", "small", ("D1", 2), ("U0", 2), ("D2", 3), ("U2", 1), "gt", ("O", 1),
    ("Q", 0), ("D0", 3), ("S", 0), ("K", 0), ("U1", 2), ("U0", 3), ("D2", 4), ("D1", 3), ("S", 1),
    ("O", 2), ("V", 0), ("U2", 2), ("U1", 3), ("K", 1), ("S", 2), ("O", 3), ("Q", 1), ("D0", 4),
    ("V", 1), ("U0", 4), ("S", 3), ("D1", 4), ("Q", 2), ("U2", 3), ("U1", 4), ("K", 2), ("O", 4),
    ("V", 2), ("Q", 3), ("U2", 4), ("K", 3), ("Q", 4), ("V", 3), ("K", 4), ("V", 4),
)


def finish_kernel(
    h_out, h_gtok, h_down, h_up, h_wout, h_qkv, small,
    out, gtok, down, up, wout, qkv, b_qv, b_out, gain1, shift1, b_up, b_down, gain2, shift2,
    t_out, t_gtok, t_down, t_up, t_wout, t_qkv, in_sem, out_sem,
):
    moves = (
        (h_out, t_out, out),
        (h_gtok, t_gtok, gtok),
        (h_down, t_down, down),
        (h_up, t_up, up),
        (h_wout, t_wout, wout),
        (h_qkv, t_qkv, qkv),
    )
    ins = [pltpu.make_async_copy(a, b, in_sem.at[i]) for i, (a, b, _) in enumerate(moves)]
    outs = [pltpu.make_async_copy(b, c, out_sem.at[i]) for i, (_, b, c) in enumerate(moves)]
    for copy in ins:
        copy.start()
    place = lax.axis_index("batch")
    width = small.shape[1]
    size = b_out.shape[0]

    def turn(value, amount):
        return pltpu.roll(value, value.shape[1] - amount, 1)

    lines = turn(small[0:8, :], place * size)
    for i, target in enumerate((shift2, gain2, b_down, shift1, gain1, b_out)):
        target[...] = lines[i, 0:size]
    long = b_up.shape[0]
    per = width // long
    upper = turn(small[6:7, :], lax.rem(place, per) * long)
    lower = turn(small[7:8, :], lax.rem(place, per) * long)
    chosen = jnp.where(place < per, upper, lower)
    b_up[...] = chosen[0, 0:long]
    short = b_qv.shape[1]
    first = turn(small[8:9, 0 : width // 2], place * short)
    second = turn(small[8:9, width // 2 :], place * short)
    b_qv[0:1, :] = first[:, 0:short]
    b_qv[1:2, :] = second[:, 0:short]
    for a, b in zip(ins, outs):
        a.wait()
        b.start()
    for b in outs:
        b.wait()


def fast_local(
    tokens,
    segment_ids,
    head_perm,
    w_qkv,
    b_qv,
    w_out,
    b_out,
    norm1_gain,
    norm1_shift,
    w_up,
    b_up,
    w_down,
    b_down,
    norm2_gain,
    norm2_shift,
    grad_out,
):
    seq_count, block_rows, width = tokens.shape
    count = seq_count * block_rows
    local_width = w_qkv.shape[2]
    hidden = w_up.shape[1]
    n_batch = lax.axis_size("batch")
    rows = width // n_batch
    half = rows // 2
    near = head_perm.shape[0] // 2
    dim = local_width // head_perm.shape[0]
    dma, vm = pltpu.SemaphoreType.DMA, pltpu.VMEM

    def chain_buffers(number, half, size):
        steps = [(2, 2, 2, 2), (2, 2, 2), (2, 2), (2,), (), (), ()]
        return [vm((number,) + step + (half, size), BF16) for step in steps]

    in_vmem = pl.BlockSpec(memory_space=pltpu.VMEM)
    in_place = pl.BlockSpec(memory_space=pl.ANY)
    in_hbm = pl.BlockSpec(memory_space=pltpu.HBM)
    in_smem = pl.BlockSpec(memory_space=pltpu.SMEM)
    outs = pl.pallas_call(
        layer_kernel,
        out_shape=(
            jax.ShapeDtypeStruct((count, width), BF16),
            jax.ShapeDtypeStruct((count, width), BF16),
            jax.ShapeDtypeStruct((rows, hidden), F32),
            jax.ShapeDtypeStruct((rows, hidden), F32),
            jax.ShapeDtypeStruct((rows, local_width), F32),
            jax.ShapeDtypeStruct((3, rows, local_width), F32),
            jax.ShapeDtypeStruct((16, width), F32),
        ),
        in_specs=[in_vmem, in_smem] + [in_vmem] * 8 + [in_hbm] * 6,
        out_specs=[in_vmem] * 7,
        scratch_shapes=[
            vm((1, width), F32),
            vm((1, width), F32),
            vm((1, width), F32),
            vm((1, hidden), F32),
            vm((1, width), F32),
            vm((1, width), F32),
            vm((1, width), F32),
            vm((count, width), BF16),
            vm((3, width, local_width), BF16),
            vm((local_width, width), BF16),
            vm((width, hidden), BF16),
            vm((hidden, width), BF16),
            vm((count, width), BF16),
            vm((3, local_width, count), BF16),
            vm((near, 2, dim, count), BF16),
            vm((near, 2, dim, count), BF16),
            vm((near, 2, dim, count), BF16),
            vm((local_width, count), BF16),
            vm((local_width, count), BF16),
            vm((count, local_width), BF16),
            vm((8, count), F32),
            vm((2, count, 128), F32),
            vm((4, count, width), BF16),
            vm((4, count, width), BF16),
            vm((count, width), BF16),
            vm((width, count), BF16),
            vm((count, width), F32),
            vm((count, 128), F32),
            vm((count, hidden), BF16),
            vm((count, hidden), F32),
            vm((count, width), F32),
            vm((count, width), BF16),
            vm((width, count), BF16),
            vm((count, hidden), BF16),
            vm((local_width, count), BF16),
            vm((local_width, count), BF16),
            vm((local_width, count), BF16),
            vm((near, 2, dim, count), BF16),
            vm((near, 2, dim, count), BF16),
            vm((near, 2, dim, count), BF16),
            vm((count, 3 * local_width), BF16),
            vm((width, count), BF16),
            *chain_buffers(6, half, hidden // 3),
            *chain_buffers(4, half, local_width),
            vm((6, 8, width), F32),
            vm((8, hidden), F32),
            vm((8, 2 * local_width), F32),
            vm((4, 16, width), F32),
            vm((4, 16, width), F32),
            dma((8,)),
            dma((near,)),
            dma((near,)),
            dma((near,)),
            dma((near,)),
            dma((4, 2)),
            dma((4, 2)),
            dma((10, 5)),
            dma((10, 5)),
            dma((4,)),
            dma((4,)),
        ],
        compiler_params=pltpu.CompilerParams(
            collective_id=0, has_side_effects=True, vmem_limit_bytes=67043328
        ),
        name="layer",
    )(
        segment_ids,
        head_perm,
        b_qv,
        b_out,
        norm1_gain,
        norm1_shift,
        b_up,
        b_down,
        norm2_gain,
        norm2_shift,
        tokens.reshape(count, width),
        jnp.transpose(w_qkv, (1, 0, 2)),
        w_out,
        w_up,
        w_down,
        grad_out.reshape(count, width),
    )
    vec = jax.ShapeDtypeStruct((rows,), F32)
    results = pl.pallas_call(
        finish_kernel,
        out_shape=(
            *[jax.ShapeDtypeStruct(value.shape, value.dtype) for value in outs[:6]],
            jax.ShapeDtypeStruct((2, local_width // n_batch), F32),
            vec,
            vec,
            vec,
            jax.ShapeDtypeStruct((hidden // n_batch,), F32),
            vec,
            vec,
            vec,
        ),
        in_specs=[in_place] * 6 + [in_vmem],
        out_specs=[in_place] * 6 + [in_vmem] * 8,
        scratch_shapes=[vm(value.shape, value.dtype) for value in outs[:6]] + [dma((6,)), dma((6,))],
        name="finish",
    )(*outs)
    output, grad_tokens, down, up, g_out, g_qkv = results[:6]
    b_qv_grad, b_out_grad, gain1_grad, shift1_grad, b_up_grad, b_down_grad = results[6:12]
    return (
        output.reshape(tokens.shape),
        grad_tokens.reshape(tokens.shape),
        jnp.transpose(g_qkv, (1, 0, 2)),
        b_qv_grad,
        g_out.T,
        b_out_grad,
        gain1_grad,
        shift1_grad,
        up,
        b_up_grad,
        down.T,
        b_down_grad,
        results[12],
        results[13],
    )


def solution(mesh):
    placed = (
        P("batch", "block", None),
        P("batch", None),
        P("tensor"),
        P(None, None, "tensor"),
        P(None, "tensor"),
        P("tensor", None),
        P(),
        P(),
        P(),
        P(None, "tensor"),
        P("tensor"),
        P("tensor", None),
        P(),
        P(),
        P(),
        P("batch", "block", None),
    )
    small_slice = mesh.shape["batch"] == 8 and mesh.shape["block"] == 2
    return jax.shard_map(
        fast_local if small_slice else local,
        mesh=mesh,
        in_specs=placed,
        out_specs=(
            P("batch", "block", None),
            P("batch", "block", None),
            P("batch", None, "tensor"),
            P(None, ("tensor", "batch")),
            P("tensor", "batch"),
            P("batch"),
            P("batch"),
            P("batch"),
            P("batch", "tensor"),
            P(("tensor", "batch")),
            P("tensor", "batch"),
            P("batch"),
            P("batch"),
            P("batch"),
        ),
        check_vma=False,
    )
```

```python
import functools

import jax
import jax.numpy as jnp
from jax import lax
from jax.experimental import pallas as pl
from jax.experimental.pallas import tpu as pltpu
from jax.sharding import PartitionSpec as P

EPSILON = 1e-12
MASKED = -1000000000.0


def swapped(value, axis, stride):
    mask = 2**stride
    pairs = [(source, source ^ mask) for source in range(lax.axis_size(axis))]
    return lax.ppermute(value, axis, pairs)


def pair_sum(value, axis):
    total = value.astype(jnp.float32)
    return total + swapped(value, axis, 0).astype(jnp.float32)


def halve(value, axis, bit, dim):
    mine = (lax.axis_index(axis) // 2**bit) % 2
    keep = lax.dynamic_index_in_dim(value, mine, dim, keepdims=False)
    give = lax.dynamic_index_in_dim(value, 1 - mine, dim, keepdims=False)
    got = swapped(give.astype(jnp.bfloat16), axis, bit)
    return keep.astype(jnp.float32) + got.astype(jnp.float32)


def scatter_sum(value, order):
    n_batch, rows, width = value.shape
    bits = n_batch.bit_length() - 1
    live = list(reversed(range(bits)))
    value = value.reshape((2,) * bits + (rows, width))
    gather = False
    for stage in order:
        if stage == "x":
            if live:
                value = value.reshape(value.shape[:-1] + (2, value.shape[-1] // 2))
                value = halve(value, "block", 0, value.ndim - 2)
                gather = True
            else:
                value = pair_sum(value.astype(jnp.bfloat16), "block")
        else:
            value = halve(value, "batch", stage, live.index(stage))
            live.remove(stage)
        if stage != order[-1] or gather:
            value = value.astype(jnp.bfloat16)
    if gather:
        other = swapped(value, "block", 0)
        first = lax.axis_index("block") == 0
        value = jnp.concatenate(
            [jnp.where(first, value, other), jnp.where(first, other, value)], axis=-1
        )
    return value.astype(jnp.float32)


def layer_norm(hidden, gain, shift):
    center = jnp.mean(hidden, axis=-1, keepdims=True)
    offset = hidden - center
    spread = jnp.mean(offset * offset, axis=-1, keepdims=True)
    return offset * lax.rsqrt(spread + EPSILON) * gain + shift


def gelu_exact(hidden):
    return jax.nn.gelu(hidden, approximate=False)


def block_scores(queries, key_rows, score_scale):
    return (
        jnp.einsum("qhd,khd->hqk", queries, key_rows, preferred_element_type=jnp.float32)
        * score_scale
    )


def forward_block(queries, key_rows, value_rows, query_segs, key_segs, score_scale):
    allowed = query_segs[None, :, None] == key_segs[:, None, :]
    scores = block_scores(queries, key_rows, score_scale)
    row_peak = jnp.max(jnp.where(allowed, scores, MASKED), axis=-1, keepdims=True)
    weights_exp = jnp.exp(jnp.where(allowed, scores - row_peak, MASKED))
    row_total = jnp.sum(weights_exp, axis=-1, keepdims=True)
    safe_total = jnp.where(row_total > 0, row_total, 1.0)
    probabilities = weights_exp / safe_total
    context = jnp.einsum(
        "hqk,khd->qhd",
        probabilities.astype(jnp.bfloat16),
        value_rows,
        preferred_element_type=jnp.float32,
    )
    logsum = jnp.where(row_total > 0, row_peak + jnp.log(safe_total), 0.0)
    return (context.astype(jnp.bfloat16), logsum)


def backward_block(
    queries, key_rows, value_rows, query_segs, key_segs, logsum, grad_context, score_scale
):
    allowed = query_segs[None, :, None] == key_segs[:, None, :]
    scores = block_scores(queries, key_rows, score_scale)
    probabilities = jnp.exp(jnp.where(allowed, scores - logsum, MASKED))
    grad_prob = jnp.einsum(
        "qhd,khd->hqk", grad_context, value_rows, preferred_element_type=jnp.float32
    )
    row_delta = jnp.sum(probabilities * grad_prob, axis=-1, keepdims=True)
    grad_scores = (probabilities * (grad_prob - row_delta)).astype(jnp.bfloat16)
    grad_queries = (
        jnp.einsum("hqk,khd->qhd", grad_scores, key_rows, preferred_element_type=jnp.float32)
        * score_scale
    )
    grad_keys = (
        jnp.einsum("hqk,qhd->khd", grad_scores, queries, preferred_element_type=jnp.float32)
        * score_scale
    )
    grad_values = jnp.einsum(
        "hqk,qhd->khd",
        probabilities.astype(jnp.bfloat16),
        grad_context,
        preferred_element_type=jnp.float32,
    )
    return (grad_queries, grad_keys, grad_values)


def local(
    tokens,
    segment_ids,
    head_perm,
    w_qkv,
    b_qv,
    w_out,
    b_out,
    norm1_gain,
    norm1_shift,
    w_up,
    b_up,
    w_down,
    b_down,
    norm2_gain,
    norm2_shift,
    grad_out,
):
    seq_count, block_rows, model_width = tokens.shape
    head_count = head_perm.shape[0]
    local_width = w_qkv.shape[2]
    head_dim = local_width // head_count
    near_heads = head_count // 2
    split_at = near_heads * head_dim
    far_width = local_width - split_at
    score_scale = head_dim ** (-0.5)
    token_count = seq_count * block_rows
    split_shape = (seq_count, block_rows, head_count, head_dim)
    flat_rows = tokens.reshape(token_count, model_width)
    head_order = jnp.argsort(head_perm, stable=True)
    head_undo = jnp.argsort(head_order, stable=True)
    sorted_qkv = jnp.take(
        w_qkv.reshape(model_width, 3, head_count, head_dim), head_order, axis=2
    ).reshape(model_width, 3 * local_width)
    sorted_bias = jnp.take(b_qv.reshape(2, head_count, head_dim), head_order, axis=1).reshape(
        2, local_width
    )
    sorted_out = jnp.take(
        w_out.reshape(head_count, head_dim, model_width), head_order, axis=0
    ).reshape(local_width, model_width)
    projected = jnp.dot(flat_rows, sorted_qkv, preferred_element_type=jnp.float32).reshape(
        token_count, 3, local_width
    )
    queries = (projected[:, 0] + sorted_bias[0]).astype(jnp.bfloat16)
    key_rows = projected[:, 1].astype(jnp.bfloat16)
    value_rows = (projected[:, 2] + sorted_bias[1]).astype(jnp.bfloat16)
    outgoing = jnp.concatenate([key_rows[:, split_at:], value_rows[:, split_at:]], axis=1).reshape(
        seq_count, block_rows, 2 * far_width
    )
    own_block = lax.axis_index("block")
    own_segs = lax.dynamic_slice_in_dim(segment_ids, own_block * block_rows, block_rows, 1)
    other_segs = lax.dynamic_slice_in_dim(segment_ids, (1 - own_block) * block_rows, block_rows, 1)
    key_segs = jnp.concatenate(
        [
            jnp.broadcast_to(own_segs[:, None, :], (seq_count, near_heads, block_rows)),
            jnp.broadcast_to(
                other_segs[:, None, :], (seq_count, head_count - near_heads, block_rows)
            ),
        ],
        axis=1,
    )
    partner = swapped(outgoing, "block", 0).reshape(token_count, 2 * far_width)
    all_keys = jnp.concatenate([key_rows[:, :split_at], partner[:, :far_width]], axis=1)
    all_values = jnp.concatenate([value_rows[:, :split_at], partner[:, far_width:]], axis=1)
    keys_full = all_keys.reshape(split_shape)
    values_full = all_values.reshape(split_shape)
    query_blocks = queries.reshape(split_shape)

    def forward_record(record):
        return forward_block(record[0], record[1], record[2], record[3], record[4], score_scale)

    context, logsum = lax.map(
        forward_record, (query_blocks, keys_full, values_full, own_segs, key_segs)
    )
    context_rows = context.reshape(token_count, local_width)
    attention = pair_sum(
        jnp.dot(context_rows, sorted_out, preferred_element_type=jnp.float32).astype(jnp.bfloat16),
        "tensor",
    )
    first_sum = flat_rows.astype(jnp.float32) + b_out + attention
    first_norm, first_back = jax.vjp(layer_norm, first_sum, norm1_gain, norm1_shift)
    first_low = first_norm.astype(jnp.bfloat16)
    up_rows = jnp.dot(first_low, w_up, preferred_element_type=jnp.float32) + b_up
    activated, gelu_back = jax.vjp(gelu_exact, up_rows)
    activated_low = activated.astype(jnp.bfloat16)
    branch = pair_sum(
        jnp.dot(activated_low, w_down, preferred_element_type=jnp.float32).astype(jnp.bfloat16),
        "tensor",
    )
    second_sum = first_norm + b_down + branch
    result, second_back = jax.vjp(layer_norm, second_sum, norm2_gain, norm2_shift)
    grad_second, grad_gain2, grad_shift2 = second_back(
        grad_out.reshape(token_count, model_width).astype(jnp.float32)
    )
    grad_second_low = grad_second.astype(jnp.bfloat16)
    grad_b_down = jnp.sum(grad_second, axis=0)
    grad_w_down = jnp.dot(grad_second_low.T, activated_low, preferred_element_type=jnp.float32)
    n_batch = lax.axis_size("batch")
    bits = tuple(range(n_batch.bit_length() - 1))
    y_last = ("x",) + bits[1:] + bits[:1]
    x_last = bits + ("x",)
    part_rows = model_width // n_batch
    final_w_down = scatter_sum(grad_w_down.reshape(n_batch, part_rows, -1), y_last).T
    (grad_up,) = gelu_back(jnp.dot(grad_second_low, w_down.T, preferred_element_type=jnp.float32))
    grad_up_low = grad_up.astype(jnp.bfloat16)
    grad_b_up = jnp.sum(grad_up_low.astype(jnp.float32), axis=0)
    grad_w_up = jnp.dot(first_low.T, grad_up_low, preferred_element_type=jnp.float32)
    final_w_up = scatter_sum(grad_w_up.reshape(n_batch, part_rows, -1), x_last)
    grad_first = grad_second + pair_sum(
        jnp.dot(grad_up_low, w_up.T, preferred_element_type=jnp.float32).astype(jnp.bfloat16),
        "tensor",
    )
    grad_middle, grad_gain1, grad_shift1 = first_back(grad_first)
    grad_middle_low = grad_middle.astype(jnp.bfloat16)
    grad_b_out = jnp.sum(grad_middle, axis=0)
    grad_out_sorted = jnp.dot(grad_middle_low.T, context_rows, preferred_element_type=jnp.float32)
    grad_context = (
        jnp.dot(grad_middle_low, sorted_out.T, preferred_element_type=jnp.float32)
        .astype(jnp.bfloat16)
        .reshape(split_shape)
    )
    back_keys, back_values = (keys_full, values_full)

    def backward_record(record):
        return backward_block(
            record[0], record[1], record[2], record[3], record[4], record[5], record[6], score_scale
        )

    grad_query, grad_key, grad_value = lax.map(
        backward_record,
        (query_blocks, back_keys, back_values, own_segs, key_segs, logsum, grad_context),
    )
    grad_query_low = grad_query.astype(jnp.bfloat16).reshape(token_count, local_width)
    grad_key_low = grad_key.astype(jnp.bfloat16).reshape(token_count, local_width)
    grad_value_low = grad_value.astype(jnp.bfloat16).reshape(token_count, local_width)
    returning = jnp.concatenate(
        [grad_key_low[:, split_at:], grad_value_low[:, split_at:]], axis=1
    ).reshape(seq_count, block_rows, 2 * far_width)
    returned = swapped(returning, "block", 0).reshape(token_count, 2 * far_width)
    grad_key_all = jnp.concatenate([grad_key_low[:, :split_at], returned[:, :far_width]], axis=1)
    grad_value_all = jnp.concatenate(
        [grad_value_low[:, :split_at], returned[:, far_width:]], axis=1
    )
    grad_qkv = jnp.stack([grad_query_low, grad_key_all, grad_value_all], axis=1).reshape(
        token_count, 3 * local_width
    )
    grad_qkv_sorted = jnp.dot(flat_rows.T, grad_qkv, preferred_element_type=jnp.float32)
    grad_bias_sorted = jnp.stack(
        [
            jnp.sum(grad_query_low.astype(jnp.float32), axis=0),
            jnp.sum(grad_value_all.astype(jnp.float32), axis=0),
        ]
    )
    grad_input = grad_middle + pair_sum(
        jnp.dot(grad_qkv, sorted_qkv.T, preferred_element_type=jnp.float32).astype(jnp.bfloat16),
        "tensor",
    )
    grad_w_qkv = jnp.take(
        grad_qkv_sorted.reshape(model_width, 3, head_count, head_dim), head_undo, axis=2
    ).reshape(model_width, 3, local_width)
    grad_b_qv = jnp.take(
        grad_bias_sorted.reshape(2, head_count, head_dim), head_undo, axis=1
    ).reshape(2, local_width)
    grad_w_out = jnp.take(
        grad_out_sorted.reshape(model_width, head_count, head_dim), head_undo, axis=1
    ).reshape(model_width, local_width)
    by_place = grad_w_qkv.reshape(n_batch, part_rows, 3, local_width)
    first_part = scatter_sum(by_place[:, :, :2].reshape(n_batch, part_rows, -1), y_last)
    second_part = scatter_sum(
        jnp.concatenate(
            [by_place[:, :, 2], grad_w_out.reshape(n_batch, part_rows, local_width)], axis=2
        ),
        x_last,
    )
    final_w_qkv = jnp.concatenate([first_part, second_part[:, :local_width]], axis=1).reshape(
        part_rows, 3, local_width
    )
    final_w_out = second_part[:, local_width:].T
    small = [
        grad_b_qv[0],
        grad_b_qv[1],
        grad_b_out,
        grad_gain1,
        grad_shift1,
        grad_b_up,
        grad_b_down,
        grad_gain2,
        grad_shift2,
    ]
    joined = jnp.concatenate([piece.reshape(n_batch, -1) for piece in small], axis=1)
    total = scatter_sum(joined[:, None, :], x_last)[0]
    ends, at = [], 0
    for piece in small:
        ends.append(total[at : at + piece.size // n_batch])
        at += piece.size // n_batch
    (bq, bv, final_b_out, final_gain1, final_shift1, final_b_up, final_b_down) = ends[:7]
    final_gain2, final_shift2 = ends[7:]
    final_b_qv = jnp.stack([bq, bv])
    output = result.astype(jnp.bfloat16).reshape(seq_count, block_rows, model_width)
    grad_tokens = grad_input.astype(jnp.bfloat16).reshape(seq_count, block_rows, model_width)
    return (
        output,
        grad_tokens,
        final_w_qkv,
        final_b_qv,
        final_w_out,
        final_b_out,
        final_gain1,
        final_shift1,
        final_w_up,
        final_b_up,
        final_w_down,
        final_b_down,
        final_gain2,
        final_shift2,
    )


F32 = jnp.float32
BF16 = jnp.bfloat16
MESH = pl.DeviceIdType.MESH
ROOT_HALF = 0.7071067811865476
DENSITY = 0.3989422804014327


def nn(left, right):
    return jnp.dot(left, right, preferred_element_type=F32)


def nt(left, right):
    return lax.dot_general(left, right, (((1,), (1,)), ((), ())), preferred_element_type=F32)


def loop(count, start=0):
    def run(body):
        def step(index, carry):
            body(index)
            return carry

        lax.fori_loop(start, start + count, step, 0)

    return run


def row(value, step, size):
    return pl.ds(pl.multiple_of(value * step, step), size)


def fold_rows(value):
    return jnp.sum(value.reshape(value.shape[0] // 8, 8, value.shape[1]), axis=0)


def layer_kernel(
    seg,
    perm,
    b_qv,
    i_b_out,
    i_gain1,
    i_shift1,
    i_b_up,
    i_b_down,
    i_gain2,
    i_shift2,
    h_x,
    h_wqkv,
    h_wout,
    h_wup,
    h_wdown,
    h_gout,
    out,
    gtok,
    o_down,
    o_up,
    o_out,
    o_qkv,
    o_small,
    b_out,
    gain1,
    shift1,
    b_up,
    b_down,
    gain2,
    shift2,
    x,
    wqkv,
    wout,
    wup,
    wdown,
    gout,
    heads_t,
    kv_send,
    kv_recv,
    kv_near,
    q_slots,
    ctx_t,
    ctx,
    lse,
    seg_col,
    ex_send,
    ex_recv,
    a1,
    a1_t,
    n1,
    r1,
    act,
    slope,
    dz,
    dz2,
    dz_t,
    du,
    dctx_t,
    dctx_s,
    dq_t,
    dkv_near,
    dkv_far,
    dkv_send,
    dqkv,
    x_t,
    part_f,
    rf0,
    rf1,
    rf2,
    rf3,
    rf4,
    fin_f,
    part_l,
    rl0,
    rl1,
    rl2,
    rl3,
    rl4,
    fin_l,
    acc,
    acc_up,
    acc_qv,
    sm_send,
    sm_recv,
    load_sem,
    kv_ss,
    kv_rs,
    dkv_ss,
    dkv_rs,
    ex_ss,
    ex_rs,
    c_ss,
    c_rs,
    s_ss,
    s_rs,
):
    tokens = x.shape[0]
    width = x.shape[1]
    local = wout.shape[0]
    hidden = wup.shape[1]
    n_heads = perm.shape[0]
    dim = local // n_heads
    near = n_heads // 2
    span = near * dim
    scale = dim ** (-0.5)
    half = part_f.shape[5]
    rows = 2 * half

    me_b = lax.axis_index("batch")
    bx = lax.axis_index("block")
    tc = lax.axis_index("tensor")
    yi = lax.rem(me_b, 2)
    zl = lax.rem(me_b // 2, 2)
    zh = me_b // 4
    to_core = {"tensor": 1 - tc}
    to_x = {"block": 1 - bx}
    to_y = {"batch": me_b + 1 - 2 * yi}
    to_z1 = {"batch": me_b + 2 - 4 * zl}
    to_z2 = {"batch": me_b + 4 - 8 * zh}

    def remote(src, dst, send, recv, where):
        return pltpu.make_async_remote_copy(
            src_ref=src,
            dst_ref=dst,
            send_sem=send,
            recv_sem=recv,
            device_id=where,
            device_id_type=MESH,
        )

    def load(source, target, index):
        return pltpu.make_async_copy(source, target, load_sem.at[index])

    l_x = load(h_x, x, 0)
    l_qkv = [load(h_wqkv.at[i], wqkv.at[i], 1 + i) for i in range(3)]
    l_wout = load(h_wout, wout, 4)
    l_wup = load(h_wup, wup, 5)
    l_wdown = load(h_wdown, wdown, 6)
    l_gout = load(h_gout, gout, 7)
    l_x.start()
    for which in (1, 2, 0):
        l_qkv[which].start()

    barrier = pltpu.get_barrier_semaphore()
    for where in (to_core, to_x, to_y, to_z1, to_z2):
        pl.semaphore_signal(barrier, inc=1, device_id=where, device_id_type=MESH)

    for target, source in (
        (b_out, i_b_out),
        (gain1, i_gain1),
        (shift1, i_shift1),
        (b_up, i_b_up),
        (b_down, i_b_down),
        (gain2, i_gain2),
        (shift2, i_shift2),
    ):
        target[...] = source[...].reshape(target.shape)

    far = [perm[h] for h in range(n_heads)]
    far_rank, near_rank = [], []
    f_count, n_count = jnp.int32(0), jnp.int32(0)
    for h in range(n_heads):
        far_rank.append(f_count)
        near_rank.append(n_count)
        f_count = f_count + far[h]
        n_count = n_count + (1 - far[h])
    rank = [far[h] * far_rank[h] + (1 - far[h]) * near_rank[h] for h in range(n_heads)]

    held = [
        [[(far[h] == g) & (rank[h] == j) for h in range(n_heads)] for j in range(near)]
        for g in range(2)
    ]

    def pick(g, j, bands):
        value = bands(j)
        for h in range(j + 1, j + 1 + n_heads - near):
            value = jnp.where(held[g][j][h], bands(h), value)
        return value

    def unpick(h, bands):
        value = None
        for g in range(2):
            for j in range(max(0, h - (n_heads - near)), min(h, near - 1) + 1):
                band = bands(g, j)
                value = band if value is None else jnp.where(held[g][j][h], band, value)
        return value

    def turned(which):
        return lambda h: heads_t[which, h * dim : (h + 1) * dim, :]

    for g in range(2):
        block = bx if g == 0 else 1 - bx
        line = seg[:, row(block, tokens, tokens)].astype(F32)
        seg_col[g] = jnp.broadcast_to(line, (128, tokens)).T

    l_x.wait()

    for which in (1, 2, 0):
        l_qkv[which].wait()
        bias = None if which == 1 else b_qv[0 if which == 0 else 1 : (0 if which == 0 else 1) + 1, :]

        @loop(2)
        def _(blk, which=which, bias=bias):
            value = nn(x[row(blk, tokens // 2, tokens // 2), :], wqkv[which])
            if bias is not None:
                value = value + bias
            heads_t[which, :, row(blk, tokens // 2, tokens // 2)] = value.astype(BF16).T

        if which == 2:

            l_wout.start()
            l_wup.start()
            pl.semaphore_wait(barrier, 5)
            kv_copies = []
            for j in range(near):
                kv_send[j, 0] = pick(1, j, turned(1))
                kv_send[j, 1] = pick(1, j, turned(2))
                kv_copies.append(
                    remote(kv_send.at[j], kv_recv.at[j], kv_ss.at[j], kv_rs.at[j], to_x)
                )
                kv_copies[j].start()

    q_tile = tokens // 2
    for j in range(near):
        kv_near[j, 0] = pick(0, j, turned(1))
        kv_near[j, 1] = pick(0, j, turned(2))
        for g in range(2):
            q_slots[g * span + j * dim : g * span + (j + 1) * dim, :] = pick(g, j, turned(0))

    def head_bands(g, j):
        source = kv_recv if g else kv_near
        return q_slots[row(g * near + j, dim, dim), :], source[j, 0], source[j, 1]

    def allowed_of(g, t):
        key_side = jnp.concatenate([seg_col[g]] * (q_tile // 128), axis=1)
        query_side = seg[:, row(2 * bx + t, q_tile, q_tile)].astype(F32)
        return key_side == query_side

    def attend(g, first, count, tiles=(0, 1)):
        @loop(count, start=first)
        def _(j):
            q_band, k_band, v_band = head_bands(g, j)
            keys = k_band.T
            for t in tiles:
                cols = slice(t * q_tile, (t + 1) * q_tile)
                scores = nn(keys, q_band[:, cols]) * scale
                allowed = allowed_of(g, t)
                peak = jnp.max(jnp.where(allowed, scores, MASKED), axis=0, keepdims=True)
                weights = jnp.exp(jnp.where(allowed, scores - peak, MASKED))
                total = jnp.sum(weights, axis=0, keepdims=True)
                safe = jnp.where(total > 0, total, 1.0)
                probs = (weights * (1.0 / safe)).astype(BF16)
                band = row(g * near + j, dim, dim)
                ctx_t[band, cols] = nn(v_band, probs).astype(BF16)
                lse[pl.ds(g * near + j, 1), cols] = jnp.where(total > 0, peak + jnp.log(safe), 0.0)

    r_tile = tokens // 2

    def exchange(index, blk):
        area = pl.ds(blk * r_tile, r_tile)
        return remote(
            ex_send.at[index, area],
            ex_recv.at[index, area],
            ex_ss.at[index, blk],
            ex_rs.at[index, blk],
            to_core,
        )

    def both(index, area):
        return ex_send[index, area, :].astype(F32) + ex_recv[index, area, :].astype(F32)

    def project_out(blk):
        area = slice(blk * r_tile, (blk + 1) * r_tile)
        for h in range(n_heads):
            band = unpick(
                h, lambda g, j: ctx_t[(g * near + j) * dim : (g * near + j + 1) * dim, area]
            )
            ctx[area, h * dim : (h + 1) * dim] = band.T
        ex_send[0, area, :] = nn(ctx[area, :], wout[...]).astype(BF16)
        exchange(0, blk).start()

    attend(0, 0, near)
    l_wout.wait()
    l_wdown.start()
    for j in range(near - 1):
        kv_copies[j].wait()
        attend(1, j, 1)
    kv_copies[near - 1].wait()
    for blk in range(2):
        attend(1, near - 1, 1, (blk,))
        project_out(blk)

    sub = 128
    f_tile = 256

    def norm(value):
        center = jnp.mean(value, axis=-1, keepdims=True)
        offset = value - center
        spread = jnp.mean(offset * offset, axis=-1, keepdims=True)
        inverse = lax.rsqrt(spread + EPSILON)
        return offset * inverse, inverse

    l_wup.wait()
    l_gout.start()
    for blk in range(2):
        whole = slice(blk * r_tile, (blk + 1) * r_tile)
        exchange(0, blk).wait()

        @loop(r_tile // sub, start=blk * (r_tile // sub))
        def _(i):
            area = row(i, sub, sub)
            value = x[area, :].astype(F32) + b_out[...] + both(0, area)
            normal, inverse = norm(value)
            n1[area, :] = normal
            r1[area, :] = jnp.broadcast_to(inverse, (sub, 128))
            low = (normal * gain1[...] + shift1[...]).astype(BF16)
            a1[area, :] = low
            a1_t[:, area] = low.T

        @loop(hidden // f_tile)
        def _(i):
            cols = row(i, f_tile, f_tile)
            up = nn(a1[whole, :], wup[:, cols]) + b_up[:, cols]
            below = 0.5 + 0.5 * lax.erf(up * ROOT_HALF)
            act[whole, cols] = (up * below).astype(BF16)
            slope[whole, cols] = below + up * (DENSITY * jnp.exp(-0.5 * up * up))

        if blk == 0:
            l_wdown.wait()
        ex_send[1, whole, :] = nn(act[whole, :], wdown[...]).astype(BF16)
        exchange(1, blk).start()

    acc[...] = jnp.zeros_like(acc)
    l_gout.wait()
    for blk in range(2):
        exchange(1, blk).wait()

        @loop(r_tile // sub, start=blk * (r_tile // sub))
        def _(i):
            area = row(i, sub, sub)
            first = n1[area, :] * gain1[...] + shift1[...]
            value = first + b_down[...] + both(1, area)
            normal, inverse = norm(value)
            out[area, :] = (normal * gain2[...] + shift2[...]).astype(BF16)
            up = gout[area, :].astype(F32)
            acc[0] += fold_rows(up)
            acc[1] += fold_rows(up * normal)
            scaled = up * gain2[...]
            mean_r = jnp.mean(scaled, axis=-1, keepdims=True)
            mean_rn = jnp.mean(scaled * normal, axis=-1, keepdims=True)
            down = (scaled - mean_r - normal * mean_rn) * inverse
            acc[2] += fold_rows(down)
            dz[area, :] = down
            low = down.astype(BF16)
            dz2[area, :] = low
            dz_t[:, area] = low.T

    mine = {"w": zh, "z": zl, "y": yi, "x": bx}
    partner = {"w": to_z2, "z": to_z1, "y": to_y, "x": to_x}

    def chain_refs(name):
        order, at, late = CHAINS[name]
        if late:
            return order, at, part_l, (rl0, rl1, rl2, rl3, rl4), fin_l, at + 6
        return order, at, part_f, (rf0, rf1, rf2, rf3, rf4), fin_f, at

    def chain_copy(name, k):
        order, at, part, got, fin, sem = chain_refs(name)
        if k == 4:
            src, where = fin.at[at], to_x
        else:
            where = partner[order[k]]
            index = [at]
            for d in "wzyx":
                if d == order[k]:
                    index.append(1 - mine[d])
                elif d in order[:k]:
                    index.append(mine[d])
                else:
                    index.append(slice(None))
            src = part.at[tuple(index)]
        return remote(src, got[k].at[at], c_ss.at[sem, k], c_rs.at[sem, k], where)

    def plus(left, right):
        return left.astype(F32) + right.astype(F32)

    def advance(name, k):
        order, at, part, got, fin, _ = chain_refs(name)
        chain_copy(name, k).wait()
        free = [d for d in "wzyx" if d not in order[: k + 1]]
        if k < 3:

            @loop(2 ** len(free))
            def _(i):
                spot = {d: lax.rem(i // 2**n, 2) for n, d in enumerate(free)}
                whole = tuple(spot[d] if d in free else mine[d] for d in "wzyx")
                some = tuple(spot[d] for d in free)
                part[(at,) + whole] = plus(part[(at,) + whole], got[k][(at,) + some]).astype(BF16)

        elif k == 3:
            total = plus(part[at, zh, zl, yi, bx], got[3][at]).astype(BF16)
            fin[at] = total
            target_of(name)[row(bx, half, half), :] = total.astype(F32)
        else:
            target_of(name)[row(1 - bx, half, half), :] = got[4][at].astype(F32)
        if k < 4:
            chain_copy(name, k + 1).start()

    def target_of(name):
        kind, n = name[0], CHAINS[name][1]
        if kind in "DU":
            size = part_f.shape[-1]
            return (o_down if kind == "D" else o_up).at[:, pl.ds((n % 3) * size, size)]
        return o_out if kind == "O" else o_qkv.at[n - 1]

    def weight_grad(name, left, right, base):
        _, at, part, _, _, _ = chain_refs(name)
        size = part.shape[-1]
        tile = 256 if size % 256 == 0 else size
        for n in range(size // tile):
            value = nn(left[...], right[:, base + n * tile : base + (n + 1) * tile])
            for d in range(16):
                part[
                    at, d // 8, (d // 4) % 2, (d // 2) % 2, d % 2, :, n * tile : (n + 1) * tile
                ] = value[d * half : (d + 1) * half, :].astype(BF16)
        chain_copy(name, 0).start()

    def grad_hidden():
        @loop(hidden // f_tile)
        def _(i):
            cols = row(i, f_tile, f_tile)
            total = jnp.zeros((8, f_tile), F32)
            for blk in range(2):
                area = pl.ds(blk * r_tile, r_tile)
                value = (nt(dz2[area, :], wdown[cols, :]) * slope[area, cols]).astype(BF16)
                du[area, cols] = value
                total = total + fold_rows(value.astype(F32))
            acc_up[:, cols] = total

    def send_first():
        for blk in range(2):
            area = pl.ds(blk * r_tile, r_tile)
            ex_send[2, area, :] = nt(du[area, :], wup[...]).astype(BF16)
            exchange(2, blk).start()

        @loop(tokens // sub)
        def _(i):
            area = row(i, sub, sub)
            x_t[:, area] = x[area, :].T

    def norm_back():
        for blk in range(2):
            exchange(2, blk).wait()

            @loop(r_tile // sub, start=blk * (r_tile // sub))
            def _(i):
                area = row(i, sub, sub)
                up = dz[area, :] + both(2, area)
                normal = n1[area, :]
                acc[3] += fold_rows(up)
                acc[4] += fold_rows(up * normal)
                scaled = up * gain1[...]
                mean_r = jnp.mean(scaled, axis=-1, keepdims=True)
                mean_rn = jnp.mean(scaled * normal, axis=-1, keepdims=True)
                down = (scaled - mean_r - normal * mean_rn) * r1[area, 0:1]
                acc[5] += fold_rows(down)
                dz[area, :] = down
                dz_t[:, area] = down.astype(BF16).T

    def grad_context():
        dctx_t[...] = nn(wout[...], dz_t[...]).astype(BF16)
        for g in range(2):
            for j in range(near):
                at = (g * near + j) * dim
                dctx_s[at : at + dim, :] = pick(g, j, lambda h: dctx_t[h * dim : (h + 1) * dim, :])

    def attend_back(g, first, count):
        target = dkv_send if g else dkv_near

        @loop(count, start=first)
        def _(j):
            q_band, k_band, v_band = head_bands(g, j)
            c_band = dctx_s[row(g * near + j, dim, dim), :]
            keys, values = k_band.T, v_band.T
            d_key = jnp.zeros((dim, tokens), F32)
            d_value = jnp.zeros((dim, tokens), F32)
            for t in range(2):
                cols = slice(t * q_tile, (t + 1) * q_tile)
                scores = nn(keys, q_band[:, cols]) * scale
                shifted = scores - lse[pl.ds(g * near + j, 1), cols]
                probs = jnp.exp(jnp.where(allowed_of(g, t), shifted, MASKED))
                d_probs = nn(values, c_band[:, cols])
                delta = jnp.sum(probs * d_probs, axis=0, keepdims=True)
                d_scores = (probs * (d_probs - delta)).astype(BF16)
                d_value = d_value + nt(c_band[:, cols], probs.astype(BF16))
                d_key = d_key + nt(q_band[:, cols], d_scores)
                dq_t[row(g * near + j, dim, dim), cols] = (nn(k_band, d_scores) * scale).astype(
                    BF16
                )
            target[j, 0] = (d_key * scale).astype(BF16)
            target[j, 1] = d_value.astype(BF16)

    def dkv_copy(j):
        return remote(dkv_send.at[j], dkv_far.at[j], dkv_ss.at[j], dkv_rs.at[j], to_x)

    def far_head(j):
        attend_back(1, j, 1)
        dkv_copy(j).start()

    def near_head(j):
        attend_back(0, j, 1)

    def keys_back():
        for j in range(near):
            dkv_copy(j).wait()

    def restore(which):
        for h in range(n_heads):
            if which == 0:
                band = unpick(
                    h, lambda g, j: dq_t[(g * near + j) * dim : (g * near + j + 1) * dim, :]
                )
            else:
                band = unpick(h, lambda g, j: (dkv_far if g else dkv_near)[j, which - 1])
            dqkv[:, which * local + h * dim : which * local + (h + 1) * dim] = band.T
        weight_grad("QKV"[which], x_t, dqkv, which * local)

    def send_input():
        for blk in range(2):
            area = pl.ds(blk * r_tile, r_tile)
            total = nt(dqkv[area, 0:local], wqkv[0])
            total = total + nt(dqkv[area, local : 2 * local], wqkv[1])
            total = total + nt(dqkv[area, 2 * local : 3 * local], wqkv[2])
            ex_send[3, area, :] = total.astype(BF16)
            exchange(3, blk).start()

    def small_copy(k):
        where = (to_x, to_y, to_z1, to_z2)[k]
        return remote(sm_send.at[k], sm_recv.at[k], s_ss.at[k], s_rs.at[k], where)

    def small_start():
        acc_qv[:, 0:local] = fold_rows(dqkv[:, 0:local].astype(F32))
        acc_qv[:, local:] = fold_rows(dqkv[:, 2 * local :].astype(F32))
        small = [jnp.sum(acc[i], axis=0, keepdims=True) for i in range(6)]
        small.append(jnp.sum(acc_up[:, 0:width], axis=0, keepdims=True))
        small.append(jnp.sum(acc_up[:, width:], axis=0, keepdims=True))
        small.append(jnp.sum(acc_qv[...], axis=0, keepdims=True))
        sm_send[...] = jnp.zeros_like(sm_send)
        for i, piece in enumerate(small):
            sm_send[0, i : i + 1, :] = piece
        small_copy(0).start()

    def small_step(k):
        small_copy(k).wait()
        total = sm_send[k] + sm_recv[k]
        if k < 3:
            sm_send[k + 1] = total
            small_copy(k + 1).start()
        else:
            o_small[...] = total

    def input_grad():
        for blk in range(2):
            exchange(3, blk).wait()

            @loop(r_tile // sub, start=blk * (r_tile // sub))
            def _(i):
                area = row(i, sub, sub)
                gtok[area, :] = (dz[area, :] + both(3, area)).astype(BF16)

    f_part = part_f.shape[-1]
    phases = {
        "gD0": lambda: weight_grad("D0", dz_t, act, 0),
        "gD1": lambda: weight_grad("D1", dz_t, act, f_part),
        "gD2": lambda: weight_grad("D2", dz_t, act, 2 * f_part),
        "dU": grad_hidden,
        "gU0": lambda: weight_grad("U0", a1_t, du, 0),
        "gU1": lambda: weight_grad("U1", a1_t, du, f_part),
        "gU2": lambda: weight_grad("U2", a1_t, du, 2 * f_part),
        "dA1": send_first,
        "ln1": norm_back,
        "dctx": grad_context,
        "gO": lambda: weight_grad("O", dz_t, ctx, 0),
        "gQ": lambda: restore(0),
        "wkv": keys_back,
        "gK": lambda: restore(1),
        "gV": lambda: restore(2),
        "dX": send_input,
        "small": small_start,
        "gt": input_grad,
    }
    for j in range(near):
        phases["f%d" % j] = functools.partial(far_head, j)
        phases["n%d" % j] = functools.partial(near_head, j)
    for item in PROGRAM:
        if isinstance(item, str):
            phases[item]()
        elif item[0] == "S":
            small_step(item[1])
        else:
            advance(*item)


CHAINS = {
    "D0": ("xyzw", 0, False),
    "D1": ("zyxw", 1, False),
    "D2": ("yzwx", 2, False),
    "U0": ("yzwx", 3, False),
    "U1": ("xyzw", 4, False),
    "U2": ("zyxw", 5, False),
    "O": ("xyzw", 0, True),
    "Q": ("zxyw", 1, True),
    "K": ("xyzw", 2, True),
    "V": ("yzxw", 3, True),
}

PROGRAM = (
    "gD0", "gD1", "gD2", "dU", "gU0", "gU1", "gU2", "dA1", "ln1", ("D0", 0), ("D1", 0), "dctx",
    ("D2", 0), "gO", "f0", "f1", "f2", ("U1", 0), ("U2", 0), ("U0", 0), "n0", ("D2", 1),
    ("D0", 1), "n1", ("O", 0), "n2", ("U0", 1), ("D1", 1), "gQ", ("D2", 2), ("D0", 2), ("U1", 1),
    "wkv", "gK", "gV", "dX", "small", ("D1", 2), ("U0", 2), ("D2", 3), ("U2", 1), "gt", ("O", 1),
    ("Q", 0), ("D0", 3), ("S", 0), ("K", 0), ("U1", 2), ("U0", 3), ("D2", 4), ("D1", 3), ("S", 1),
    ("O", 2), ("V", 0), ("U2", 2), ("U1", 3), ("K", 1), ("S", 2), ("O", 3), ("Q", 1), ("D0", 4),
    ("V", 1), ("U0", 4), ("S", 3), ("D1", 4), ("Q", 2), ("U2", 3), ("U1", 4), ("K", 2), ("O", 4),
    ("V", 2), ("Q", 3), ("U2", 4), ("K", 3), ("Q", 4), ("V", 3), ("K", 4), ("V", 4),
)


def finish_kernel(
    t_out, t_gtok, t_down, t_up, t_wout, t_qkv, small,
    out, gtok, down, up, wout, qkv, b_qv, b_out, gain1, shift1, b_up, b_down, gain2, shift2,
    out_sem,
):
    moves = ((t_out, out), (t_gtok, gtok), (t_down, down), (t_up, up), (t_wout, wout), (t_qkv, qkv))
    outs = [pltpu.make_async_copy(b, c, out_sem.at[i]) for i, (b, c) in enumerate(moves)]
    for copy in outs:
        copy.start()
    place = lax.axis_index("batch")
    width = small.shape[1]
    size = b_out.shape[0]

    def turn(value, amount):
        return pltpu.roll(value, value.shape[1] - amount, 1)

    lines = turn(small[0:8, :], place * size)
    for i, target in enumerate((shift2, gain2, b_down, shift1, gain1, b_out)):
        target[...] = lines[i, 0:size]
    long = b_up.shape[0]
    per = width // long
    upper = turn(small[6:7, :], lax.rem(place, per) * long)
    lower = turn(small[7:8, :], lax.rem(place, per) * long)
    chosen = jnp.where(place < per, upper, lower)
    b_up[...] = chosen[0, 0:long]
    short = b_qv.shape[1]
    first = turn(small[8:9, 0 : width // 2], place * short)
    second = turn(small[8:9, width // 2 :], place * short)
    b_qv[0:1, :] = first[:, 0:short]
    b_qv[1:2, :] = second[:, 0:short]
    for copy in outs:
        copy.wait()


def fast_local(
    tokens,
    segment_ids,
    head_perm,
    w_qkv,
    b_qv,
    w_out,
    b_out,
    norm1_gain,
    norm1_shift,
    w_up,
    b_up,
    w_down,
    b_down,
    norm2_gain,
    norm2_shift,
    grad_out,
):
    seq_count, block_rows, width = tokens.shape
    count = seq_count * block_rows
    local_width = w_qkv.shape[2]
    hidden = w_up.shape[1]
    n_batch = lax.axis_size("batch")
    rows = width // n_batch
    half = rows // 2
    near = head_perm.shape[0] // 2
    dim = local_width // head_perm.shape[0]
    dma, vm = pltpu.SemaphoreType.DMA, pltpu.VMEM

    def chain_buffers(number, half, size):
        steps = [(2, 2, 2, 2), (2, 2, 2), (2, 2), (2,), (), (), ()]
        return [vm((number,) + step + (half, size), BF16) for step in steps]

    in_vmem = pl.BlockSpec(memory_space=pltpu.VMEM)
    in_place = pl.BlockSpec(memory_space=pl.ANY)
    in_hbm = pl.BlockSpec(memory_space=pltpu.HBM)
    in_smem = pl.BlockSpec(memory_space=pltpu.SMEM)
    outs = pl.pallas_call(
        layer_kernel,
        out_shape=(
            vm((count, width), BF16),
            vm((count, width), BF16),
            vm((rows, hidden), F32),
            vm((rows, hidden), F32),
            vm((rows, local_width), F32),
            vm((3, rows, local_width), F32),
            vm((16, width), F32),
        ),
        in_specs=[in_vmem, in_smem] + [in_vmem] * 8 + [in_hbm] * 6,
        out_specs=[in_vmem] * 7,
        scratch_shapes=[
            vm((1, width), F32),
            vm((1, width), F32),
            vm((1, width), F32),
            vm((1, hidden), F32),
            vm((1, width), F32),
            vm((1, width), F32),
            vm((1, width), F32),
            vm((count, width), BF16),
            vm((3, width, local_width), BF16),
            vm((local_width, width), BF16),
            vm((width, hidden), BF16),
            vm((hidden, width), BF16),
            vm((count, width), BF16),
            vm((3, local_width, count), BF16),
            vm((near, 2, dim, count), BF16),
            vm((near, 2, dim, count), BF16),
            vm((near, 2, dim, count), BF16),
            vm((local_width, count), BF16),
            vm((local_width, count), BF16),
            vm((count, local_width), BF16),
            vm((8, count), F32),
            vm((2, count, 128), F32),
            vm((4, count, width), BF16),
            vm((4, count, width), BF16),
            vm((count, width), BF16),
            vm((width, count), BF16),
            vm((count, width), F32),
            vm((count, 128), F32),
            vm((count, hidden), BF16),
            vm((count, hidden), F32),
            vm((count, width), F32),
            vm((count, width), BF16),
            vm((width, count), BF16),
            vm((count, hidden), BF16),
            vm((local_width, count), BF16),
            vm((local_width, count), BF16),
            vm((local_width, count), BF16),
            vm((near, 2, dim, count), BF16),
            vm((near, 2, dim, count), BF16),
            vm((near, 2, dim, count), BF16),
            vm((count, 3 * local_width), BF16),
            vm((width, count), BF16),
            *chain_buffers(6, half, hidden // 3),
            *chain_buffers(4, half, local_width),
            vm((6, 8, width), F32),
            vm((8, hidden), F32),
            vm((8, 2 * local_width), F32),
            vm((4, 16, width), F32),
            vm((4, 16, width), F32),
            dma((8,)),
            dma((near,)),
            dma((near,)),
            dma((near,)),
            dma((near,)),
            dma((4, 2)),
            dma((4, 2)),
            dma((10, 5)),
            dma((10, 5)),
            dma((4,)),
            dma((4,)),
        ],
        compiler_params=pltpu.CompilerParams(
            collective_id=0, has_side_effects=True, vmem_limit_bytes=59000000
        ),
        name="layer",
    )(
        segment_ids,
        head_perm,
        b_qv,
        b_out,
        norm1_gain,
        norm1_shift,
        b_up,
        b_down,
        norm2_gain,
        norm2_shift,
        tokens.reshape(count, width),
        jnp.transpose(w_qkv, (1, 0, 2)),
        w_out,
        w_up,
        w_down,
        grad_out.reshape(count, width),
    )
    vec = jax.ShapeDtypeStruct((rows,), F32)
    results = pl.pallas_call(
        finish_kernel,
        out_shape=(
            *[jax.ShapeDtypeStruct(value.shape, value.dtype) for value in outs[:6]],
            jax.ShapeDtypeStruct((2, local_width // n_batch), F32),
            vec,
            vec,
            vec,
            jax.ShapeDtypeStruct((hidden // n_batch,), F32),
            vec,
            vec,
            vec,
        ),
        in_specs=[in_vmem] * 7,
        out_specs=[in_hbm] * 6 + [in_vmem] * 8,
        scratch_shapes=[dma((6,))],
        compiler_params=pltpu.CompilerParams(vmem_limit_bytes=4194304),
        name="finish",
    )(*outs)
    output, grad_tokens, down, up, g_out, g_qkv = results[:6]
    b_qv_grad, b_out_grad, gain1_grad, shift1_grad, b_up_grad, b_down_grad = results[6:12]
    return (
        output.reshape(tokens.shape),
        grad_tokens.reshape(tokens.shape),
        jnp.transpose(g_qkv, (1, 0, 2)),
        b_qv_grad,
        g_out.T,
        b_out_grad,
        gain1_grad,
        shift1_grad,
        up,
        b_up_grad,
        down.T,
        b_down_grad,
        results[12],
        results[13],
    )


def solution(mesh):
    placed = (
        P("batch", "block", None),
        P("batch", None),
        P("tensor"),
        P(None, None, "tensor"),
        P(None, "tensor"),
        P("tensor", None),
        P(),
        P(),
        P(),
        P(None, "tensor"),
        P("tensor"),
        P("tensor", None),
        P(),
        P(),
        P(),
        P("batch", "block", None),
    )
    small_slice = mesh.shape["batch"] == 8 and mesh.shape["block"] == 2
    return jax.shard_map(
        fast_local if small_slice else local,
        mesh=mesh,
        in_specs=placed,
        out_specs=(
            P("batch", "block", None),
            P("batch", "block", None),
            P("batch", None, "tensor"),
            P(None, ("tensor", "batch")),
            P("tensor", "batch"),
            P("batch"),
            P("batch"),
            P("batch"),
            P("batch", "tensor"),
            P(("tensor", "batch")),
            P("tensor", "batch"),
            P("batch"),
            P("batch"),
            P("batch"),
        ),
        check_vma=False,
    )
```
